32 devices in a mesh: gz: 8 (over z, y), gy: 4 (over x, core).
Axes of the slice: x: 2, y: 2, z: 4, core: 2. Of those that a mesh axis runs over, the one named last changes fastest.
Arguments:
- orbitals: bfloat16 [96, 96, 96, 256], P('gz', 'gy'), may hold values from -6 to 6
- pair_list: int32 [64, 2], replicated, may hold values from 0 to 255
- box_anchor: int32 [256, 3], replicated, may hold values from 0 to 95
- pair_live: int32 [64], replicated, may hold values from 0 to 1, as said below
Outputs:
- gradient: float32 [96, 96, 96, 256], P('gz', 'gy')
The draws below stay inside these ranges and needn't reach their ends.
Inputs may be any that keep to these rules, and one draw needn't show every extreme that they name: `pair_live`: in each owner's block of 2 slots the live slots come first; at least one slot of every block is live, some block has all 2 live, and some other block has exactly one live.
All inputs are finite; a program needn't handle non-finite values.
Results may differ from the reference program's by a relative error of at most 0.0035.
Values may be sent and summed in bfloat16 or wider, within the bound.
A program may use at most 192 MiB of HBM per device.

```python
import jax
import jax.numpy as jnp
from jax import lax

ORB = 256
GRID = 96
B = 64
PAIR_DEV = 2
PAIRS = 64


def draw_pair_live(key, part):
    base = jax.random.fold_in(key, 7)
    first_key, second_key, third_key = jax.random.split(base, 3)
    owners = PAIRS // PAIR_DEV
    counts = jax.random.randint(first_key, (owners,), 1, PAIR_DEV + 1)
    fullest = jax.random.randint(second_key, (), 0, owners)
    offset = jax.random.randint(third_key, (), 1, owners)
    sparsest = (fullest + offset) % owners
    counts = jnp.where(jnp.arange(owners) == fullest, PAIR_DEV, counts)
    counts = jnp.where(jnp.arange(owners) == sparsest, 1, counts)
    slot = jnp.arange(PAIRS) % PAIR_DEV
    return (slot < jnp.repeat(counts, PAIR_DEV)).astype(jnp.int32)


def place_ends(values, key, smallest, high):
    longest = values.shape.index(max(values.shape))
    spots = []
    for shift in (0, 1):
        where = [jax.random.randint(jax.random.fold_in(key, axis), (), 0, length) for axis, length in enumerate(values.shape)]
        where[longest] = (where[longest] + shift) % values.shape[longest]
        spots.append(tuple(where))
    return values.at[spots[0]].set(smallest).at[spots[1]].set(high)


def steps_of(rng, shape, pieces, least, largest):
    def one(axis_at, shards_of):
        steps = jax.random.uniform(jax.random.fold_in(jax.random.fold_in(rng, 6), axis_at), (shards_of,), jnp.float32, least / len(pieces), largest / len(pieces))
        return jnp.repeat(jnp.exp(steps), shape[axis_at] // shards_of).reshape((-1,) + (1,) * (len(shape) - axis_at - 1))

    gain = one(*pieces[0])
    for cut in pieces[1:]:
        gain = gain * one(*cut)
    return gain


def centred(key, dims, scale, limit, shards=(), held_as=jnp.bfloat16):
    gain = steps_of(key, dims, shards, -0.22, 0.18) if shards else 1.0
    values = jax.random.normal(key, dims, jnp.float32) * scale * gain
    return jnp.minimum(jnp.maximum(values, -limit), limit).astype(held_as)


def setup_inputs(seed: int = 0) -> dict:
    key_of = jax.random.split(jax.random.key(seed), 5)
    return {
        "orbitals": centred(key_of[0], (GRID, GRID, GRID, ORB), 1.0, 6.0, ((0, 8), (1, 4))),
        "pair_list": place_ends(jax.random.randint(key_of[1], (PAIRS, 2), 0, ORB), jax.random.fold_in(key_of[1], 1), 0, ORB - 1).astype(jnp.int32),
        "box_anchor": place_ends(jax.random.randint(key_of[2], (ORB, 3), 0, GRID), jax.random.fold_in(key_of[2], 1), 0, GRID - 1).astype(jnp.int32),
        "pair_live": draw_pair_live(jax.random.fold_in(key_of[4], 71), 0),
    }


def poisson_box(density):
    side = density.shape[-1]
    index = jnp.arange(1, side + 1).astype(jnp.float32)
    table = jnp.sqrt(2.0 / (side + 1.0)) * jnp.sin(jnp.pi * index[:, None] * index[None, :] / (side + 1.0))
    eigen = 2.0 - 2.0 * jnp.cos(jnp.pi * index / (side + 1.0))
    denom = eigen[:, None, None] + eigen[None, :, None] + eigen[None, None, :]
    hp = lax.Precision.HIGHEST

    def apply_all(field):
        field = jnp.einsum('...abc,ai->...ibc', field, table, precision=hp)
        field = jnp.einsum('...ibc,bj->...ijc', field, table, precision=hp)
        return jnp.einsum('...ijc,ck->...ijk', field, table, precision=hp)
    return apply_all(apply_all(density) / denom)

def shift_grid(grid, anchor, sign):
    grid = jnp.roll(grid, sign * anchor[0], axis=0)
    grid = jnp.roll(grid, sign * anchor[1], axis=1)
    return jnp.roll(grid, sign * anchor[2], axis=2)

def reference(orbitals, pair_list, box_anchor, pair_live):
    major = jnp.transpose(orbitals, (3, 0, 1, 2))
    side = B

    def one_pair(p, carry):
        first = pair_list[p, 0]
        second = pair_list[p, 1]
        anchor = box_anchor[first]
        left = shift_grid(major[first], anchor, -1)[:side, :side, :side]
        right = shift_grid(major[second], anchor, -1)[:side, :side, :side]
        density = left.astype(jnp.float32) * right.astype(jnp.float32)
        potential = poisson_box(density)
        live = pair_live[p].astype(jnp.float32)
        term = (potential * right.astype(jnp.float32) * live).astype(jnp.bfloat16)
        padded = jnp.pad(term, ((0, GRID - side), (0, GRID - side), (0, GRID - side)))
        placed = shift_grid(padded, anchor, 1).astype(jnp.float32)
        return carry.at[first].add(placed)
    start = jnp.zeros((ORB, GRID, GRID, GRID), jnp.float32)
    action_major = lax.fori_loop(0, PAIRS, one_pair, start)
    action = jnp.transpose(action_major, (1, 2, 3, 0)).reshape(-1, ORB)
    action_low = action.astype(jnp.bfloat16)
    flat = orbitals.reshape(-1, ORB)
    tiles = lax.dot_general(flat, action_low, (((0,), (0,)), ((), ())), preferred_element_type=jnp.float32)
    tiles = (tiles / (float(B) ** 3 / 4.0)).astype(jnp.bfloat16)
    gradient = action - jnp.dot(flat, tiles, preferred_element_type=jnp.float32)
    return gradient.reshape(GRID, GRID, GRID, ORB)
```

```python
import functools

import jax
import jax.numpy as jnp
import numpy as np
from jax import lax
from jax.experimental import pallas as pl
from jax.experimental.pallas import tpu as pltpu
from jax.sharding import PartitionSpec as P

B = 64
LANES = 128
GAP = 8
BF = jnp.bfloat16
F32 = jnp.float32
VMEM_LIMIT = 56 * 1024 * 1024


def dot_nt(a, b):
    return lax.dot_general(a, b, (((1,), (1,)), ((), ())), preferred_element_type=F32)


def dot_nn(a, b):
    return lax.dot_general(a, b, (((1,), (0,)), ((), ())), preferred_element_type=F32)


def dot_tn(a, b):
    return lax.dot_general(a, b, (((0,), (0,)), ((), ())), preferred_element_type=F32)


def split(a):
    hi = a.astype(BF)
    return hi, (a - hi.astype(F32)).astype(BF)


def density_kernel(ax_ref, onehot_ref, lower_ref, upper_ref, out_ref, psi_ref, scr):
    _, rows, across, _ = lower_ref.shape
    pairs = onehot_ref.shape[0] // 2
    pitch = pairs + GAP

    for h, orb_ref in enumerate((lower_ref, upper_ref)):

        def row(y, carry):
            both = dot_nt(onehot_ref[...], orb_ref[0, y])
            value = both[:pairs] * both[pairs:] + carry
            sent = value.astype(BF).astype(F32)
            scr[h, pl.ds(pl.multiple_of(y * pitch, 8), pairs), :across] = sent
            psi_ref[h, 0, y] = both[pairs:].astype(BF)
            return value - sent

        lax.fori_loop(0, rows, row, jnp.zeros((pairs, across), F32), unroll=4)
    lane = lax.broadcasted_iota(jnp.int32, (rows, LANES), 1)

    def pair(p, _):
        acc = jnp.zeros((rows, LANES), F32)
        a = ax_ref[p]
        for h in range(2):
            base = h * B
            x = scr[h, pl.ds(p, rows, stride=pitch), :]
            near = pltpu.roll(x, lax.rem(base - a + 2 * LANES, LANES), 1)
            far = pltpu.roll(x, lax.rem(base + across - a + 2 * LANES, LANES), 1)
            rel = lane - base
            acc = jnp.where((rel >= 0) & (rel < B), jnp.where(rel < across - a, near, far), acc)
        out_ref[p, 0] = acc.astype(BF)
        return 0

    lax.fori_loop(0, pairs, pair, 0, unroll=8)


def window_at(ay_ref, q, table_ref, extent):
    at = pl.ds(extent - ay_ref[q], extent)
    return table_ref[0, at, :], table_ref[1, at, :]


def cell_index(az, extent, z):
    a = lax.rem(z - az + 2 * extent, extent)
    live = a < B
    return jnp.where(live, a + 1, 0), jnp.where(live, B - a, 0)


def weights_of(e_ref, lane, low, high):
    return jnp.where(lane < B, e_ref[low], e_ref[high])


def fill_powers(r_ref, e_ref):
    r2 = r_ref[...] * r_ref[...]
    e_ref[0] = jnp.zeros_like(r2)

    def one(n, power):
        power = power * r2
        e_ref[n] = 1.0 - power
        return power

    lax.fori_loop(1, B + 1, one, jnp.ones_like(r2))


def power_of(r, n):
    out = None
    while n:
        if n & 1:
            out = r if out is None else out * r
        r = r * r
        n >>= 1
    return out


def step_rates(r, lane, half, depth):
    return [r if half + t < depth else jnp.where(lane < B, r, 1.0) for t in range(half)]


def forward_kernel(depth, extent, chunks, ay_ref, az_ref, slab_ref, table_ref, wide_ref, r_ref, g_ref, *refs):
    parts = refs[:len(chunks)]
    pq_ref, d_ref, f_ref, h_ref, in_ref, e_ref, sems = refs[len(chunks):]
    n_gy, count, half, rows, _ = in_ref.shape
    copies = [
        pltpu.make_async_copy(part, in_ref.at[:, :, start:start + size], sems.at[k])
        for k, (part, (start, size)) in enumerate(zip(parts, chunks))
    ]
    for copy in copies:
        copy.start()
    fill_powers(r_ref, e_ref)
    for copy in copies:
        copy.wait()
    lane = lax.broadcasted_iota(jnp.int32, (B, LANES), 1)
    base = slab_ref[0] * depth

    def pair(q, _):
        m = window_at(ay_ref, q, table_ref, extent)[0].astype(BF)
        planes = []
        for t in range(half):
            got = [in_ref[gy, q, t].astype(F32) for gy in range(n_gy)]
            planes.append(jnp.concatenate(got, axis=0).astype(BF))
        y = dot_tn(m, jnp.concatenate(planes, axis=1))
        y = y[:B] + y[B:]
        hi, lo = split(jnp.concatenate([y[:, t * LANES:(t + 1) * LANES] for t in range(half)], axis=0))
        x = dot_nn(jnp.concatenate([hi, lo], axis=1), wide_ref[...])
        x = x[:, :LANES] + x[:, LANES:]
        r = r_ref[...]
        rates = step_rates(r, lane, half, depth)
        d = [x[t * B:(t + 1) * B] * g_ref[...] for t in range(half)]
        at = []
        for t in range(half):
            lu, lw = cell_index(az_ref[q], extent, base + t)
            hu, hw = cell_index(az_ref[q], extent, base + half + t)
            if half + t >= depth:
                hu, hw = 0, 0
            at.append((weights_of(e_ref, lane, lu, hu), weights_of(e_ref, lane, lw, hw)))
        f = at[0][0] * d[0]
        for t in range(1, half):
            f = rates[t] * f + at[t][0] * d[t]
        h = jnp.zeros((B, LANES), F32)
        for t in reversed(range(half)):
            h = r * (h + at[t][1] * d[t])
        for t in range(half):
            d_ref[q, t] = d[t]
        f_ref[q] = f
        h_ref[q] = h
        p_sum = power_of(r, depth - half) * f + pltpu.roll(f, B, 1)
        q_sum = pltpu.roll(h, B, 1) + power_of(r, half) * h
        pq_ref[q] = jnp.where(lane < B, p_sum, q_sum).astype(BF)
        return 0

    lax.fori_loop(0, count, pair, 0)


def chain_kernel(depth, extent, az_ref, r_ref, in_ref, out_ref, keep):
    n, count, _, _ = in_ref.shape
    lane = lax.broadcasted_iota(jnp.int32, (B, LANES), 1)
    rate = power_of(r_ref[...], depth)
    for s in range(count):
        f = jnp.zeros((B, LANES), F32)
        h = jnp.zeros((B, LANES), F32)
        for k in range(2 * n):
            i = k % n
            start = lax.rem(depth * i - az_ref[s] + extent, extent)
            f = jnp.where(start < B, f, 0.0)
            if k >= n:
                keep[i] = f
            f = in_ref[i, s].astype(F32) + rate * f
        for k in range(2 * n):
            i = (-k) % n
            end = lax.rem(depth * i + depth - 1 - az_ref[s] + extent, extent)
            h = jnp.where(end < B, h, 0.0)
            if k >= n:
                out_ref[i, s] = jnp.where(lane < B, keep[i], h).astype(BF)
            h = in_ref[i, s].astype(F32) + rate * h


def inverse_kernel(depth, extent, chunks, ay_ref, az_ref, slab_ref, table_ref, wide_ref, r_ref, in_ref, d_ref, f_ref, h_ref, *refs):
    outs = refs[:len(chunks)]
    e_ref = refs[-1]
    count, half, _, _ = d_ref.shape
    n_gy, _, _, rows, _ = outs[0].shape
    fill_powers(r_ref, e_ref)
    lane = lax.broadcasted_iota(jnp.int32, (B, LANES), 1)
    base = slab_ref[0] * depth

    def pair(q, _):
        m = jnp.concatenate(window_at(ay_ref, q, table_ref, extent), axis=1).astype(BF)[:, :3 * B]
        r = r_ref[...]
        rates = step_rates(r, lane, half, depth)
        came = in_ref[q].astype(F32)
        swap = pltpu.roll(came, B, 1)
        f = jnp.where(lane < B, came, power_of(r, half) * swap + pltpu.roll(f_ref[q], B, 1))
        h = jnp.where(lane < B, power_of(r, depth - half) * swap + pltpu.roll(h_ref[q], B, 1), came)
        d = [d_ref[q, t] for t in range(half)]
        at = []
        for t in range(half):
            lu, lw = cell_index(az_ref[q], extent, base + t)
            hu, hw = cell_index(az_ref[q], extent, base + half + t)
            if half + t >= depth:
                hu, hw = 0, 0
            at.append((weights_of(e_ref, lane, lu, hu), weights_of(e_ref, lane, lw, hw)))
        v = []
        for t in range(half):
            f = rates[t] * f + at[t][0] * d[t]
            v.append(at[t][1] * f)
        for t in reversed(range(half)):
            v[t] = v[t] + at[t][0] * h
            step = r if half + t < depth else jnp.where(lane < B, r, 1.0)
            h = step * (h + at[t][1] * d[t])
        hi, lo = split(jnp.concatenate(v, axis=0))
        x = dot_nn(jnp.concatenate([hi, lo], axis=1), wide_ref[...])
        x = x[:, :LANES] + x[:, LANES:]
        hi, lo = split(jnp.concatenate([x[t * B:(t + 1) * B] for t in range(half)], axis=1))
        y = dot_nn(m, jnp.concatenate([hi, hi, lo], axis=0))
        for out_ref, (start, size) in zip(outs, chunks):
            for t in range(start, start + size):
                for gy in range(n_gy):
                    out_ref[gy, q, t - start] = y[gy * rows:(gy + 1) * rows, t * LANES:(t + 1) * LANES].astype(BF)
        return 0

    lax.fori_loop(0, count, pair, 0)


def term_kernel(ax_ref, live_ref, psi_ref, lower_ref, upper_ref, in_ref, *refs):
    _, rows, across, _ = lower_ref.shape
    term_ref, tile_ref, scr = refs[-3:]
    pairs = psi_ref.shape[3]
    pitch = pairs + GAP
    lane = lax.broadcasted_iota(jnp.int32, (rows, LANES), 1)

    def pair(p, _):
        v = in_ref[p, 0].astype(F32)
        a = ax_ref[p]
        lit = live_ref[p] > 0
        rel = lane - a
        for h in range(2):
            base = h * B
            near = pltpu.roll(v, lax.rem(a - base + 2 * LANES, LANES), 1)
            far = pltpu.roll(v, lax.rem(a - across - base + 3 * LANES, LANES), 1)
            v_p = jnp.where((rel >= 0) & (rel < B) & lit, near, 0.0)
            v_p = jnp.where((rel + across < B) & lit, far, v_p)
            scr[h, pl.ds(p, rows, stride=pitch), :] = v_p
        return 0

    lax.fori_loop(0, pairs, pair, 0, unroll=4)

    @pl.when(pl.program_id(0) == 0)
    def _():
        tile_ref[...] = jnp.zeros_like(tile_ref)

    step = 4 if rows % 4 == 0 else 1
    acc = jnp.zeros(tile_ref.shape, F32)
    for h, orb_ref in enumerate((lower_ref, upper_ref)):

        def row(i, acc):
            for k in range(step):
                y = i * step + k
                v = scr[h, pl.ds(pl.multiple_of(y * pitch, 8), pairs), :across]
                t = (v * psi_ref[h, 0, y].astype(F32)).astype(BF)
                term_ref[h, 0, y] = t
                acc = acc + dot_nn(t, orb_ref[0, y])
            return acc

        acc = lax.fori_loop(0, rows // step, row, acc)
    tile_ref[...] += acc


def gradient_kernel(sel_ref, tiles_ref, orb_ref, term_ref, out_ref):
    _, rows, across, norb = orb_ref.shape
    step = 4 if rows % 4 == 0 else 1

    def some(i, _):
        at = pl.ds(i * step, step)
        o = orb_ref[0, at].reshape(step * across, norb)
        c = jnp.concatenate([term_ref[0, 0, i * step + k].T for k in range(step)], axis=0)
        total = dot_nn(c, sel_ref[...]) - dot_nn(o, tiles_ref[...])
        out_ref[0, at] = total.reshape(step, across, norb)
        return 0

    lax.fori_loop(0, rows // step, some, 0, unroll=2)


def tables():
    index = np.arange(1, B + 1, dtype=np.float64)
    s = np.sqrt(2.0 / (B + 1.0)) * np.sin(np.pi * index[:, None] * index[None, :] / (B + 1.0))
    eigen = 2.0 - 2.0 * np.cos(np.pi * index / (B + 1.0))
    hi = s.astype(jnp.bfloat16).astype(np.float64)
    lo = (s - hi).astype(jnp.bfloat16).astype(np.float64)
    eye = np.eye(LANES // B)
    bd = lambda m: np.kron(eye, m)
    wide = np.block([[bd(hi), bd(lo)], [bd(hi), np.zeros((LANES, LANES))]]).astype(jnp.bfloat16)
    left = np.stack([np.concatenate([hi, lo], axis=1), np.concatenate([hi, np.zeros((B, B))], axis=1)])
    cosh = 1.0 + 0.5 * (eigen[:, None] + eigen[None, :])
    r = cosh - np.sqrt(cosh * cosh - 1.0)
    g = 1.0 / ((1.0 / r - r) * (1.0 - r ** (2 * B + 2)))
    twice = lambda m: np.tile(m, (1, LANES // B)).astype(np.float32)
    return left.astype(np.float32), wide, twice(r), twice(g)


def body(orbitals, pair_list, box_anchor, pair_live):
    depth, rows, across, norb = orbitals.shape
    n_gz = lax.axis_size("gz")
    n_gy = lax.axis_size("gy")
    owners = n_gz * n_gy
    pairs = pair_list.shape[0]
    per_dev = pairs // owners
    group = pairs // n_gy
    extent = depth * n_gz
    half = (depth + 1) // 2
    firsts = pair_list[:, 0]
    seconds = pair_list[:, 1]
    anchors = box_anchor[firsts]
    ax = anchors[:, 2]
    gz = lax.axis_index("gz")
    gy = lax.axis_index("gy")
    mine = lax.dynamic_slice_in_dim(anchors, gy * group, group, 0)
    owned = lax.dynamic_slice_in_dim(mine, gz * per_dev, per_dev, 0)
    slab = jnp.reshape(gz, (1,)).astype(jnp.int32)
    orbs = jnp.arange(norb)
    sel = firsts[:, None] == orbs[None, :]
    hot_first = sel.astype(BF)
    hot_second = (seconds[:, None] == orbs[None, :]).astype(BF)
    hot_both = jnp.concatenate([hot_first, hot_second], axis=0)

    lead = max(half // 3, 1)
    chunks = [(start, size) for start, size in ((0, lead), (lead, half - lead)) if size]
    smem = pl.BlockSpec(memory_space=pltpu.SMEM)
    vmem = pl.BlockSpec(memory_space=pltpu.VMEM)
    hbm = pl.BlockSpec(memory_space=pl.ANY)
    full = lambda shape: pl.BlockSpec(shape, lambda t: (0,) * len(shape))
    lower = lambda start: pl.BlockSpec((1, rows, across, norb), lambda t: (t + start, 0, 0, 0))
    upper = lambda start: pl.BlockSpec(
        (1, rows, across, norb), lambda t: (jnp.minimum(t + start + half, depth - 1), 0, 0, 0)
    )
    twin = lambda start: pl.BlockSpec((2, 1, rows, pairs, across), lambda t: (0, t + start, 0, 0, 0))
    slab_spec = pl.BlockSpec((pairs, 1, rows, LANES), lambda t: (0, t, 0, 0))
    params = pltpu.CompilerParams(dimension_semantics=("arbitrary",), vmem_limit_bytes=VMEM_LIMIT)
    cells = rows * across

    incoming, psis = [], []
    for start, size in chunks:
        density, psi = pl.pallas_call(
            density_kernel,
            grid=(size,),
            out_shape=(
                jax.ShapeDtypeStruct((pairs, size, rows, LANES), BF),
                jax.ShapeDtypeStruct((2, size, rows, pairs, across), BF),
            ),
            in_specs=[smem, full((2 * pairs, norb)), lower(start), upper(start)],
            out_specs=(slab_spec, twin(0)),
            scratch_shapes=[pltpu.VMEM((2, rows * (pairs + GAP), LANES), F32)],
            compiler_params=params,
            cost_estimate=pl.CostEstimate(
                flops=8 * size * cells * norb * pairs, bytes_accessed=32 * size * cells * norb, transcendentals=0
            ),
            name="density",
        )(ax, hot_both, orbitals, orbitals)
        got = lax.all_to_all(
            density.reshape(n_gy, group, size, rows, LANES), "gy", split_axis=0, concat_axis=0, tiled=True
        )
        incoming.append(got)
        psis.append(psi)

    left, wide, rate, gain = (jnp.asarray(m) for m in tables())
    cycle = jnp.concatenate([left, jnp.zeros((2, extent - B, LANES), F32)], axis=1)
    table = jnp.concatenate([cycle, cycle], axis=1)
    single = pltpu.CompilerParams(vmem_limit_bytes=VMEM_LIMIT)
    mode = (group, B, LANES)
    pq, modes, firsts_half, seconds_half = pl.pallas_call(
        functools.partial(forward_kernel, depth, extent, chunks),
        out_shape=(
            jax.ShapeDtypeStruct(mode, BF),
            jax.ShapeDtypeStruct((group, half, B, LANES), F32),
            jax.ShapeDtypeStruct(mode, F32),
            jax.ShapeDtypeStruct(mode, F32),
        ),
        in_specs=[smem, smem, smem, vmem, vmem, vmem, vmem] + [hbm] * len(chunks),
        out_specs=(vmem,) * 4,
        scratch_shapes=[
            pltpu.VMEM((n_gy, group, half, rows, LANES), BF),
            pltpu.VMEM((B + 1, B, LANES), F32),
            pltpu.SemaphoreType.DMA((len(chunks),)),
        ],
        compiler_params=single,
        name="forward",
    )(mine[:, 1], mine[:, 0], slab, table, wide, rate, gain, *incoming)
    met = lax.all_to_all(pq, "gz", split_axis=0, concat_axis=0, tiled=True)
    chained = pl.pallas_call(
        functools.partial(chain_kernel, depth, extent),
        out_shape=jax.ShapeDtypeStruct((n_gz, per_dev, B, LANES), BF),
        in_specs=[smem, vmem, vmem],
        out_specs=vmem,
        scratch_shapes=[pltpu.VMEM((n_gz, B, LANES), F32)],
        compiler_params=single,
        name="chain",
    )(owned[:, 0], rate, met.reshape(n_gz, per_dev, B, LANES))
    edges = lax.all_to_all(chained.reshape(mode), "gz", split_axis=0, concat_axis=0, tiled=True)
    potential = pl.pallas_call(
        functools.partial(inverse_kernel, depth, extent, chunks),
        out_shape=[jax.ShapeDtypeStruct(got.shape, BF) for got in incoming],
        in_specs=[smem, smem, smem] + [vmem] * 7,
        out_specs=[vmem] * len(chunks),
        scratch_shapes=[pltpu.VMEM((B + 1, B, LANES), F32)],
        compiler_params=single,
        name="inverse",
    )(mine[:, 1], mine[:, 0], slab, table, wide, rate, edges, modes, firsts_half, seconds_half)

    term, part = None, 0.0
    for (start, size), psi, field in reversed(list(zip(chunks, psis, potential))):
        back = lax.all_to_all(field, "gy", split_axis=0, concat_axis=0, tiled=True)
        held = [] if term is None else [term]
        term, share = pl.pallas_call(
            term_kernel,
            grid=(size,),
            out_shape=(
                jax.ShapeDtypeStruct((2, half, rows, pairs, across), BF),
                jax.ShapeDtypeStruct((pairs, norb), F32),
            ),
            in_specs=[smem, smem, twin(0), lower(start), upper(start), slab_spec] + [hbm] * len(held),
            out_specs=(twin(start), full((pairs, norb))),
            scratch_shapes=[pltpu.VMEM((2, rows * (pairs + GAP), LANES), F32)],
            input_output_aliases={6: 0} if held else {},
            compiler_params=params,
            cost_estimate=pl.CostEstimate(
                flops=4 * size * cells * norb * pairs, bytes_accessed=32 * size * cells * norb, transcendentals=0
            ),
            name="term",
        )(ax, pair_live, psi, orbitals, orbitals, back.reshape(pairs, size, rows, LANES), *held)
        part = part + share
    whole = lambda x: lax.all_to_all(x, ("gz", "gy"), split_axis=0, concat_axis=0, tiled=True)
    shares = whole(part.reshape(owners, per_dev, norb))
    mine_sum = jnp.sum(shares, axis=0, keepdims=True)
    summed = whole(jnp.broadcast_to(mine_sum, shares.shape)).reshape(pairs, norb)
    inner = lax.dot_general(
        summed, sel.astype(F32), (((0,), (0,)), ((), ())), precision=lax.Precision.HIGHEST, preferred_element_type=F32
    )
    tiles = (inner / (float(B) ** 3 / 4.0)).astype(BF)

    plane = pl.BlockSpec((1, rows, across, norb), lambda z: (z, 0, 0, 0))
    return pl.pallas_call(
        gradient_kernel,
        grid=(depth,),
        out_shape=jax.ShapeDtypeStruct(orbitals.shape, F32),
        in_specs=[
            full((pairs, norb)),
            full((norb, norb)),
            plane,
            pl.BlockSpec((1, 1, rows, pairs, across), lambda z: (z // half, z % half, 0, 0, 0)),
        ],
        out_specs=plane,
        compiler_params=params,
        name="gradient",
    )(hot_first, tiles, orbitals, term)


def solution(mesh):
    return jax.shard_map(
        body,
        mesh=mesh,
        in_specs=(P("gz", "gy", None, None), P(), P(), P()),
        out_specs=P("gz", "gy", None, None),
        check_vma=False,
    )
```

```python
import functools

import jax
import jax.numpy as jnp
import numpy as np
from jax import lax
from jax.experimental import pallas as pl
from jax.experimental.pallas import tpu as pltpu
from jax.sharding import PartitionSpec as P

B = 64
LANES = 128
GAP = 8
MESH = pl.DeviceIdType.MESH
BF = jnp.bfloat16
F32 = jnp.float32
VMEM_LIMIT = 56 * 1024 * 1024


def dot_nt(a, b):
    return lax.dot_general(a, b, (((1,), (1,)), ((), ())), preferred_element_type=F32)


def dot_nn(a, b):
    return lax.dot_general(a, b, (((1,), (0,)), ((), ())), preferred_element_type=F32)


def dot_tn(a, b):
    return lax.dot_general(a, b, (((0,), (0,)), ((), ())), preferred_element_type=F32)


def split(a):
    hi = a.astype(BF)
    return hi, (a - hi.astype(F32)).astype(BF)


def cell_index(az, extent, z):
    a = lax.rem(z - az + 2 * extent, extent)
    live = a < B
    return jnp.where(live, a + 1, 0), jnp.where(live, B - a, 0)


def power_of(r, n):
    out = None
    while n:
        if n & 1:
            out = r if out is None else out * r
        r = r * r
        n >>= 1
    return out


def exchange_kernel(
    n_gz, n_gy, ax_ref, ay_ref, az_ref, own_ref, live_ref, hot_ref, table_ref, wide_ref, r_ref, g_ref, orb_hbm,
    term_hbm, sum_ref,
    orb, psi, scr, send, recv, d_ref, e_ref, f_ref, h_ref, pq, pq_in, edge, edge_in, keep, field, field_in,
    term_buf, part, part_in, slab_sum, slab_in, total,
    orb_sem, y_out, y_in, z_out, z_in, e_out, e_in, v_out, v_in, t_sem, a_out, a_in, b_out, b_in, c_out, c_in,
):
    depth, rows, across, norb = orb_hbm.shape
    half = psi.shape[1]
    pairs = psi.shape[3]
    group = pairs // n_gy
    per_dev = group // n_gz
    extent = depth * n_gz
    pitch = pairs + GAP
    wide = 2 if half % 2 == 0 else 1
    chunks = half // wide
    block = 8 if rows % 8 == 0 else 1
    gz = lax.axis_index("gz")
    gy = lax.axis_index("gy")
    at_y = lambda k: lax.rem(gy + k, n_gy)
    at_z = lambda k: lax.rem(gz + 1 + k, n_gz)
    from_z = lambda k: lax.rem(gz + 2 * n_gz - 1 - k, n_gz)
    of = lambda j, size: pl.ds(pl.multiple_of(j * size, size), size)

    def remote(src, dst, out_sem, in_sem, axis, index):
        return pltpu.make_async_remote_copy(
            src_ref=src, dst_ref=dst, send_sem=out_sem, recv_sem=in_sem, device_id={axis: index}, device_id_type=MESH
        )

    def fetch(z):
        return pltpu.make_async_copy(orb_hbm.at[z], orb.at[z, :, pl.ds(0, across), :], orb_sem.at[z])

    def pad_and_fetch(z, _):
        orb[z, :, across:, :] = jnp.zeros((rows, LANES - across, norb), BF)
        fetch(z).start()
        return 0

    def pad_and_fetch_both(t, _):
        pad_and_fetch(t, 0)

        @pl.when(half + t < depth)
        def _():
            pad_and_fetch(half + t, 0)

        return 0

    lax.fori_loop(0, half, pad_and_fetch_both, 0)

    barrier = pltpu.get_barrier_semaphore()
    for k in range(1, n_gy):
        pl.semaphore_signal(barrier, inc=1, device_id={"gy": at_y(k)}, device_id_type=MESH)

    def greet(k, _):
        pl.semaphore_signal(barrier, inc=1, device_id={"gz": at_z(k)}, device_id_type=MESH)
        return 0

    lax.fori_loop(0, n_gz - 1, greet, 0)
    pl.semaphore_wait(barrier, n_gy + n_gz - 2)

    r2 = r_ref[...] * r_ref[...]
    e_ref[0] = jnp.zeros_like(r2)

    def fill(n, power):
        power = power * r2
        e_ref[n] = 1.0 - power
        return power

    lax.fori_loop(1, B + 1, fill, jnp.ones_like(r2))

    def across_y(source, target, out_sem, in_sem, t, k):
        return remote(
            source.at[t, of(at_y(k), group)], target.at[t, of(gy, group)], out_sem.at[t, k], in_sem.at[t, k], "gy", at_y(k)
        )

    def stay_y(source, target, in_sem, t):
        return pltpu.make_async_copy(source.at[t, of(gy, group)], target.at[t, of(gy, group)], in_sem.at[t, 0])

    def start_y(source, target, out_sem, in_sem, t):
        for k in range(1, n_gy):
            across_y(source, target, out_sem, in_sem, t, k).start()
        stay_y(source, target, in_sem, t).start()

    def wait_y(source, target, out_sem, in_sem, t):
        stay_y(source, target, in_sem, t).wait()
        for k in range(1, n_gy):
            across_y(source, target, out_sem, in_sem, t, k).wait_recv()

    lane_rows = lax.broadcasted_iota(jnp.int32, (rows, LANES), 1)
    lane = lax.broadcasted_iota(jnp.int32, (B, LANES), 1)
    lower = lane < B

    def density(t):
        for h in range(2):
            z = jnp.minimum(h * half + t, depth - 1)

            @pl.when(h * half + t < depth)
            def _():
                fetch(z).wait()

            def some(i, carry):
                both = dot_nt(hot_ref[...], orb[z, pl.ds(i * 2, 2)].reshape(2 * LANES, norb))
                for k in range(2):
                    y = i * 2 + k
                    mine = both[:, k * LANES:(k + 1) * LANES]
                    value = mine[:pairs] * mine[pairs:] + carry
                    sent = value.astype(BF).astype(F32)
                    scr[h, pl.ds(pl.multiple_of(y * pitch, 8), pairs), :] = sent
                    psi[h, t, y] = mine[pairs:].astype(BF)
                    carry = value - sent
                return carry

            lax.fori_loop(0, rows // 2, some, jnp.zeros((pairs, LANES), F32), unroll=2)

        def pair(p, _):
            acc = jnp.zeros((rows, LANES), F32)
            a = ax_ref[p]
            for h in range(2):
                base = h * B
                x = scr[h, pl.ds(p, rows, stride=pitch), :]
                near = pltpu.roll(x, lax.rem(base - a + 2 * LANES, LANES), 1)
                far = pltpu.roll(x, lax.rem(base + across - a + 2 * LANES, LANES), 1)
                rel = lane_rows - base
                acc = jnp.where((rel >= 0) & (rel < B), jnp.where(rel < across - a, near, far), acc)
            send[t, p] = acc.astype(BF)
            return 0

        lax.fori_loop(0, pairs, pair, 0, unroll=8)
        start_y(send, recv, y_out, y_in, t)

    def forward(c):
        for s in range(wide):
            wait_y(send, recv, y_out, y_in, c * wide + s)

        def pair(q, _):
            m = table_ref[0, pl.ds(extent - ay_ref[q], extent), :].astype(BF)
            planes = []
            for s in range(wide):
                got = [recv[c * wide + s, j * group + q].astype(F32) for j in range(n_gy)]
                planes.append(jnp.concatenate(got, axis=0).astype(BF))
            y = dot_tn(m, jnp.concatenate(planes, axis=1))
            y = y[:B] + y[B:]
            hi, lo = split(jnp.concatenate([y[:, s * LANES:(s + 1) * LANES] for s in range(wide)], axis=0))
            x = dot_nn(jnp.concatenate([hi, lo], axis=1), wide_ref[...])
            x = x[:, :LANES] + x[:, LANES:]
            for s in range(wide):
                d_ref[q, c * wide + s] = x[s * B:(s + 1) * B] * g_ref[...]
            return 0

        lax.fori_loop(0, group, pair, 0, unroll=2)

    def stage(c, _):
        @pl.when(c < chunks)
        def _():
            def one(s, _):
                density(c * wide + s)
                return 0

            lax.fori_loop(0, wide, one, 0)

        @pl.when(c >= 1)
        def _():
            forward(c - 1)

        return 0

    lax.fori_loop(0, chunks + 1, stage, 0)

    def weights(q):
        az = az_ref[q]
        out = []
        for t in range(half):
            lu, lw = cell_index(az, extent, gz * depth + t)
            hu, hw = cell_index(az, extent, gz * depth + half + t)
            if half + t >= depth:
                hu, hw = 0, 0
            out.append((jnp.where(lower, e_ref[lu], e_ref[hu]), jnp.where(lower, e_ref[lw], e_ref[hw])))
        return out

    def rate(r, t):
        return r if half + t < depth else jnp.where(lower, r, 1.0)

    def give(k):
        j = at_z(k)
        return remote(pq.at[of(j, per_dev)], pq_in.at[gz], z_out.at[k], z_in.at[k], "gz", j)

    def give_back(k):
        j = at_z(k)
        return remote(edge.at[j], edge_in.at[of(gz, per_dev)], e_out.at[k], e_in.at[k], "gz", j)

    keep_own = pltpu.make_async_copy(pq.at[of(gz, per_dev)], pq_in.at[gz], z_in.at[n_gz - 1])
    keep_edge = pltpu.make_async_copy(edge.at[gz], edge_in.at[of(gz, per_dev)], e_in.at[n_gz - 1])

    def ends(k, _):
        j = at_z(k)
        r = r_ref[...]
        for s in range(per_dev):
            q = j * per_dev + s
            at = weights(q)
            d = [d_ref[q, t] for t in range(half)]
            f = at[0][0] * d[0]
            for t in range(1, half):
                f = rate(r, t) * f + at[t][0] * d[t]
            h = r * (at[half - 1][1] * d[half - 1])
            for t in reversed(range(half - 1)):
                h = r * (h + at[t][1] * d[t])
            f_ref[q] = f
            h_ref[q] = h
            p_sum = power_of(r, depth - half) * f + pltpu.roll(f, B, 1)
            q_sum = pltpu.roll(h, B, 1) + power_of(r, half) * h
            pq[q] = jnp.where(lower, p_sum, q_sum).astype(BF)

        @pl.when(k < n_gz - 1)
        def _():
            give(k).start()

        return 0

    lax.fori_loop(0, n_gz, ends, 0)
    keep_own.start()
    keep_own.wait()

    def taken(k, _):
        give(k).wait_recv()
        return 0

    lax.fori_loop(0, n_gz - 1, taken, 0)
    slab_rate = power_of(r_ref[...], depth)
    for s in range(per_dev):
        az = own_ref[s]

        def up(k, f):
            i = lax.rem(k, n_gz)
            start = lax.rem(depth * i - az + extent, extent)
            f = jnp.where(start < B, f, 0.0)
            keep[i] = f
            return pq_in[i, s].astype(F32) + slab_rate * f

        lax.fori_loop(0, 2 * n_gz, up, jnp.zeros((B, LANES), F32))

        def down(k, h):
            i = lax.rem(2 * n_gz - k, n_gz)
            end = lax.rem(depth * i + depth - 1 - az + extent, extent)
            h = jnp.where(end < B, h, 0.0)
            edge[i, s] = jnp.where(lower, keep[i], h).astype(BF)
            return pq_in[i, s].astype(F32) + slab_rate * h

        lax.fori_loop(0, 2 * n_gz, down, jnp.zeros((B, LANES), F32))

    def back(k, _):
        give_back(k).start()
        return 0

    lax.fori_loop(0, n_gz - 1, back, 0)
    keep_edge.start()
    keep_edge.wait()

    def solve(k, _):
        j = from_z(k)

        @pl.when(k < n_gz - 1)
        def _():
            give_back(k).wait_recv()

        r = r_ref[...]
        for s in range(per_dev):
            q = j * per_dev + s
            at = weights(q)
            came = edge_in[q].astype(F32)
            swap = pltpu.roll(came, B, 1)
            f = jnp.where(lower, came, power_of(r, half) * swap + pltpu.roll(f_ref[q], B, 1))
            h = jnp.where(lower, power_of(r, depth - half) * swap + pltpu.roll(h_ref[q], B, 1), came)
            d = [d_ref[q, t] for t in range(half)]
            v = []
            for t in range(half):
                f = rate(r, t) * f + at[t][0] * d[t]
                v.append(at[t][1] * f)
            for t in reversed(range(half)):
                d_ref[q, t] = v[t] + at[t][0] * h
                h = rate(r, t) * (h + at[t][1] * d[t])
        return 0

    lax.fori_loop(0, n_gz, solve, 0)

    def inverse(c, _):
        def pair(q, _):
            at = pl.ds(extent - ay_ref[q], extent)
            m = jnp.concatenate([table_ref[0, at, :], table_ref[1, at, :]], axis=1).astype(BF)[:, :3 * B]
            hi, lo = split(jnp.concatenate([d_ref[q, c * wide + s] for s in range(wide)], axis=0))
            x = dot_nn(jnp.concatenate([hi, lo], axis=1), wide_ref[...])
            x = x[:, :LANES] + x[:, LANES:]
            hi, lo = split(jnp.concatenate([x[s * B:(s + 1) * B] for s in range(wide)], axis=1))
            y = dot_nn(m, jnp.concatenate([hi, hi, lo], axis=0))
            for s in range(wide):
                for j in range(n_gy):
                    out = y[j * rows:(j + 1) * rows, s * LANES:(s + 1) * LANES]
                    field[c * wide + s, j * group + q] = out.astype(BF)
            return 0

        lax.fori_loop(0, group, pair, 0, unroll=2)
        for s in range(wide):
            start_y(field, field_in, v_out, v_in, c * wide + s)
        return 0

    lax.fori_loop(0, chunks, inverse, 0)
    part[...] = jnp.zeros_like(part)

    def put(t):
        slot = lax.rem(t, 2)
        return pltpu.make_async_copy(term_buf.at[slot], term_hbm.at[:, t], t_sem.at[slot])

    def term(t, _):
        wait_y(field, field_in, v_out, v_in, t)

        def pair(p, _):
            v = field_in[t, p].astype(F32)
            a = ax_ref[p]
            lit = live_ref[p] > 0
            rel = lane_rows - a
            for h in range(2):
                base = h * B
                near = pltpu.roll(v, lax.rem(a - base + 2 * LANES, LANES), 1)
                far = pltpu.roll(v, lax.rem(a - across - base + 3 * LANES, LANES), 1)
                v_p = jnp.where((rel >= 0) & (rel < B) & lit, near, 0.0)
                v_p = jnp.where((rel + across < B) & lit, far, v_p)
                scr[h, pl.ds(p, rows, stride=pitch), :] = v_p
            return 0

        lax.fori_loop(0, pairs, pair, 0, unroll=4)

        @pl.when(t >= 2)
        def _():
            put(t - 2).wait()

        slot = lax.rem(t, 2)
        for h in range(2):
            z = jnp.minimum(h * half + t, depth - 1)

            def some(i, _):
                got = []
                for k in range(block):
                    y = i * block + k
                    v = scr[h, pl.ds(pl.multiple_of(y * pitch, 8), pairs), :]
                    got.append((v * psi[h, t, y].astype(F32)).astype(BF))
                    term_buf[slot, h, y] = got[k]
                o = orb[z, pl.ds(i * block, block)].reshape(block * LANES, norb)
                part[...] += dot_nn(jnp.concatenate(got, axis=1), o)
                return 0

            lax.fori_loop(0, rows // block, some, 0)
        put(t).start()
        return 0

    lax.fori_loop(0, half, term, 0)

    def share(k):
        return remote(part.at[of(at_y(k), group)], part_in.at[k], a_out.at[k], a_in.at[k], "gy", at_y(k))

    def spread(k):
        return remote(slab_sum, slab_in.at[gz], b_out.at[k], b_in.at[k], "gz", at_z(k))

    def gather(k):
        return remote(total.at[of(gy, group)], total.at[of(gy, group)], c_out.at[k], c_in.at[k], "gy", at_y(k))

    for k in range(1, n_gy):
        share(k).start()
    own = part[of(gy, group), :]
    for k in range(1, n_gy):
        share(k).wait_recv()
        own = own + part_in[k]
    slab_sum[...] = own

    def begin(k, _):
        spread(k).start()
        return 0

    lax.fori_loop(0, n_gz - 1, begin, 0)
    slab_in[gz] = own

    def arrived(k, _):
        spread(k).wait_recv()
        return 0

    lax.fori_loop(0, n_gz - 1, arrived, 0)

    def add(i, acc):
        return acc + slab_in[i]

    total[of(gy, group), :] = lax.fori_loop(1, n_gz, add, slab_in[0])
    for k in range(1, n_gy):
        gather(k).start()
    for k in range(1, n_gy):
        gather(k).wait_recv()
    sum_ref[...] = total[...]

    def sent(t, _):
        for k in range(1, n_gy):
            across_y(send, recv, y_out, y_in, t, k).wait_send()
            across_y(field, field_in, v_out, v_in, t, k).wait_send()
        return 0

    lax.fori_loop(0, half, sent, 0)

    def drained(k, _):
        give(k).wait_send()
        give_back(k).wait_send()
        spread(k).wait_send()
        return 0

    lax.fori_loop(0, n_gz - 1, drained, 0)
    for k in range(1, n_gy):
        share(k).wait_send()
        gather(k).wait_send()
    for t in range(max(half - 2, 0), half):
        put(t).wait()


def gradient_kernel(sel_ref, tiles_ref, orb_ref, term_ref, out_ref):
    _, rows, across, norb = orb_ref.shape
    step = 4 if rows % 4 == 0 else 1

    def some(i, _):
        at = pl.ds(i * step, step)
        o = orb_ref[0, at].reshape(step * across, norb)
        c = jnp.concatenate([term_ref[0, 0, i * step + k].T[:across] for k in range(step)], axis=0)
        total = dot_nn(c, sel_ref[...]) - dot_nn(o, tiles_ref[...])
        out_ref[0, at] = total.reshape(step, across, norb)
        return 0

    lax.fori_loop(0, rows // step, some, 0, unroll=2)


def tables():
    index = np.arange(1, B + 1, dtype=np.float64)
    s = np.sqrt(2.0 / (B + 1.0)) * np.sin(np.pi * index[:, None] * index[None, :] / (B + 1.0))
    eigen = 2.0 - 2.0 * np.cos(np.pi * index / (B + 1.0))
    hi = s.astype(jnp.bfloat16).astype(np.float64)
    lo = (s - hi).astype(jnp.bfloat16).astype(np.float64)
    eye = np.eye(LANES // B)
    bd = lambda m: np.kron(eye, m)
    wide = np.block([[bd(hi), bd(lo)], [bd(hi), np.zeros((LANES, LANES))]]).astype(jnp.bfloat16)
    left = np.stack([np.concatenate([hi, lo], axis=1), np.concatenate([hi, np.zeros((B, B))], axis=1)])
    cosh = 1.0 + 0.5 * (eigen[:, None] + eigen[None, :])
    r = cosh - np.sqrt(cosh * cosh - 1.0)
    g = 1.0 / ((1.0 / r - r) * (1.0 - r ** (2 * B + 2)))
    twice = lambda m: np.tile(m, (1, LANES // B)).astype(np.float32)
    return left.astype(np.float32), wide, twice(r), twice(g)


def body(orbitals, pair_list, box_anchor, pair_live):
    depth, rows, across, norb = orbitals.shape
    n_gz = lax.axis_size("gz")
    n_gy = lax.axis_size("gy")
    pairs = pair_list.shape[0]
    group = pairs // n_gy
    per_dev = group // n_gz
    extent = depth * n_gz
    half = (depth + 1) // 2
    firsts = pair_list[:, 0]
    seconds = pair_list[:, 1]
    anchors = box_anchor[firsts]
    ax = anchors[:, 2]
    mine = lax.dynamic_slice_in_dim(anchors, lax.axis_index("gy") * group, group, 0)
    owned = lax.dynamic_slice_in_dim(mine, lax.axis_index("gz") * per_dev, per_dev, 0)
    orbs = jnp.arange(norb)
    sel = firsts[:, None] == orbs[None, :]
    hot_first = sel.astype(BF)
    hot_second = (seconds[:, None] == orbs[None, :]).astype(BF)
    hot_both = jnp.concatenate([hot_first, hot_second], axis=0)

    smem = pl.BlockSpec(memory_space=pltpu.SMEM)
    vmem = pl.BlockSpec(memory_space=pltpu.VMEM)
    hbm = pl.BlockSpec(memory_space=pl.ANY)
    left, wide, rate, gain = (jnp.asarray(m) for m in tables())
    cycle = jnp.concatenate([left, jnp.zeros((2, extent - B, LANES), F32)], axis=1)
    table = jnp.concatenate([cycle, cycle], axis=1)
    mail = pltpu.VMEM((half, pairs, rows, LANES), BF)
    mode = pltpu.VMEM((group, B, LANES), F32)
    edges = pltpu.VMEM((group, B, LANES), BF)
    owners = pltpu.VMEM((n_gz, per_dev, B, LANES), BF)
    flags = lambda *shape: pltpu.SemaphoreType.DMA(shape)
    term, summed = pl.pallas_call(
        functools.partial(exchange_kernel, n_gz, n_gy),
        out_shape=(
            jax.ShapeDtypeStruct((2, half, rows, pairs, LANES), BF),
            jax.ShapeDtypeStruct((pairs, norb), F32),
        ),
        in_specs=[smem] * 5 + [vmem] * 5 + [hbm],
        out_specs=(hbm, vmem),
        scratch_shapes=[
            pltpu.VMEM((depth, rows, LANES, norb), BF),
            pltpu.VMEM((2, half, rows, pairs, LANES), BF),
            pltpu.VMEM((2, rows * (pairs + GAP), LANES), F32),
            mail,
            mail,
            pltpu.VMEM((group, half, B, LANES), F32),
            pltpu.VMEM((B + 1, B, LANES), F32),
            mode,
            mode,
            edges,
            owners,
            owners,
            edges,
            pltpu.VMEM((n_gz, B, LANES), F32),
            mail,
            mail,
            pltpu.VMEM((2, 2, rows, pairs, LANES), BF),
            pltpu.VMEM((pairs, norb), F32),
            pltpu.VMEM((n_gy, group, norb), F32),
            pltpu.VMEM((group, norb), F32),
            pltpu.VMEM((n_gz, group, norb), F32),
            pltpu.VMEM((pairs, norb), F32),
            flags(depth),
            flags(half, n_gy),
            flags(half, n_gy),
            flags(n_gz),
            flags(n_gz),
            flags(n_gz),
            flags(n_gz),
            flags(half, n_gy),
            flags(half, n_gy),
            flags(2),
            flags(n_gy),
            flags(n_gy),
            flags(n_gz),
            flags(n_gz),
            flags(n_gy),
            flags(n_gy),
        ],
        compiler_params=pltpu.CompilerParams(
            vmem_limit_bytes=VMEM_LIMIT, collective_id=0, has_side_effects=True
        ),
        name="exchange",
    )(ax, mine[:, 1], mine[:, 0], owned[:, 0], pair_live, hot_both, table, wide, rate, gain, orbitals)
    inner = lax.dot_general(
        summed, sel.astype(F32), (((0,), (0,)), ((), ())), precision=lax.Precision.HIGHEST, preferred_element_type=F32
    )
    tiles = (inner / (float(B) ** 3 / 4.0)).astype(BF)

    plane = pl.BlockSpec((1, rows, across, norb), lambda z: (z, 0, 0, 0))
    return pl.pallas_call(
        gradient_kernel,
        grid=(depth,),
        out_shape=jax.ShapeDtypeStruct(orbitals.shape, F32),
        in_specs=[
            pl.BlockSpec((pairs, norb), lambda z: (0, 0)),
            pl.BlockSpec((norb, norb), lambda z: (0, 0)),
            plane,
            pl.BlockSpec((1, 1, rows, pairs, LANES), lambda z: (z // half, z % half, 0, 0, 0)),
        ],
        out_specs=plane,
        compiler_params=pltpu.CompilerParams(dimension_semantics=("arbitrary",), vmem_limit_bytes=VMEM_LIMIT),
        name="gradient",
    )(hot_first, tiles, orbitals, term)


def solution(mesh):
    return jax.shard_map(
        body,
        mesh=mesh,
        in_specs=(P("gz", "gy", None, None), P(), P(), P()),
        out_specs=P("gz", "gy", None, None),
        check_vma=False,
    )
```

```python
import functools

import jax
import jax.numpy as jnp
import numpy as np
from jax import lax
from jax.experimental import pallas as pl
from jax.experimental.pallas import tpu as pltpu
from jax.sharding import PartitionSpec as P

B = 64
LANES = 128
GAP = 8
MESH = pl.DeviceIdType.MESH
BF = jnp.bfloat16
F32 = jnp.float32
VMEM_LIMIT = 56 * 1024 * 1024


def dot_nt(a, b):
    return lax.dot_general(a, b, (((1,), (1,)), ((), ())), preferred_element_type=F32)


def dot_nn(a, b):
    return lax.dot_general(a, b, (((1,), (0,)), ((), ())), preferred_element_type=F32)


def dot_tn(a, b):
    return lax.dot_general(a, b, (((0,), (0,)), ((), ())), preferred_element_type=F32)


def split(a):
    hi = a.astype(BF)
    return hi, (a - hi.astype(F32)).astype(BF)


def cell_index(az, extent, z):
    a = lax.rem(z - az + 2 * extent, extent)
    live = a < B
    return jnp.where(live, a + 1, 0), jnp.where(live, B - a, 0)


def power_of(r, n):
    out = None
    while n:
        if n & 1:
            out = r if out is None else out * r
        r = r * r
        n >>= 1
    return out


def exchange_kernel(
    n_gz, n_gy, ax_ref, ay_ref, az_ref, own_ref, live_ref, hot_ref, table_ref, wide_ref, r_ref, g_ref, orb_hbm,
    term_hbm, sum_ref,
    orb, psi, scr, send, recv, d_ref, e_ref, f_ref, h_ref, pq, pq_in, edge, edge_in, keep, field, field_in,
    term_buf, part, part_in, slab_sum, slab_in, total,
    orb_sem, y_out, y_in, z_out, z_in, e_out, e_in, v_out, v_in, t_sem, a_out, a_in, b_out, b_in, c_out, c_in,
):
    depth, rows, across, norb = orb_hbm.shape
    half = psi.shape[1]
    pairs = psi.shape[3]
    group = pairs // n_gy
    per_dev = group // n_gz
    extent = depth * n_gz
    pitch = pairs + GAP
    wide = 2 if half % 2 == 0 else 1
    chunks = half // wide
    block = 8 if rows % 8 == 0 else 1
    gz = lax.axis_index("gz")
    gy = lax.axis_index("gy")
    at_y = lambda k: lax.rem(gy + k, n_gy)
    at_z = lambda k: lax.rem(gz + 1 + k, n_gz)
    from_z = lambda k: lax.rem(gz + 2 * n_gz - 1 - k, n_gz)
    lot = lambda j, h: pl.ds(pl.multiple_of(j * group + h * n_gz, n_gz), n_gz)
    of = lambda j, size: pl.ds(pl.multiple_of(j * size, size), size)

    def remote(src, dst, out_sem, in_sem, axis, index):
        return pltpu.make_async_remote_copy(
            src_ref=src, dst_ref=dst, send_sem=out_sem, recv_sem=in_sem, device_id={axis: index}, device_id_type=MESH
        )

    def fetch(z):
        return pltpu.make_async_copy(orb_hbm.at[z], orb.at[z, :, pl.ds(0, across), :], orb_sem.at[z])

    def pad_and_fetch(z, _):
        orb[z, :, across:, :] = jnp.zeros((rows, LANES - across, norb), BF)
        fetch(z).start()
        return 0

    def pad_and_fetch_both(t, _):
        pad_and_fetch(t, 0)

        @pl.when(half + t < depth)
        def _():
            pad_and_fetch(half + t, 0)

        return 0

    lax.fori_loop(0, half, pad_and_fetch_both, 0)

    barrier = pltpu.get_barrier_semaphore()
    for k in range(1, n_gy):
        pl.semaphore_signal(barrier, inc=1, device_id={"gy": at_y(k)}, device_id_type=MESH)

    def greet(k, _):
        pl.semaphore_signal(barrier, inc=1, device_id={"gz": at_z(k)}, device_id_type=MESH)
        return 0

    lax.fori_loop(0, n_gz - 1, greet, 0)
    pl.semaphore_wait(barrier, n_gy + n_gz - 2)

    r2 = r_ref[...] * r_ref[...]
    e_ref[0] = jnp.zeros_like(r2)

    def fill(n, power):
        power = power * r2
        e_ref[n] = 1.0 - power
        return power

    lax.fori_loop(1, B + 1, fill, jnp.ones_like(r2))

    def across_y(mail, h, t, k):
        source, target, out_sem, in_sem = mail
        j = at_y(k)
        return remote(
            source.at[t, lot(j, h)], target.at[t, lot(gy, h)], out_sem.at[h, t, k], in_sem.at[h, t, k], "gy", j
        )

    def stay_y(mail, h, t):
        source, target, _, in_sem = mail
        return pltpu.make_async_copy(source.at[t, lot(gy, h)], target.at[t, lot(gy, h)], in_sem.at[h, t, 0])

    def start_y(mail, h, t):
        for k in range(1, n_gy):
            across_y(mail, h, t, k).start()
        stay_y(mail, h, t).start()

    def wait_y(mail, h, t):
        stay_y(mail, h, t).wait()
        for k in range(1, n_gy):
            across_y(mail, h, t, k).wait_recv()

    outward = (send, recv, y_out, y_in)
    inward = (field, field_in, v_out, v_in)

    lane_rows = lax.broadcasted_iota(jnp.int32, (rows, LANES), 1)
    lane = lax.broadcasted_iota(jnp.int32, (B, LANES), 1)
    lower = lane < B

    def density(t):
        for h in range(2):
            z = jnp.minimum(h * half + t, depth - 1)

            @pl.when(h * half + t < depth)
            def _():
                fetch(z).wait()

            def some(i, carry):
                both = dot_nt(hot_ref[...], orb[z, pl.ds(i * 2, 2)].reshape(2 * LANES, norb))
                for k in range(2):
                    y = i * 2 + k
                    mine = both[:, k * LANES:(k + 1) * LANES]
                    value = mine[:pairs] * mine[pairs:] + carry
                    sent = value.astype(BF).astype(F32)
                    scr[h, pl.ds(pl.multiple_of(y * pitch, 8), pairs), :] = sent
                    psi[h, t, y] = mine[pairs:].astype(BF)
                    carry = value - sent
                return carry

            lax.fori_loop(0, rows // 2, some, jnp.zeros((pairs, LANES), F32), unroll=2)

        def pair(p, _):
            acc = jnp.zeros((rows, LANES), F32)
            a = ax_ref[p]
            for h in range(2):
                base = h * B
                x = scr[h, pl.ds(p, rows, stride=pitch), :]
                near = pltpu.roll(x, lax.rem(base - a + 2 * LANES, LANES), 1)
                far = pltpu.roll(x, lax.rem(base + across - a + 2 * LANES, LANES), 1)
                rel = lane_rows - base
                acc = jnp.where((rel >= 0) & (rel < B), jnp.where(rel < across - a, near, far), acc)
            send[t, p] = acc.astype(BF)
            return 0

        lax.fori_loop(0, pairs, pair, 0, unroll=8)
        start_y(outward, 0, t)

    def forward(part_at, c):
        for s in range(wide):
            wait_y(outward, part_at, c * wide + s)

        def pair(n, _):
            q = part_at * n_gz + n
            m = table_ref[0, pl.ds(extent - ay_ref[q], extent), :].astype(BF)
            planes = []
            for s in range(wide):
                got = [recv[c * wide + s, j * group + q].astype(F32) for j in range(n_gy)]
                planes.append(jnp.concatenate(got, axis=0).astype(BF))
            y = dot_tn(m, jnp.concatenate(planes, axis=1))
            y = y[:B] + y[B:]
            hi, lo = split(jnp.concatenate([y[:, s * LANES:(s + 1) * LANES] for s in range(wide)], axis=0))
            x = dot_nn(jnp.concatenate([hi, lo], axis=1), wide_ref[...])
            x = x[:, :LANES] + x[:, LANES:]
            for s in range(wide):
                d_ref[q, c * wide + s] = x[s * B:(s + 1) * B] * g_ref[...]
            return 0

        lax.fori_loop(0, n_gz, pair, 0, unroll=2)

    def stage(c, _):
        @pl.when(c < chunks)
        def _():
            def one(s, _):
                density(c * wide + s)
                return 0

            lax.fori_loop(0, wide, one, 0)

        @pl.when(c == chunks)
        def _():
            def rest(t, _):
                for h in range(1, per_dev):
                    start_y(outward, h, t)
                return 0

            lax.fori_loop(0, half, rest, 0)

        @pl.when(c >= 1)
        def _():
            forward(0, c - 1)

        return 0

    lax.fori_loop(0, chunks + 1, stage, 0)

    def weights(q):
        az = az_ref[q]
        out = []
        for t in range(half):
            lu, lw = cell_index(az, extent, gz * depth + t)
            hu, hw = cell_index(az, extent, gz * depth + half + t)
            if half + t >= depth:
                hu, hw = 0, 0
            out.append((jnp.where(lower, e_ref[lu], e_ref[hu]), jnp.where(lower, e_ref[lw], e_ref[hw])))
        return out

    def rate(r, t):
        return r if half + t < depth else jnp.where(lower, r, 1.0)

    def give(h, k):
        j = at_z(k)
        return remote(pq.at[h * n_gz + j], pq_in.at[h, gz], z_out.at[h, k], z_in.at[h, k], "gz", j)

    def give_back(h, k):
        j = at_z(k)
        return remote(edge.at[h, j], edge_in.at[h * n_gz + gz], e_out.at[h, k], e_in.at[h, k], "gz", j)

    def keep_own(h):
        return pltpu.make_async_copy(pq.at[h * n_gz + gz], pq_in.at[h, gz], z_in.at[h, n_gz - 1])

    def keep_edge(h):
        return pltpu.make_async_copy(edge.at[h, gz], edge_in.at[h * n_gz + gz], e_in.at[h, n_gz - 1])

    def ends(h):
        def one(k, _):
            q = h * n_gz + at_z(k)
            r = r_ref[...]
            at = weights(q)
            d = [d_ref[q, t] for t in range(half)]
            f = at[0][0] * d[0]
            for t in range(1, half):
                f = rate(r, t) * f + at[t][0] * d[t]
            b = r * (at[half - 1][1] * d[half - 1])
            for t in reversed(range(half - 1)):
                b = r * (b + at[t][1] * d[t])
            f_ref[q] = f
            h_ref[q] = b
            p_sum = power_of(r, depth - half) * f + pltpu.roll(f, B, 1)
            q_sum = pltpu.roll(b, B, 1) + power_of(r, half) * b
            pq[q] = jnp.where(lower, p_sum, q_sum).astype(BF)

            @pl.when(k < n_gz - 1)
            def _():
                give(h, k).start()

            return 0

        lax.fori_loop(0, n_gz, one, 0)
        keep_own(h).start()

    def chain(h):
        keep_own(h).wait()

        def taken(k, _):
            give(h, k).wait_recv()
            return 0

        lax.fori_loop(0, n_gz - 1, taken, 0)
        slab_rate = power_of(r_ref[...], depth)
        az = own_ref[h]

        def up(k, f):
            i = lax.rem(k, n_gz)
            start = lax.rem(depth * i - az + extent, extent)
            f = jnp.where(start < B, f, 0.0)
            keep[i] = f
            return pq_in[h, i].astype(F32) + slab_rate * f

        lax.fori_loop(0, 2 * n_gz, up, jnp.zeros((B, LANES), F32))

        def down(k, b):
            i = lax.rem(2 * n_gz - k, n_gz)
            end = lax.rem(depth * i + depth - 1 - az + extent, extent)
            b = jnp.where(end < B, b, 0.0)
            edge[h, i] = jnp.where(lower, keep[i], b).astype(BF)
            return pq_in[h, i].astype(F32) + slab_rate * b

        lax.fori_loop(0, 2 * n_gz, down, jnp.zeros((B, LANES), F32))

        def back(k, _):
            give_back(h, k).start()
            return 0

        lax.fori_loop(0, n_gz - 1, back, 0)
        keep_edge(h).start()

    def solve(h):
        keep_edge(h).wait()

        def one(k, _):
            q = h * n_gz + from_z(k)

            @pl.when(k < n_gz - 1)
            def _():
                give_back(h, k).wait_recv()

            r = r_ref[...]
            at = weights(q)
            came = edge_in[q].astype(F32)
            swap = pltpu.roll(came, B, 1)
            f = jnp.where(lower, came, power_of(r, half) * swap + pltpu.roll(f_ref[q], B, 1))
            b = jnp.where(lower, power_of(r, depth - half) * swap + pltpu.roll(h_ref[q], B, 1), came)
            d = [d_ref[q, t] for t in range(half)]
            v = []
            for t in range(half):
                f = rate(r, t) * f + at[t][0] * d[t]
                v.append(at[t][1] * f)
            for t in reversed(range(half)):
                d_ref[q, t] = v[t] + at[t][0] * b
                b = rate(r, t) * (b + at[t][1] * d[t])
            return 0

        lax.fori_loop(0, n_gz, one, 0)

    def inverse(part_at, c):
        def pair(n, _):
            q = part_at * n_gz + n
            at = pl.ds(extent - ay_ref[q], extent)
            m = jnp.concatenate([table_ref[0, at, :], table_ref[1, at, :]], axis=1).astype(BF)[:, :3 * B]
            hi, lo = split(jnp.concatenate([d_ref[q, c * wide + s] for s in range(wide)], axis=0))
            x = dot_nn(jnp.concatenate([hi, lo], axis=1), wide_ref[...])
            x = x[:, :LANES] + x[:, LANES:]
            hi, lo = split(jnp.concatenate([x[s * B:(s + 1) * B] for s in range(wide)], axis=1))
            y = dot_nn(m, jnp.concatenate([hi, hi, lo], axis=0))
            for s in range(wide):
                for j in range(n_gy):
                    out = y[j * rows:(j + 1) * rows, s * LANES:(s + 1) * LANES]
                    field[c * wide + s, j * group + q] = out.astype(BF)
            return 0

        lax.fori_loop(0, n_gz, pair, 0, unroll=2)
        for s in range(wide):
            start_y(inward, part_at, c * wide + s)

    def each_chunk(work, when, extra):
        def one(c, _):
            if extra is not None:

                @pl.when(c == when)
                def _():
                    extra()

            work(c)
            return 0

        lax.fori_loop(0, chunks, one, 0)

    ends(0)
    for h in range(1, per_dev):
        each_chunk(functools.partial(forward, h), chunks - 1, functools.partial(chain, h - 1))
        ends(h)
        solve(h - 1)
        last = functools.partial(chain, h) if h == per_dev - 1 else None
        each_chunk(functools.partial(inverse, h - 1), min(1, chunks - 1), last)
    if per_dev == 1:
        chain(0)
    solve(per_dev - 1)
    each_chunk(functools.partial(inverse, per_dev - 1), 0, None)
    part[...] = jnp.zeros_like(part)

    def put(t):
        slot = lax.rem(t, 2)
        return pltpu.make_async_copy(term_buf.at[slot], term_hbm.at[:, t], t_sem.at[slot])

    def term(t, _):
        for h in range(per_dev):
            wait_y(inward, h, t)

        def pair(p, _):
            v = field_in[t, p].astype(F32)
            a = ax_ref[p]
            lit = live_ref[p] > 0
            rel = lane_rows - a
            for h in range(2):
                base = h * B
                near = pltpu.roll(v, lax.rem(a - base + 2 * LANES, LANES), 1)
                far = pltpu.roll(v, lax.rem(a - across - base + 3 * LANES, LANES), 1)
                v_p = jnp.where((rel >= 0) & (rel < B) & lit, near, 0.0)
                v_p = jnp.where((rel + across < B) & lit, far, v_p)
                scr[h, pl.ds(p, rows, stride=pitch), :] = v_p
            return 0

        lax.fori_loop(0, pairs, pair, 0, unroll=4)

        @pl.when(t >= 2)
        def _():
            put(t - 2).wait()

        slot = lax.rem(t, 2)
        for h in range(2):
            z = jnp.minimum(h * half + t, depth - 1)

            def some(i, _):
                got = []
                for k in range(block):
                    y = i * block + k
                    v = scr[h, pl.ds(pl.multiple_of(y * pitch, 8), pairs), :]
                    got.append((v * psi[h, t, y].astype(F32)).astype(BF))
                    term_buf[slot, h, y] = got[k]
                o = orb[z, pl.ds(i * block, block)].reshape(block * LANES, norb)
                part[...] += dot_nn(jnp.concatenate(got, axis=1), o)
                return 0

            lax.fori_loop(0, rows // block, some, 0)
        put(t).start()
        return 0

    lax.fori_loop(0, half, term, 0)

    def share(k):
        return remote(part.at[of(at_y(k), group)], part_in.at[k], a_out.at[k], a_in.at[k], "gy", at_y(k))

    def spread(k):
        return remote(slab_sum, slab_in.at[gz], b_out.at[k], b_in.at[k], "gz", at_z(k))

    def gather(k):
        return remote(total.at[of(gy, group)], total.at[of(gy, group)], c_out.at[k], c_in.at[k], "gy", at_y(k))

    for k in range(1, n_gy):
        share(k).start()
    own = part[of(gy, group), :]
    for k in range(1, n_gy):
        share(k).wait_recv()
        own = own + part_in[k]
    slab_sum[...] = own

    def begin(k, _):
        spread(k).start()
        return 0

    lax.fori_loop(0, n_gz - 1, begin, 0)
    slab_in[gz] = own

    def arrived(k, _):
        spread(k).wait_recv()
        return 0

    lax.fori_loop(0, n_gz - 1, arrived, 0)

    def add(i, acc):
        return acc + slab_in[i]

    total[of(gy, group), :] = lax.fori_loop(1, n_gz, add, slab_in[0])
    for k in range(1, n_gy):
        gather(k).start()
    for k in range(1, n_gy):
        gather(k).wait_recv()
    sum_ref[...] = total[...]

    def sent(t, _):
        for k in range(1, n_gy):
            for h in range(per_dev):
                across_y(outward, h, t, k).wait_send()
                across_y(inward, h, t, k).wait_send()
        return 0

    lax.fori_loop(0, half, sent, 0)

    def drained(k, _):
        for h in range(per_dev):
            give(h, k).wait_send()
            give_back(h, k).wait_send()
        spread(k).wait_send()
        return 0

    lax.fori_loop(0, n_gz - 1, drained, 0)
    for k in range(1, n_gy):
        share(k).wait_send()
        gather(k).wait_send()
    for t in range(max(half - 2, 0), half):
        put(t).wait()


def gradient_kernel(sel_ref, tiles_ref, orb_ref, term_ref, out_ref):
    _, rows, across, norb = orb_ref.shape
    step = 4 if rows % 4 == 0 else 1

    def some(i, _):
        at = pl.ds(i * step, step)
        o = orb_ref[0, at].reshape(step * across, norb)
        c = jnp.concatenate([term_ref[0, 0, i * step + k].T[:across] for k in range(step)], axis=0)
        total = dot_nn(c, sel_ref[...]) - dot_nn(o, tiles_ref[...])
        out_ref[0, at] = total.reshape(step, across, norb)
        return 0

    lax.fori_loop(0, rows // step, some, 0, unroll=2)


def tables():
    index = np.arange(1, B + 1, dtype=np.float64)
    s = np.sqrt(2.0 / (B + 1.0)) * np.sin(np.pi * index[:, None] * index[None, :] / (B + 1.0))
    eigen = 2.0 - 2.0 * np.cos(np.pi * index / (B + 1.0))
    hi = s.astype(jnp.bfloat16).astype(np.float64)
    lo = (s - hi).astype(jnp.bfloat16).astype(np.float64)
    eye = np.eye(LANES // B)
    bd = lambda m: np.kron(eye, m)
    wide = np.block([[bd(hi), bd(lo)], [bd(hi), np.zeros((LANES, LANES))]]).astype(jnp.bfloat16)
    left = np.stack([np.concatenate([hi, lo], axis=1), np.concatenate([hi, np.zeros((B, B))], axis=1)])
    cosh = 1.0 + 0.5 * (eigen[:, None] + eigen[None, :])
    r = cosh - np.sqrt(cosh * cosh - 1.0)
    g = 1.0 / ((1.0 / r - r) * (1.0 - r ** (2 * B + 2)))
    twice = lambda m: np.tile(m, (1, LANES // B)).astype(np.float32)
    return left.astype(np.float32), wide, twice(r), twice(g)


def body(orbitals, pair_list, box_anchor, pair_live):
    depth, rows, across, norb = orbitals.shape
    n_gz = lax.axis_size("gz")
    n_gy = lax.axis_size("gy")
    pairs = pair_list.shape[0]
    group = pairs // n_gy
    per_dev = group // n_gz
    extent = depth * n_gz
    half = (depth + 1) // 2
    firsts = pair_list[:, 0]
    seconds = pair_list[:, 1]
    anchors = box_anchor[firsts]
    ax = anchors[:, 2]
    mine = lax.dynamic_slice_in_dim(anchors, lax.axis_index("gy") * group, group, 0)
    owned = lax.dynamic_index_in_dim(mine.reshape(per_dev, n_gz, 3), lax.axis_index("gz"), 1, keepdims=False)
    orbs = jnp.arange(norb)
    sel = firsts[:, None] == orbs[None, :]
    hot_first = sel.astype(BF)
    hot_second = (seconds[:, None] == orbs[None, :]).astype(BF)
    hot_both = jnp.concatenate([hot_first, hot_second], axis=0)

    smem = pl.BlockSpec(memory_space=pltpu.SMEM)
    vmem = pl.BlockSpec(memory_space=pltpu.VMEM)
    hbm = pl.BlockSpec(memory_space=pl.ANY)
    left, wide, rate, gain = (jnp.asarray(m) for m in tables())
    cycle = jnp.concatenate([left, jnp.zeros((2, extent - B, LANES), F32)], axis=1)
    table = jnp.concatenate([cycle, cycle], axis=1)
    mail = pltpu.VMEM((half, pairs, rows, LANES), BF)
    mode = pltpu.VMEM((group, B, LANES), F32)
    edges = pltpu.VMEM((group, B, LANES), BF)
    owners = pltpu.VMEM((per_dev, n_gz, B, LANES), BF)
    flags = lambda *shape: pltpu.SemaphoreType.DMA(shape)
    term, summed = pl.pallas_call(
        functools.partial(exchange_kernel, n_gz, n_gy),
        out_shape=(
            jax.ShapeDtypeStruct((2, half, rows, pairs, LANES), BF),
            jax.ShapeDtypeStruct((pairs, norb), F32),
        ),
        in_specs=[smem] * 5 + [vmem] * 5 + [hbm],
        out_specs=(hbm, vmem),
        scratch_shapes=[
            pltpu.VMEM((depth, rows, LANES, norb), BF),
            pltpu.VMEM((2, half, rows, pairs, LANES), BF),
            pltpu.VMEM((2, rows * (pairs + GAP), LANES), F32),
            mail,
            mail,
            pltpu.VMEM((group, half, B, LANES), F32),
            pltpu.VMEM((B + 1, B, LANES), F32),
            mode,
            mode,
            edges,
            owners,
            owners,
            edges,
            pltpu.VMEM((n_gz, B, LANES), F32),
            mail,
            mail,
            pltpu.VMEM((2, 2, rows, pairs, LANES), BF),
            pltpu.VMEM((pairs, norb), F32),
            pltpu.VMEM((n_gy, group, norb), F32),
            pltpu.VMEM((group, norb), F32),
            pltpu.VMEM((n_gz, group, norb), F32),
            pltpu.VMEM((pairs, norb), F32),
            flags(depth),
            flags(per_dev, half, n_gy),
            flags(per_dev, half, n_gy),
            flags(per_dev, n_gz),
            flags(per_dev, n_gz),
            flags(per_dev, n_gz),
            flags(per_dev, n_gz),
            flags(per_dev, half, n_gy),
            flags(per_dev, half, n_gy),
            flags(2),
            flags(n_gy),
            flags(n_gy),
            flags(n_gz),
            flags(n_gz),
            flags(n_gy),
            flags(n_gy),
        ],
        compiler_params=pltpu.CompilerParams(
            vmem_limit_bytes=VMEM_LIMIT, collective_id=0, has_side_effects=True
        ),
        name="exchange",
    )(ax, mine[:, 1], mine[:, 0], owned[:, 0], pair_live, hot_both, table, wide, rate, gain, orbitals)
    inner = lax.dot_general(
        summed, sel.astype(F32), (((0,), (0,)), ((), ())), precision=lax.Precision.HIGHEST, preferred_element_type=F32
    )
    tiles = (inner / (float(B) ** 3 / 4.0)).astype(BF)

    plane = pl.BlockSpec((1, rows, across, norb), lambda z: (z, 0, 0, 0))
    return pl.pallas_call(
        gradient_kernel,
        grid=(depth,),
        out_shape=jax.ShapeDtypeStruct(orbitals.shape, F32),
        in_specs=[
            pl.BlockSpec((pairs, norb), lambda z: (0, 0)),
            pl.BlockSpec((norb, norb), lambda z: (0, 0)),
            plane,
            pl.BlockSpec((1, 1, rows, pairs, LANES), lambda z: (z // half, z % half, 0, 0, 0)),
        ],
        out_specs=plane,
        compiler_params=pltpu.CompilerParams(dimension_semantics=("arbitrary",), vmem_limit_bytes=VMEM_LIMIT),
        name="gradient",
    )(hot_first, tiles, orbitals, term)


def solution(mesh):
    return jax.shard_map(
        body,
        mesh=mesh,
        in_specs=(P("gz", "gy", None, None), P(), P(), P()),
        out_specs=P("gz", "gy", None, None),
        check_vma=False,
    )
```

```python
import functools

import jax
import jax.numpy as jnp
import numpy as np
from jax import lax
from jax.experimental import pallas as pl
from jax.experimental.pallas import tpu as pltpu
from jax.sharding import PartitionSpec as P

B = 64
LANES = 128
GAP = 8
MESH = pl.DeviceIdType.MESH
BF = jnp.bfloat16
F32 = jnp.float32
VMEM_LIMIT = 56 * 1024 * 1024


def dot_nt(a, b):
    return lax.dot_general(a, b, (((1,), (1,)), ((), ())), preferred_element_type=F32)


def dot_nn(a, b):
    return lax.dot_general(a, b, (((1,), (0,)), ((), ())), preferred_element_type=F32)


def dot_tn(a, b):
    return lax.dot_general(a, b, (((0,), (0,)), ((), ())), preferred_element_type=F32)


def split(a):
    hi = a.astype(BF)
    return hi, (a - hi.astype(F32)).astype(BF)


def cell_index(az, extent, z):
    a = lax.rem(z - az + 2 * extent, extent)
    live = a < B
    return jnp.where(live, a + 1, 0), jnp.where(live, B - a, 0)


def power_of(r, n):
    out = None
    while n:
        if n & 1:
            out = r if out is None else out * r
        r = r * r
        n >>= 1
    return out


def exchange_kernel(
    n_gz, n_gy, ax_ref, ay_ref, az_ref, own_ref, live_ref, hot_ref, table_ref, wide_ref, r_ref, g_ref, orb_hbm,
    term_hbm, sum_ref,
    orb, psi, scr, send, recv, d_ref, e_ref, f_ref, h_ref, pq, pq_in, edge, edge_in, keep, field, field_in,
    term_buf, part, part_in, slab_sum, slab_in, total,
    orb_sem, y_out, y_in, z_out, z_in, e_out, e_in, v_out, v_in, t_sem, a_out, a_in, b_out, b_in, c_out, c_in,
):
    depth, rows, across, norb = orb_hbm.shape
    half = psi.shape[1]
    pairs = psi.shape[3]
    group = pairs // n_gy
    per_dev = group // n_gz
    extent = depth * n_gz
    pitch = pairs + GAP
    wide = 2 if half % 2 == 0 else 1
    chunks = half // wide
    block = 8 if rows % 8 == 0 else 1
    gz = lax.axis_index("gz")
    gy = lax.axis_index("gy")
    at_y = lambda k: lax.rem(gy + k, n_gy)
    at_z = lambda k: lax.rem(gz + 1 + k, n_gz)
    from_z = lambda k: lax.rem(gz + 2 * n_gz - 1 - k, n_gz)
    lot = lambda j, h: pl.ds(pl.multiple_of(j * group + h * n_gz, n_gz), n_gz)
    of = lambda j, size: pl.ds(pl.multiple_of(j * size, size), size)

    def remote(src, dst, out_sem, in_sem, axis, index):
        return pltpu.make_async_remote_copy(
            src_ref=src, dst_ref=dst, send_sem=out_sem, recv_sem=in_sem, device_id={axis: index}, device_id_type=MESH
        )

    def fetch(z):
        return pltpu.make_async_copy(orb_hbm.at[z], orb.at[z, :, pl.ds(0, across), :], orb_sem.at[z])

    def pad_and_fetch(z, _):
        orb[z, :, across:, :] = jnp.zeros((rows, LANES - across, norb), BF)
        fetch(z).start()
        return 0

    def pad_and_fetch_both(t, _):
        pad_and_fetch(t, 0)

        @pl.when(half + t < depth)
        def _():
            pad_and_fetch(half + t, 0)

        return 0

    lax.fori_loop(0, half, pad_and_fetch_both, 0)

    barrier = pltpu.get_barrier_semaphore()
    for k in range(1, n_gy):
        pl.semaphore_signal(barrier, inc=1, device_id={"gy": at_y(k)}, device_id_type=MESH)

    def greet(k, _):
        pl.semaphore_signal(barrier, inc=1, device_id={"gz": at_z(k)}, device_id_type=MESH)
        return 0

    lax.fori_loop(0, n_gz - 1, greet, 0)

    r2 = r_ref[...] * r_ref[...]
    e_ref[0] = jnp.zeros_like(r2)

    def fill(n, power):
        power = power * r2
        e_ref[n] = 1.0 - power
        return power

    lax.fori_loop(1, B + 1, fill, jnp.ones_like(r2))

    def across_y(mail, h, t, k):
        source, target, out_sem, in_sem = mail
        j = at_y(k)
        return remote(
            source.at[t, lot(j, h)], target.at[t, lot(gy, h)], out_sem.at[h, t, k], in_sem.at[h, t, k], "gy", j
        )

    def stay_y(mail, h, t):
        source, target, _, in_sem = mail
        return pltpu.make_async_copy(source.at[t, lot(gy, h)], target.at[t, lot(gy, h)], in_sem.at[h, t, 0])

    def start_y(mail, h, t):
        for k in range(1, n_gy):
            across_y(mail, h, t, k).start()
        stay_y(mail, h, t).start()

    def wait_y(mail, h, t):
        stay_y(mail, h, t).wait()
        for k in range(1, n_gy):
            across_y(mail, h, t, k).wait_recv()

    outward = (send, recv, y_out, y_in)
    inward = (field, field_in, v_out, v_in)

    lane_rows = lax.broadcasted_iota(jnp.int32, (rows, LANES), 1)
    lane = lax.broadcasted_iota(jnp.int32, (B, LANES), 1)
    lower = lane < B

    def density(t):
        for h in range(2):
            z = jnp.minimum(h * half + t, depth - 1)

            @pl.when(h * half + t < depth)
            def _():
                fetch(z).wait()

            def some(i, carry):
                both = dot_nt(hot_ref[...], orb[z, pl.ds(i * 2, 2)].reshape(2 * LANES, norb))
                for k in range(2):
                    y = i * 2 + k
                    mine = both[:, k * LANES:(k + 1) * LANES]
                    value = mine[:pairs] * mine[pairs:] + carry
                    sent = value.astype(BF).astype(F32)
                    scr[h, pl.ds(pl.multiple_of(y * pitch, 8), pairs), :] = sent
                    psi[h, t, y] = mine[pairs:].astype(BF)
                    carry = value - sent
                return carry

            lax.fori_loop(0, rows // 2, some, jnp.zeros((pairs, LANES), F32), unroll=12)

        def pair(p, _):
            acc = jnp.zeros((rows, LANES), F32)
            a = ax_ref[p]
            for h in range(2):
                base = h * B
                x = scr[h, pl.ds(p, rows, stride=pitch), :]
                near = pltpu.roll(x, lax.rem(base - a + 2 * LANES, LANES), 1)
                far = pltpu.roll(x, lax.rem(base + across - a + 2 * LANES, LANES), 1)
                rel = lane_rows - base
                acc = jnp.where((rel >= 0) & (rel < B), jnp.where(rel < across - a, near, far), acc)
            send[t, p] = acc.astype(BF)
            return 0

        lax.fori_loop(0, pairs, pair, 0, unroll=16)
        @pl.when(t == 0)
        def _():
            pl.semaphore_wait(barrier, n_gy + n_gz - 2)

        start_y(outward, 0, t)

    def forward(part_at, c):
        for s in range(wide):
            wait_y(outward, part_at, c * wide + s)

        def pair(n, _):
            q = part_at * n_gz + n
            m = table_ref[0, pl.ds(extent - ay_ref[q], extent), :].astype(BF)
            planes = []
            for s in range(wide):
                got = [recv[c * wide + s, j * group + q].astype(F32) for j in range(n_gy)]
                planes.append(jnp.concatenate(got, axis=0).astype(BF))
            y = dot_tn(m, jnp.concatenate(planes, axis=1))
            y = y[:B] + y[B:]
            hi, lo = split(jnp.concatenate([y[:, s * LANES:(s + 1) * LANES] for s in range(wide)], axis=0))
            x = dot_nn(jnp.concatenate([hi, lo], axis=1), wide_ref[...])
            x = x[:, :LANES] + x[:, LANES:]
            for s in range(wide):
                d_ref[q, c * wide + s] = x[s * B:(s + 1) * B] * g_ref[...]
            return 0

        lax.fori_loop(0, n_gz, pair, 0, unroll=8)

    def stage(c, _):
        @pl.when(c < chunks)
        def _():
            def one(s, _):
                density(c * wide + s)
                return 0

            lax.fori_loop(0, wide, one, 0)

        @pl.when(c == chunks)
        def _():
            def rest(t, _):
                for h in range(1, per_dev):
                    start_y(outward, h, t)
                return 0

            lax.fori_loop(0, half, rest, 0)

        @pl.when(c >= 1)
        def _():
            forward(0, c - 1)

        return 0

    lax.fori_loop(0, chunks + 1, stage, 0)

    def weights(q):
        az = az_ref[q]
        out = []
        for t in range(half):
            lu, lw = cell_index(az, extent, gz * depth + t)
            hu, hw = cell_index(az, extent, gz * depth + half + t)
            if half + t >= depth:
                hu, hw = 0, 0
            out.append((jnp.where(lower, e_ref[lu], e_ref[hu]), jnp.where(lower, e_ref[lw], e_ref[hw])))
        return out

    def rate(r, t):
        return r if half + t < depth else jnp.where(lower, r, 1.0)

    def give(h, k):
        j = at_z(k)
        return remote(pq.at[h * n_gz + j], pq_in.at[h, gz], z_out.at[h, k], z_in.at[h, k], "gz", j)

    def give_back(h, k):
        j = at_z(k)
        return remote(edge.at[h, j], edge_in.at[h * n_gz + gz], e_out.at[h, k], e_in.at[h, k], "gz", j)

    def keep_own(h):
        return pltpu.make_async_copy(pq.at[h * n_gz + gz], pq_in.at[h, gz], z_in.at[h, n_gz - 1])

    def keep_edge(h):
        return pltpu.make_async_copy(edge.at[h, gz], edge_in.at[h * n_gz + gz], e_in.at[h, n_gz - 1])

    def ends(h):
        def one(k, _):
            q = h * n_gz + at_z(k)
            r = r_ref[...]
            at = weights(q)
            d = [d_ref[q, t] for t in range(half)]
            f = at[0][0] * d[0]
            for t in range(1, half):
                f = rate(r, t) * f + at[t][0] * d[t]
            b = r * (at[half - 1][1] * d[half - 1])
            for t in reversed(range(half - 1)):
                b = r * (b + at[t][1] * d[t])
            f_ref[q] = f
            h_ref[q] = b
            p_sum = power_of(r, depth - half) * f + pltpu.roll(f, B, 1)
            q_sum = pltpu.roll(b, B, 1) + power_of(r, half) * b
            pq[q] = jnp.where(lower, p_sum, q_sum).astype(BF)

            @pl.when(k < n_gz - 1)
            def _():
                give(h, k).start()

            return 0

        lax.fori_loop(0, n_gz, one, 0)
        keep_own(h).start()

    def chain(h):
        keep_own(h).wait()

        def taken(k, _):
            give(h, k).wait_recv()
            return 0

        lax.fori_loop(0, n_gz - 1, taken, 0)
        slab_rate = power_of(r_ref[...], depth)
        az = own_ref[h]

        def up(k, f):
            i = lax.rem(k, n_gz)
            start = lax.rem(depth * i - az + extent, extent)
            f = jnp.where(start < B, f, 0.0)
            keep[i] = f
            return pq_in[h, i].astype(F32) + slab_rate * f

        lax.fori_loop(0, 2 * n_gz, up, jnp.zeros((B, LANES), F32))

        def down(k, b):
            i = lax.rem(2 * n_gz - k, n_gz)
            end = lax.rem(depth * i + depth - 1 - az + extent, extent)
            b = jnp.where(end < B, b, 0.0)
            edge[h, i] = jnp.where(lower, keep[i], b).astype(BF)
            return pq_in[h, i].astype(F32) + slab_rate * b

        lax.fori_loop(0, 2 * n_gz, down, jnp.zeros((B, LANES), F32))

        def back(k, _):
            give_back(h, k).start()
            return 0

        lax.fori_loop(0, n_gz - 1, back, 0)
        keep_edge(h).start()

    def solve(h):
        keep_edge(h).wait()

        def one(k, _):
            q = h * n_gz + from_z(k)

            @pl.when(k < n_gz - 1)
            def _():
                give_back(h, k).wait_recv()

            r = r_ref[...]
            at = weights(q)
            came = edge_in[q].astype(F32)
            swap = pltpu.roll(came, B, 1)
            f = jnp.where(lower, came, power_of(r, half) * swap + pltpu.roll(f_ref[q], B, 1))
            b = jnp.where(lower, power_of(r, depth - half) * swap + pltpu.roll(h_ref[q], B, 1), came)
            d = [d_ref[q, t] for t in range(half)]
            v = []
            for t in range(half):
                f = rate(r, t) * f + at[t][0] * d[t]
                v.append(at[t][1] * f)
            for t in reversed(range(half)):
                d_ref[q, t] = v[t] + at[t][0] * b
                b = rate(r, t) * (b + at[t][1] * d[t])
            return 0

        lax.fori_loop(0, n_gz, one, 0)

    def inverse(part_at, c):
        def pair(n, _):
            q = part_at * n_gz + n
            at = pl.ds(extent - ay_ref[q], extent)
            m = jnp.concatenate([table_ref[0, at, :], table_ref[1, at, :]], axis=1).astype(BF)[:, :3 * B]
            hi, lo = split(jnp.concatenate([d_ref[q, c * wide + s] for s in range(wide)], axis=0))
            x = dot_nn(jnp.concatenate([hi, lo], axis=1), wide_ref[...])
            x = x[:, :LANES] + x[:, LANES:]
            hi, lo = split(jnp.concatenate([x[s * B:(s + 1) * B] for s in range(wide)], axis=1))
            y = dot_nn(m, jnp.concatenate([hi, hi, lo], axis=0))
            for s in range(wide):
                for j in range(n_gy):
                    out = y[j * rows:(j + 1) * rows, s * LANES:(s + 1) * LANES]
                    field[c * wide + s, j * group + q] = out.astype(BF)
            return 0

        lax.fori_loop(0, n_gz, pair, 0, unroll=8)
        for s in range(wide):
            start_y(inward, part_at, c * wide + s)

    def each_chunk(work, when, extra):
        def one(c, _):
            if extra is not None:

                @pl.when(c == when)
                def _():
                    extra()

            work(c)
            return 0

        lax.fori_loop(0, chunks, one, 0)

    ends(0)
    for h in range(1, per_dev):
        each_chunk(functools.partial(forward, h), chunks - 1, functools.partial(chain, h - 1))
        ends(h)
        solve(h - 1)
        last = functools.partial(chain, h) if h == per_dev - 1 else None
        each_chunk(functools.partial(inverse, h - 1), min(1, chunks - 1), last)
    if per_dev == 1:
        chain(0)
    solve(per_dev - 1)
    each_chunk(functools.partial(inverse, per_dev - 1), 0, None)
    part[...] = jnp.zeros_like(part)

    def put(t):
        slot = lax.rem(t, 2)
        return pltpu.make_async_copy(term_buf.at[slot], term_hbm.at[:, t], t_sem.at[slot])

    def term(t, _):
        for h in range(per_dev):
            wait_y(inward, h, t)

        def pair(p, _):
            v = field_in[t, p].astype(F32)
            a = ax_ref[p]
            lit = live_ref[p] > 0
            rel = lane_rows - a
            for h in range(2):
                base = h * B
                near = pltpu.roll(v, lax.rem(a - base + 2 * LANES, LANES), 1)
                far = pltpu.roll(v, lax.rem(a - across - base + 3 * LANES, LANES), 1)
                v_p = jnp.where((rel >= 0) & (rel < B) & lit, near, 0.0)
                v_p = jnp.where((rel + across < B) & lit, far, v_p)
                scr[h, pl.ds(p, rows, stride=pitch), :] = v_p
            return 0

        lax.fori_loop(0, pairs, pair, 0, unroll=16)

        @pl.when(t >= 2)
        def _():
            put(t - 2).wait()

        slot = lax.rem(t, 2)
        for h in range(2):
            z = jnp.minimum(h * half + t, depth - 1)

            def some(i, _):
                got = []
                for k in range(block):
                    y = i * block + k
                    v = scr[h, pl.ds(pl.multiple_of(y * pitch, 8), pairs), :]
                    got.append((v * psi[h, t, y].astype(F32)).astype(BF))
                    term_buf[slot, h, y] = got[k]
                o = orb[z, pl.ds(i * block, block)].reshape(block * LANES, norb)
                part[...] += dot_nn(jnp.concatenate(got, axis=1), o)
                return 0

            lax.fori_loop(0, rows // block, some, 0, unroll=True)
        put(t).start()
        return 0

    lax.fori_loop(0, half, term, 0)

    def share(k):
        return remote(part.at[of(at_y(k), group)], part_in.at[k], a_out.at[k], a_in.at[k], "gy", at_y(k))

    def spread(k):
        return remote(slab_sum, slab_in.at[gz], b_out.at[k], b_in.at[k], "gz", at_z(k))

    def gather(k):
        return remote(total.at[of(gy, group)], total.at[of(gy, group)], c_out.at[k], c_in.at[k], "gy", at_y(k))

    for k in range(1, n_gy):
        share(k).start()
    own = part[of(gy, group), :]
    for k in range(1, n_gy):
        share(k).wait_recv()
        own = own + part_in[k]
    slab_sum[...] = own

    def begin(k, _):
        spread(k).start()
        return 0

    lax.fori_loop(0, n_gz - 1, begin, 0)
    slab_in[gz] = own

    def arrived(k, _):
        spread(k).wait_recv()
        return 0

    lax.fori_loop(0, n_gz - 1, arrived, 0)

    def add(i, acc):
        return acc + slab_in[i]

    total[of(gy, group), :] = lax.fori_loop(1, n_gz, add, slab_in[0])
    for k in range(1, n_gy):
        gather(k).start()
    for k in range(1, n_gy):
        gather(k).wait_recv()
    sum_ref[...] = total[...]

    def sent(t, _):
        for k in range(1, n_gy):
            for h in range(per_dev):
                across_y(outward, h, t, k).wait_send()
                across_y(inward, h, t, k).wait_send()
        return 0

    lax.fori_loop(0, half, sent, 0)

    def drained(k, _):
        for h in range(per_dev):
            give(h, k).wait_send()
            give_back(h, k).wait_send()
        spread(k).wait_send()
        return 0

    lax.fori_loop(0, n_gz - 1, drained, 0)
    for k in range(1, n_gy):
        share(k).wait_send()
        gather(k).wait_send()
    for t in range(max(half - 2, 0), half):
        put(t).wait()


def gradient_kernel(sel_ref, tiles_ref, orb_ref, term_ref, out_ref):
    _, rows, across, norb = orb_ref.shape
    step = 4 if rows % 4 == 0 else 1

    def some(i, _):
        at = pl.ds(i * step, step)
        o = orb_ref[0, at].reshape(step * across, norb)
        c = jnp.concatenate([term_ref[0, 0, i * step + k].T[:across] for k in range(step)], axis=0)
        total = dot_nn(c, sel_ref[...]) - dot_nn(o, tiles_ref[...])
        out_ref[0, at] = total.reshape(step, across, norb)
        return 0

    lax.fori_loop(0, rows // step, some, 0, unroll=2)


def tables():
    index = np.arange(1, B + 1, dtype=np.float64)
    s = np.sqrt(2.0 / (B + 1.0)) * np.sin(np.pi * index[:, None] * index[None, :] / (B + 1.0))
    eigen = 2.0 - 2.0 * np.cos(np.pi * index / (B + 1.0))
    hi = s.astype(jnp.bfloat16).astype(np.float64)
    lo = (s - hi).astype(jnp.bfloat16).astype(np.float64)
    eye = np.eye(LANES // B)
    bd = lambda m: np.kron(eye, m)
    wide = np.block([[bd(hi), bd(lo)], [bd(hi), np.zeros((LANES, LANES))]]).astype(jnp.bfloat16)
    left = np.stack([np.concatenate([hi, lo], axis=1), np.concatenate([hi, np.zeros((B, B))], axis=1)])
    cosh = 1.0 + 0.5 * (eigen[:, None] + eigen[None, :])
    r = cosh - np.sqrt(cosh * cosh - 1.0)
    g = 1.0 / ((1.0 / r - r) * (1.0 - r ** (2 * B + 2)))
    twice = lambda m: np.tile(m, (1, LANES // B)).astype(np.float32)
    return left.astype(np.float32), wide, twice(r), twice(g)


def body(orbitals, pair_list, box_anchor, pair_live):
    depth, rows, across, norb = orbitals.shape
    n_gz = lax.axis_size("gz")
    n_gy = lax.axis_size("gy")
    pairs = pair_list.shape[0]
    group = pairs // n_gy
    per_dev = group // n_gz
    extent = depth * n_gz
    half = (depth + 1) // 2
    firsts = pair_list[:, 0]
    seconds = pair_list[:, 1]
    anchors = box_anchor[firsts]
    ax = anchors[:, 2]
    mine = lax.dynamic_slice_in_dim(anchors, lax.axis_index("gy") * group, group, 0)
    owned = lax.dynamic_index_in_dim(mine.reshape(per_dev, n_gz, 3), lax.axis_index("gz"), 1, keepdims=False)
    orbs = jnp.arange(norb)
    sel = firsts[:, None] == orbs[None, :]
    hot_first = sel.astype(BF)
    hot_second = (seconds[:, None] == orbs[None, :]).astype(BF)
    hot_both = jnp.concatenate([hot_first, hot_second], axis=0)

    smem = pl.BlockSpec(memory_space=pltpu.SMEM)
    vmem = pl.BlockSpec(memory_space=pltpu.VMEM)
    hbm = pl.BlockSpec(memory_space=pl.ANY)
    left, wide, rate, gain = (jnp.asarray(m) for m in tables())
    cycle = jnp.concatenate([left, jnp.zeros((2, extent - B, LANES), F32)], axis=1)
    table = jnp.concatenate([cycle, cycle], axis=1)
    mail = pltpu.VMEM((half, pairs, rows, LANES), BF)
    mode = pltpu.VMEM((group, B, LANES), F32)
    edges = pltpu.VMEM((group, B, LANES), BF)
    owners = pltpu.VMEM((per_dev, n_gz, B, LANES), BF)
    flags = lambda *shape: pltpu.SemaphoreType.DMA(shape)
    term, summed = pl.pallas_call(
        functools.partial(exchange_kernel, n_gz, n_gy),
        out_shape=(
            jax.ShapeDtypeStruct((2, half, rows, pairs, LANES), BF),
            jax.ShapeDtypeStruct((pairs, norb), F32),
        ),
        in_specs=[smem] * 5 + [vmem] * 5 + [hbm],
        out_specs=(hbm, vmem),
        scratch_shapes=[
            pltpu.VMEM((depth, rows, LANES, norb), BF),
            pltpu.VMEM((2, half, rows, pairs, LANES), BF),
            pltpu.VMEM((2, rows * (pairs + GAP), LANES), F32),
            mail,
            mail,
            pltpu.VMEM((group, half, B, LANES), F32),
            pltpu.VMEM((B + 1, B, LANES), F32),
            mode,
            mode,
            edges,
            owners,
            owners,
            edges,
            pltpu.VMEM((n_gz, B, LANES), F32),
            mail,
            mail,
            pltpu.VMEM((2, 2, rows, pairs, LANES), BF),
            pltpu.VMEM((pairs, norb), F32),
            pltpu.VMEM((n_gy, group, norb), F32),
            pltpu.VMEM((group, norb), F32),
            pltpu.VMEM((n_gz, group, norb), F32),
            pltpu.VMEM((pairs, norb), F32),
            flags(depth),
            flags(per_dev, half, n_gy),
            flags(per_dev, half, n_gy),
            flags(per_dev, n_gz),
            flags(per_dev, n_gz),
            flags(per_dev, n_gz),
            flags(per_dev, n_gz),
            flags(per_dev, half, n_gy),
            flags(per_dev, half, n_gy),
            flags(2),
            flags(n_gy),
            flags(n_gy),
            flags(n_gz),
            flags(n_gz),
            flags(n_gy),
            flags(n_gy),
        ],
        compiler_params=pltpu.CompilerParams(
            vmem_limit_bytes=VMEM_LIMIT, collective_id=0, has_side_effects=True
        ),
        name="exchange",
    )(ax, mine[:, 1], mine[:, 0], owned[:, 0], pair_live, hot_both, table, wide, rate, gain, orbitals)
    inner = lax.dot_general(
        summed, sel.astype(F32), (((0,), (0,)), ((), ())), precision=lax.Precision.HIGHEST, preferred_element_type=F32
    )
    tiles = (inner / (float(B) ** 3 / 4.0)).astype(BF)

    plane = pl.BlockSpec((1, rows, across, norb), lambda z: (z, 0, 0, 0))
    return pl.pallas_call(
        gradient_kernel,
        grid=(depth,),
        out_shape=jax.ShapeDtypeStruct(orbitals.shape, F32),
        in_specs=[
            pl.BlockSpec((pairs, norb), lambda z: (0, 0)),
            pl.BlockSpec((norb, norb), lambda z: (0, 0)),
            plane,
            pl.BlockSpec((1, 1, rows, pairs, LANES), lambda z: (z // half, z % half, 0, 0, 0)),
        ],
        out_specs=plane,
        compiler_params=pltpu.CompilerParams(dimension_semantics=("arbitrary",), vmem_limit_bytes=VMEM_LIMIT),
        name="gradient",
    )(hot_first, tiles, orbitals, term)


def solution(mesh):
    return jax.shard_map(
        body,
        mesh=mesh,
        in_specs=(P("gz", "gy", None, None), P(), P(), P()),
        out_specs=P("gz", "gy", None, None),
        check_vma=False,
    )
```

```python
import functools
import math

import jax
import jax.numpy as jnp
import numpy as np
from jax import lax
from jax.experimental import pallas as pl
from jax.experimental.pallas import tpu as pltpu
from jax.sharding import PartitionSpec as P

B = 64
LANES = 128
GAP = 8
MESH = pl.DeviceIdType.MESH
BF = jnp.bfloat16
F32 = jnp.float32
SPARE_VMEM = 5 * 512 * 1024
GRADIENT_VMEM = 16 * 1024 * 1024


def dot_nt(a, b):
    return lax.dot_general(a, b, (((1,), (1,)), ((), ())), preferred_element_type=F32)


def dot_nn(a, b):
    return lax.dot_general(a, b, (((1,), (0,)), ((), ())), preferred_element_type=F32)


def dot_tn(a, b):
    return lax.dot_general(a, b, (((0,), (0,)), ((), ())), preferred_element_type=F32)


def split(a):
    hi = a.astype(BF)
    return hi, (a - hi.astype(F32)).astype(BF)


def cell_index(az, extent, z):
    a = lax.rem(z - az + 2 * extent, extent)
    live = a < B
    return jnp.where(live, a + 1, 0), jnp.where(live, B - a, 0)


def power_of(r, n):
    out = None
    while n:
        if n & 1:
            out = r if out is None else out * r
        r = r * r
        n >>= 1
    return out


def exchange_kernel(
    n_gz, n_gy, list_ref, anchor_ref, live_ref, table_ref, wide_ref, r_ref, g_ref, orb_hbm,
    term_hbm, mix_ref,
    hot, hot_ref, orb, psi, scr, send, recv, d_ref, e_ref, f_ref, h_ref, pq, pq_in, edge, edge_in, keep, field, field_in,
    term_buf, part, part_in, slab_sum, slab_in, total,
    orb_sem, y_out, y_in, z_out, z_in, e_out, e_in, v_out, v_in, t_sem, a_out, a_in, b_out, b_in, c_out, c_in,
):
    depth, rows, across, norb = orb_hbm.shape
    half = psi.shape[1]
    pairs = psi.shape[3]
    group = pairs // n_gy
    per_dev = group // n_gz
    extent = depth * n_gz
    pitch = pairs + GAP
    wide = 2 if half % 2 == 0 else 1
    chunks = half // wide
    block = 8 if rows % 8 == 0 else 1
    side = max(LANES // pairs, 1) if block > 1 else 1
    gz = lax.axis_index("gz")
    gy = lax.axis_index("gy")
    at_y = lambda k: lax.rem(gy + k, n_gy)
    at_z = lambda k: lax.rem(gz + 1 + k, n_gz)
    from_z = lambda k: lax.rem(gz + 2 * n_gz - 1 - k, n_gz)
    lot = lambda j, h: pl.ds(pl.multiple_of(j * group + h * n_gz, n_gz), n_gz)
    of = lambda j, size: pl.ds(pl.multiple_of(j * size, size), size)

    def anchor(axis, p):
        return anchor_ref[axis, list_ref[0, p]]

    def start_y_of(q):
        return extent - anchor(1, gy * group + q)

    def remote(src, dst, out_sem, in_sem, axis, index):
        return pltpu.make_async_remote_copy(
            src_ref=src, dst_ref=dst, send_sem=out_sem, recv_sem=in_sem, device_id={axis: index}, device_id_type=MESH
        )

    def fetch(z):
        return pltpu.make_async_copy(orb_hbm.at[z], orb.at[z, :, pl.ds(0, across), :], orb_sem.at[z])

    def pad_and_fetch(z, _):
        orb[z, :, across:, :] = jnp.zeros((rows, LANES - across, norb), BF)
        fetch(z).start()
        return 0

    def pad_and_fetch_both(t, _):
        pad_and_fetch(t, 0)

        @pl.when(half + t < depth)
        def _():
            pad_and_fetch(half + t, 0)

        return 0

    lax.fori_loop(0, half, pad_and_fetch_both, 0)

    barrier = pltpu.get_barrier_semaphore()
    for k in range(1, n_gy):
        pl.semaphore_signal(barrier, inc=1, device_id={"gy": at_y(k)}, device_id_type=MESH)

    def greet(k, _):
        pl.semaphore_signal(barrier, inc=1, device_id={"gz": at_z(k)}, device_id_type=MESH)
        return 0

    lax.fori_loop(0, n_gz - 1, greet, 0)

    orbital = lax.broadcasted_iota(jnp.int32, (1, norb), 1)

    def mark(p, _):
        for k in range(2):
            hot[pl.ds(k * pairs + p, 1), :] = (orbital == list_ref[k, p]).astype(F32)
        return 0

    lax.fori_loop(0, pairs, mark, 0, unroll=8)
    hot_ref[...] = hot[...].astype(BF)
    r2 = r_ref[...] * r_ref[...]
    e_ref[0] = jnp.zeros_like(r2)

    def fill(n, power):
        power = power * r2
        e_ref[n] = 1.0 - power
        return power

    lax.fori_loop(1, B + 1, fill, jnp.ones_like(r2))

    def across_y(mail, h, t, k):
        source, target, out_sem, in_sem = mail
        j = at_y(k)
        return remote(
            source.at[t, lot(j, h)], target.at[t, lot(gy, h)], out_sem.at[h, t, k], in_sem.at[h, t, k], "gy", j
        )

    def stay_y(mail, h, t):
        source, target, _, in_sem = mail
        return pltpu.make_async_copy(source.at[t, lot(gy, h)], target.at[t, lot(gy, h)], in_sem.at[h, t, 0])

    def start_y(mail, h, t):
        for k in range(1, n_gy):
            across_y(mail, h, t, k).start()
        stay_y(mail, h, t).start()

    def wait_y(mail, h, t):
        stay_y(mail, h, t).wait()
        for k in range(1, n_gy):
            across_y(mail, h, t, k).wait_recv()

    outward = (send, recv, y_out, y_in)
    inward = (field, field_in, v_out, v_in)

    lane_rows = lax.broadcasted_iota(jnp.int32, (rows, LANES), 1)
    lane = lax.broadcasted_iota(jnp.int32, (B, LANES), 1)
    lower = lane < B

    def density(t):
        for h in range(2):
            z = jnp.minimum(h * half + t, depth - 1)

            @pl.when(h * half + t < depth)
            def _():
                fetch(z).wait()

            def some(i, carry):
                both = dot_nt(hot_ref[...], orb[z, pl.ds(i * 2, 2)].reshape(2 * LANES, norb))
                for k in range(2):
                    y = i * 2 + k
                    mine = both[:, k * LANES:(k + 1) * LANES]
                    value = mine[:pairs] * mine[pairs:] + carry
                    sent = value.astype(BF).astype(F32)
                    scr[h, pl.ds(pl.multiple_of(y * pitch, 8), pairs), :] = sent
                    psi[h, t, y] = mine[pairs:].astype(BF)
                    carry = value - sent
                return carry

            lax.fori_loop(0, rows // 2, some, jnp.zeros((pairs, LANES), F32), unroll=12)

        def pair(p, _):
            acc = jnp.zeros((rows, LANES), F32)
            a = anchor(2, p)
            for h in range(2):
                base = h * B
                x = scr[h, pl.ds(p, rows, stride=pitch), :]
                near = pltpu.roll(x, lax.rem(base - a + 2 * LANES, LANES), 1)
                far = pltpu.roll(x, lax.rem(base + across - a + 2 * LANES, LANES), 1)
                rel = lane_rows - base
                acc = jnp.where((rel >= 0) & (rel < B), jnp.where(rel < across - a, near, far), acc)
            send[t, p] = acc.astype(BF)
            return 0

        lax.fori_loop(0, pairs, pair, 0, unroll=16)
        @pl.when(t == 0)
        def _():
            pl.semaphore_wait(barrier, n_gy + n_gz - 2)

        start_y(outward, 0, t)

    def forward(part_at, c):
        for s in range(wide):
            wait_y(outward, part_at, c * wide + s)

        def pair(n, _):
            q = part_at * n_gz + n
            m = table_ref[0, pl.ds(start_y_of(q), extent), :].astype(BF)
            planes = []
            for s in range(wide):
                got = [recv[c * wide + s, j * group + q].astype(F32) for j in range(n_gy)]
                planes.append(jnp.concatenate(got, axis=0).astype(BF))
            y = dot_tn(m, jnp.concatenate(planes, axis=1))
            y = y[:B] + y[B:]
            hi, lo = split(jnp.concatenate([y[:, s * LANES:(s + 1) * LANES] for s in range(wide)], axis=0))
            x = dot_nn(jnp.concatenate([hi, lo], axis=1), wide_ref[...])
            x = x[:, :LANES] + x[:, LANES:]
            for s in range(wide):
                d_ref[q, c * wide + s] = x[s * B:(s + 1) * B] * g_ref[...]
            return 0

        lax.fori_loop(0, n_gz, pair, 0, unroll=8)

    def stage(c, _):
        @pl.when(c < chunks)
        def _():
            def one(s, _):
                density(c * wide + s)
                return 0

            lax.fori_loop(0, wide, one, 0)

        @pl.when(c == chunks)
        def _():
            def rest(t, _):
                for h in range(1, per_dev):
                    start_y(outward, h, t)
                return 0

            lax.fori_loop(0, half, rest, 0)

        @pl.when(c >= 1)
        def _():
            forward(0, c - 1)

        return 0

    lax.fori_loop(0, chunks + 1, stage, 0)

    def weights(q):
        az = anchor(0, gy * group + q)
        out = []
        for t in range(half):
            lu, lw = cell_index(az, extent, gz * depth + t)
            hu, hw = cell_index(az, extent, gz * depth + half + t)
            if half + t >= depth:
                hu, hw = 0, 0
            out.append((jnp.where(lower, e_ref[lu], e_ref[hu]), jnp.where(lower, e_ref[lw], e_ref[hw])))
        return out

    def rate(r, t):
        return r if half + t < depth else jnp.where(lower, r, 1.0)

    def give(h, k):
        j = at_z(k)
        return remote(pq.at[h * n_gz + j], pq_in.at[h, gz], z_out.at[h, k], z_in.at[h, k], "gz", j)

    def give_back(h, k):
        j = at_z(k)
        return remote(edge.at[h, j], edge_in.at[h * n_gz + gz], e_out.at[h, k], e_in.at[h, k], "gz", j)

    def keep_own(h):
        return pltpu.make_async_copy(pq.at[h * n_gz + gz], pq_in.at[h, gz], z_in.at[h, n_gz - 1])

    def keep_edge(h):
        return pltpu.make_async_copy(edge.at[h, gz], edge_in.at[h * n_gz + gz], e_in.at[h, n_gz - 1])

    def ends(h):
        def one(k, _):
            q = h * n_gz + at_z(k)
            r = r_ref[...]
            at = weights(q)
            d = [d_ref[q, t] for t in range(half)]
            f = at[0][0] * d[0]
            for t in range(1, half):
                f = rate(r, t) * f + at[t][0] * d[t]
            b = r * (at[half - 1][1] * d[half - 1])
            for t in reversed(range(half - 1)):
                b = r * (b + at[t][1] * d[t])
            f_ref[q] = f
            h_ref[q] = b
            p_sum = power_of(r, depth - half) * f + pltpu.roll(f, B, 1)
            q_sum = pltpu.roll(b, B, 1) + power_of(r, half) * b
            pq[q] = jnp.where(lower, p_sum, q_sum).astype(BF)

            @pl.when(k < n_gz - 1)
            def _():
                give(h, k).start()

            return 0

        lax.fori_loop(0, n_gz, one, 0)
        keep_own(h).start()

    def chain(h):
        keep_own(h).wait()

        def taken(k, _):
            give(h, k).wait_recv()
            return 0

        lax.fori_loop(0, n_gz - 1, taken, 0)
        slab_rate = power_of(r_ref[...], depth)
        az = anchor(0, gy * group + h * n_gz + gz)

        def up(k, f):
            i = lax.rem(k, n_gz)
            start = lax.rem(depth * i - az + extent, extent)
            f = jnp.where(start < B, f, 0.0)
            keep[i] = f
            return pq_in[h, i].astype(F32) + slab_rate * f

        lax.fori_loop(0, 2 * n_gz, up, jnp.zeros((B, LANES), F32))

        def down(k, b):
            i = lax.rem(2 * n_gz - k, n_gz)
            end = lax.rem(depth * i + depth - 1 - az + extent, extent)
            b = jnp.where(end < B, b, 0.0)
            edge[h, i] = jnp.where(lower, keep[i], b).astype(BF)
            return pq_in[h, i].astype(F32) + slab_rate * b

        lax.fori_loop(0, 2 * n_gz, down, jnp.zeros((B, LANES), F32))

        def back(k, _):
            give_back(h, k).start()
            return 0

        lax.fori_loop(0, n_gz - 1, back, 0)
        keep_edge(h).start()

    def solve(h):
        keep_edge(h).wait()

        def one(k, _):
            q = h * n_gz + from_z(k)

            @pl.when(k < n_gz - 1)
            def _():
                give_back(h, k).wait_recv()

            r = r_ref[...]
            at = weights(q)
            came = edge_in[q].astype(F32)
            swap = pltpu.roll(came, B, 1)
            f = jnp.where(lower, came, power_of(r, half) * swap + pltpu.roll(f_ref[q], B, 1))
            b = jnp.where(lower, power_of(r, depth - half) * swap + pltpu.roll(h_ref[q], B, 1), came)
            d = [d_ref[q, t] for t in range(half)]
            v = []
            for t in range(half):
                f = rate(r, t) * f + at[t][0] * d[t]
                v.append(at[t][1] * f)
            for t in reversed(range(half)):
                d_ref[q, t] = v[t] + at[t][0] * b
                b = rate(r, t) * (b + at[t][1] * d[t])
            return 0

        lax.fori_loop(0, n_gz, one, 0)

    def inverse(part_at, c):
        def pair(n, _):
            q = part_at * n_gz + n
            at = pl.ds(start_y_of(q), extent)
            m = jnp.concatenate([table_ref[0, at, :], table_ref[1, at, :]], axis=1).astype(BF)[:, :3 * B]
            hi, lo = split(jnp.concatenate([d_ref[q, c * wide + s] for s in range(wide)], axis=0))
            x = dot_nn(jnp.concatenate([hi, lo], axis=1), wide_ref[...])
            x = x[:, :LANES] + x[:, LANES:]
            hi, lo = split(jnp.concatenate([x[s * B:(s + 1) * B] for s in range(wide)], axis=1))
            y = dot_nn(m, jnp.concatenate([hi, hi, lo], axis=0))
            for s in range(wide):
                for j in range(n_gy):
                    out = y[j * rows:(j + 1) * rows, s * LANES:(s + 1) * LANES]
                    field[c * wide + s, j * group + q] = out.astype(BF)
            return 0

        lax.fori_loop(0, n_gz, pair, 0, unroll=8)
        for s in range(wide):
            start_y(inward, part_at, c * wide + s)

    def each(first, last, work):
        def one(c, _):
            work(c)
            return 0

        lax.fori_loop(first, last, one, 0)

    ends(0)
    for h in range(1, per_dev):
        ahead = functools.partial(inverse, h - 1)

        def pull(c, h=h, ahead=ahead):
            @pl.when(c == chunks - 1)
            def _():
                solve(h - 1)
                ahead(0)

            forward(h, c)

            @pl.when(c == 0)
            def _():
                chain(h - 1)

        if chunks > 1:
            each(0, chunks, pull)
            ends(h)
            each(1, chunks, ahead)
        else:
            forward(h, 0)
            chain(h - 1)
            ends(h)
            solve(h - 1)
            ahead(0)
    chain(per_dev - 1)
    solve(per_dev - 1)
    each(0, chunks, functools.partial(inverse, per_dev - 1))
    part[...] = jnp.zeros_like(part)

    def put(t):
        slot = lax.rem(t, 2)
        return pltpu.make_async_copy(term_buf.at[slot], term_hbm.at[:, t], t_sem.at[slot])

    def term(t, _):
        for h in range(per_dev):
            wait_y(inward, h, t)

        def pair(p, _):
            v = field_in[t, p].astype(F32)
            a = anchor(2, p)
            lit = live_ref[p] > 0
            rel = lane_rows - a
            for h in range(2):
                base = h * B
                near = pltpu.roll(v, lax.rem(a - base + 2 * LANES, LANES), 1)
                far = pltpu.roll(v, lax.rem(a - across - base + 3 * LANES, LANES), 1)
                v_p = jnp.where((rel >= 0) & (rel < B) & lit, near, 0.0)
                v_p = jnp.where((rel + across < B) & lit, far, v_p)
                scr[h, pl.ds(p, rows, stride=pitch), :] = v_p
            return 0

        lax.fori_loop(0, pairs, pair, 0, unroll=16)

        @pl.when(t >= 2)
        def _():
            put(t - 2).wait()

        slot = lax.rem(t, 2)
        for h in range(2):
            z = jnp.minimum(h * half + t, depth - 1)

            def some(i, _):
                got = []
                for k in range(block):
                    y = i * block + k
                    v = scr[h, pl.ds(pl.multiple_of(y * pitch, 8), pairs), :]
                    got.append((v * psi[h, t, y].astype(F32)).astype(BF))
                for k in range(0, block, side):
                    turned = jnp.concatenate(got[k:k + side], axis=0).T
                    term_buf[slot, h, i * (block // side) + k // side] = turned[:across]
                o = orb[z, pl.ds(i * block, block)].reshape(block * LANES, norb)
                part[...] += dot_nn(jnp.concatenate(got, axis=1), o)
                return 0

            lax.fori_loop(0, rows // block, some, 0, unroll=True)
        put(t).start()
        return 0

    lax.fori_loop(0, half, term, 0)

    def share(k):
        return remote(part.at[of(at_y(k), group)], part_in.at[k], a_out.at[k], a_in.at[k], "gy", at_y(k))

    def spread(k):
        return remote(slab_sum, slab_in.at[gz], b_out.at[k], b_in.at[k], "gz", at_z(k))

    def gather(k):
        return remote(total.at[of(gy, group)], total.at[of(gy, group)], c_out.at[k], c_in.at[k], "gy", at_y(k))

    for k in range(1, n_gy):
        share(k).start()
    own = part[of(gy, group), :]
    for k in range(1, n_gy):
        share(k).wait_recv()
        own = own + part_in[k]
    slab_sum[...] = own

    def begin(k, _):
        spread(k).start()
        return 0

    lax.fori_loop(0, n_gz - 1, begin, 0)
    slab_in[gz] = own

    def arrived(k, _):
        spread(k).wait_recv()
        return 0

    lax.fori_loop(0, n_gz - 1, arrived, 0)

    def add(i, acc):
        return acc + slab_in[i]

    total[of(gy, group), :] = lax.fori_loop(1, n_gz, add, slab_in[0])
    for k in range(1, n_gy):
        gather(k).start()
    for k in range(1, n_gy):
        gather(k).wait_recv()
    high, low = split(total[...])
    rest = (total[...] - high.astype(F32) - low.astype(F32)).astype(BF)
    sel = hot_ref[:pairs]
    inner = dot_tn(jnp.concatenate([high, low, rest], axis=0), jnp.concatenate([sel, sel, sel], axis=0))
    mix_ref[:norb] = -(inner / (float(B) ** 3 / 4.0)).astype(BF)
    for k in range(side):
        mix_ref[norb + k * pairs:norb + (k + 1) * pairs] = sel

    def sent(t, _):
        for k in range(1, n_gy):
            for h in range(per_dev):
                across_y(outward, h, t, k).wait_send()
                across_y(inward, h, t, k).wait_send()
        return 0

    lax.fori_loop(0, half, sent, 0)

    def drained(k, _):
        for h in range(per_dev):
            give(h, k).wait_send()
            give_back(h, k).wait_send()
        spread(k).wait_send()
        return 0

    lax.fori_loop(0, n_gz - 1, drained, 0)
    for k in range(1, n_gy):
        share(k).wait_send()
        gather(k).wait_send()
    for t in range(max(half - 2, 0), half):
        put(t).wait()


def gradient_kernel(side, mix_ref, orb_ref, term_ref, out_ref):
    _, rows, across, norb = orb_ref.shape
    pairs = term_ref.shape[-1] // side
    lane = lax.broadcasted_iota(jnp.int32, (across, side * pairs), 1)
    held = []
    for y in range(rows):
        c = term_ref[0, 0, y // side]
        if side > 1:
            k = y % side
            c = jnp.where((lane >= k * pairs) & (lane < (k + 1) * pairs), c, jnp.zeros_like(c))
        held.append(c)
    o = orb_ref[0].reshape(rows * across, norb)
    out = dot_nn(jnp.concatenate([o, jnp.concatenate(held, axis=0)], axis=1), mix_ref[...])
    out_ref[0] = out.reshape(rows, across, norb)


def tables():
    index = np.arange(1, B + 1, dtype=np.float64)
    s = np.sqrt(2.0 / (B + 1.0)) * np.sin(np.pi * index[:, None] * index[None, :] / (B + 1.0))
    eigen = 2.0 - 2.0 * np.cos(np.pi * index / (B + 1.0))
    hi = s.astype(jnp.bfloat16).astype(np.float64)
    lo = (s - hi).astype(jnp.bfloat16).astype(np.float64)
    eye = np.eye(LANES // B)
    bd = lambda m: np.kron(eye, m)
    wide = np.block([[bd(hi), bd(lo)], [bd(hi), np.zeros((LANES, LANES))]]).astype(jnp.bfloat16)
    left = np.stack([np.concatenate([hi, lo], axis=1), np.concatenate([hi, np.zeros((B, B))], axis=1)])
    cosh = 1.0 + 0.5 * (eigen[:, None] + eigen[None, :])
    r = cosh - np.sqrt(cosh * cosh - 1.0)
    g = 1.0 / ((1.0 / r - r) * (1.0 - r ** (2 * B + 2)))
    twice = lambda m: np.tile(m, (1, LANES // B)).astype(np.float32)
    return left.astype(np.float32), wide, twice(r), twice(g)


def body(orbitals, pair_list, box_anchor, pair_live):
    depth, rows, across, norb = orbitals.shape
    n_gz = lax.axis_size("gz")
    n_gy = lax.axis_size("gy")
    pairs = pair_list.shape[0]
    group = pairs // n_gy
    per_dev = group // n_gz
    extent = depth * n_gz
    half = (depth + 1) // 2
    block = 8 if rows % 8 == 0 else 1
    side = max(LANES // pairs, 1) if block > 1 else 1

    smem = pl.BlockSpec(memory_space=pltpu.SMEM)
    vmem = pl.BlockSpec(memory_space=pltpu.VMEM)
    hbm = pl.BlockSpec(memory_space=pl.ANY)
    left, wide, rate, gain = (jnp.asarray(m) for m in tables())
    cycle = jnp.concatenate([left, jnp.zeros((2, extent - B, LANES), F32)], axis=1)
    table = jnp.concatenate([cycle, cycle], axis=1)
    mail = pltpu.VMEM((half, pairs, rows, LANES), BF)
    mode = pltpu.VMEM((group, B, LANES), F32)
    edges = pltpu.VMEM((group, B, LANES), BF)
    owners = pltpu.VMEM((per_dev, n_gz, B, LANES), BF)
    flags = lambda *shape: pltpu.SemaphoreType.DMA(shape)
    scratch = [
        pltpu.VMEM((2 * pairs, norb), F32),
        pltpu.VMEM((2 * pairs, norb), BF),
        pltpu.VMEM((depth, rows, LANES, norb), BF),
        pltpu.VMEM((2, half, rows, pairs, LANES), BF),
        pltpu.VMEM((2, rows * (pairs + GAP), LANES), F32),
        mail,
        mail,
        pltpu.VMEM((group, half, B, LANES), F32),
        pltpu.VMEM((B + 1, B, LANES), F32),
        mode,
        mode,
        edges,
        owners,
        owners,
        edges,
        pltpu.VMEM((n_gz, B, LANES), F32),
        mail,
        mail,
        pltpu.VMEM((2, 2, rows // side, across, side * pairs), BF),
        pltpu.VMEM((pairs, norb), F32),
        pltpu.VMEM((n_gy, group, norb), F32),
        pltpu.VMEM((group, norb), F32),
        pltpu.VMEM((n_gz, group, norb), F32),
        pltpu.VMEM((pairs, norb), F32),
    ]
    semaphores = [
        flags(depth),
        flags(per_dev, half, n_gy),
        flags(per_dev, half, n_gy),
        flags(per_dev, n_gz),
        flags(per_dev, n_gz),
        flags(per_dev, n_gz),
        flags(per_dev, n_gz),
        flags(per_dev, half, n_gy),
        flags(per_dev, half, n_gy),
        flags(2),
        flags(n_gy),
        flags(n_gy),
        flags(n_gz),
        flags(n_gz),
        flags(n_gy),
        flags(n_gy),
    ]
    held = sum(math.prod(buffer.shape) * buffer.dtype.itemsize for buffer in scratch)
    stay = lambda x: pltpu.with_memory_space_constraint(x, pltpu.HBM)
    term, mix = pl.pallas_call(
        functools.partial(exchange_kernel, n_gz, n_gy),
        out_shape=(
            jax.ShapeDtypeStruct((2, half, rows // side, across, side * pairs), BF),
            jax.ShapeDtypeStruct((norb + side * pairs, norb), BF),
        ),
        in_specs=[smem] * 3 + [vmem] * 4 + [hbm],
        out_specs=(hbm, vmem),
        scratch_shapes=scratch + semaphores,
        compiler_params=pltpu.CompilerParams(
            vmem_limit_bytes=held + SPARE_VMEM, collective_id=0, has_side_effects=True
        ),
        name="exchange",
    )(*(stay(x) for x in (pair_list.T, box_anchor.T, pair_live, table, wide, rate, gain, orbitals)))

    plane = pl.BlockSpec((1, rows, across, norb), lambda z: (z, 0, 0, 0))
    return pl.pallas_call(
        functools.partial(gradient_kernel, side),
        grid=(depth,),
        out_shape=jax.ShapeDtypeStruct(orbitals.shape, F32),
        in_specs=[
            pl.BlockSpec((norb + side * pairs, norb), lambda z: (0, 0)),
            plane,
            pl.BlockSpec((1, 1, rows // side, across, side * pairs), lambda z: (z // half, z % half, 0, 0, 0)),
        ],
        out_specs=plane,
        compiler_params=pltpu.CompilerParams(dimension_semantics=("arbitrary",), vmem_limit_bytes=GRADIENT_VMEM),
        name="gradient",
    )(mix, orbitals, term)


def solution(mesh):
    return jax.shard_map(
        body,
        mesh=mesh,
        in_specs=(P("gz", "gy", None, None), P(), P(), P()),
        out_specs=P("gz", "gy", None, None),
        check_vma=False,
    )
```

```python
import functools
import math

import jax
import jax.numpy as jnp
import numpy as np
from jax import lax
from jax.experimental import pallas as pl
from jax.experimental.pallas import tpu as pltpu
from jax.sharding import PartitionSpec as P

B = 64
LANES = 128
GAP = 8
MESH = pl.DeviceIdType.MESH
BF = jnp.bfloat16
F32 = jnp.float32
SPARE_VMEM = 5 * 512 * 1024
GRADIENT_VMEM = 24 * 1024 * 1024


def dot_nt(a, b):
    return lax.dot_general(a, b, (((1,), (1,)), ((), ())), preferred_element_type=F32)


def dot_nn(a, b):
    return lax.dot_general(a, b, (((1,), (0,)), ((), ())), preferred_element_type=F32)


def dot_tn(a, b):
    return lax.dot_general(a, b, (((0,), (0,)), ((), ())), preferred_element_type=F32)


def split(a):
    hi = a.astype(BF)
    return hi, (a - hi.astype(F32)).astype(BF)


def cell_index(az, extent, z):
    a = lax.rem(z - az + 2 * extent, extent)
    live = a < B
    return jnp.where(live, a + 1, 0), jnp.where(live, B - a, 0)


def power_of(r, n):
    out = None
    while n:
        if n & 1:
            out = r if out is None else out * r
        r = r * r
        n >>= 1
    return out


def exchange_kernel(
    n_gz, n_gy, list_ref, anchor_ref, live_ref, table_ref, wide_ref, r_ref, g_ref, orb_hbm,
    term_hbm, mix_ref,
    hot, hot_ref, orb, psi, scr, send, recv, d_ref, e_ref, f_ref, h_ref, pq, pq_in, edge, edge_in, keep, field, field_in,
    term_buf, part, part_in, slab_sum, slab_in, total,
    orb_sem, y_out, y_in, z_out, z_in, e_out, e_in, v_out, v_in, t_sem, a_out, a_in, b_out, b_in, c_out, c_in,
):
    depth, rows, across, norb = orb_hbm.shape
    half = psi.shape[1]
    pairs = psi.shape[3]
    group = pairs // n_gy
    per_dev = group // n_gz
    extent = depth * n_gz
    pitch = pairs + GAP
    wide = 2 if half % 2 == 0 else 1
    chunks = half // wide
    block = 8 if rows % 8 == 0 else 1
    gate = min(1, half - 1)
    behind = min(2, chunks)
    gz = lax.axis_index("gz")
    gy = lax.axis_index("gy")
    at_y = lambda k: lax.rem(gy + k, n_gy)
    at_z = lambda k: lax.rem(gz + 1 + k, n_gz)
    parts = pq_in.shape[0]
    few = group // parts
    soon = half // 2
    sets = term_hbm.shape[0]
    side = term_hbm.shape[-1] * sets // pairs
    seat = group // sets
    share_of = pairs // sets
    lot = lambda j, h: pl.ds(pl.multiple_of(h * few // seat * share_of + j * seat + h * few % seat, few), few)

    def place(j, q):
        return lax.div(q, seat) * share_of + j * seat + lax.rem(q, seat)

    def pair_of(p):
        inner = lax.rem(p, share_of)
        return lax.div(inner, seat) * group + lax.div(p, share_of) * seat + lax.rem(inner, seat)

    of = lambda j, size: pl.ds(pl.multiple_of(j * size, size), size)

    def anchor(axis, p):
        return anchor_ref[axis, list_ref[0, p]]

    def start_y_of(q):
        return extent - anchor(1, gy * group + q)

    def remote(src, dst, out_sem, in_sem, axis, index):
        return pltpu.make_async_remote_copy(
            src_ref=src, dst_ref=dst, send_sem=out_sem, recv_sem=in_sem, device_id={axis: index}, device_id_type=MESH
        )

    def fetch(z):
        return pltpu.make_async_copy(orb_hbm.at[z], orb.at[z, :, pl.ds(0, across), :], orb_sem.at[z])

    def pad_and_fetch(z, _):
        orb[z, :, across:, :] = jnp.zeros((rows, LANES - across, norb), BF)
        fetch(z).start()
        return 0

    def pad_and_fetch_both(t, _):
        pad_and_fetch(t, 0)

        @pl.when(half + t < depth)
        def _():
            pad_and_fetch(half + t, 0)

        return 0

    lax.fori_loop(0, half, pad_and_fetch_both, 0)

    barrier = pltpu.get_barrier_semaphore()
    for k in range(1, n_gy):
        pl.semaphore_signal(barrier, inc=1, device_id={"gy": at_y(k)}, device_id_type=MESH)

    def greet(k, _):
        pl.semaphore_signal(barrier, inc=1, device_id={"gz": at_z(k)}, device_id_type=MESH)
        return 0

    lax.fori_loop(0, n_gz - 1, greet, 0)

    orbital = lax.broadcasted_iota(jnp.int32, (1, norb), 1)

    def mark(p, _):
        for k in range(2):
            hot[pl.ds(k * pairs + p, 1), :] = (orbital == list_ref[k, pair_of(p)]).astype(F32)
        return 0

    lax.fori_loop(0, pairs, mark, 0, unroll=8)
    hot_ref[...] = hot[...].astype(BF)
    r2 = r_ref[...] * r_ref[...]
    e_ref[0] = jnp.zeros_like(r2)

    def fill(n, power):
        power = power * r2
        e_ref[n] = 1.0 - power
        return power

    lax.fori_loop(1, B + 1, fill, jnp.ones_like(r2))

    def across_y(mail, h, t, k):
        source, target, out_sem, in_sem = mail
        j = at_y(k)
        return remote(
            source.at[t, lot(j, h)], target.at[t, lot(gy, h)], out_sem, in_sem.at[h, t], "gy", j
        )

    def stay_y(mail, h, t):
        source, target, _, in_sem = mail
        return pltpu.make_async_copy(source.at[t, lot(gy, h)], target.at[t, lot(gy, h)], in_sem.at[h, t])

    def start_y(mail, h, t):
        for k in range(1, n_gy):
            across_y(mail, h, t, k).start()
        stay_y(mail, h, t).start()

    def wait_y(mail, h, t):
        _, target, _, in_sem = mail
        every = target.at[t, pl.ds(0, n_gy * few)]
        pltpu.make_async_copy(every, every, in_sem.at[h, t]).wait()

    def sent_y(mail):
        source, target, out_sem, in_sem = mail
        every = pl.ds(0, (n_gy - 1) * group)
        remote(source.at[:, every], target.at[:, every], out_sem, in_sem.at[0, 0], "gy", at_y(1)).wait_send()

    outward = (send, recv, y_out, y_in)
    inward = (field, field_in, v_out, v_in)

    lane_rows = lax.broadcasted_iota(jnp.int32, (rows, LANES), 1)
    lane = lax.broadcasted_iota(jnp.int32, (B, LANES), 1)
    lower = lane < B

    def density(t):
        for h in range(2):
            z = jnp.minimum(h * half + t, depth - 1)

            @pl.when(h * half + t < depth)
            def _():
                fetch(z).wait()

            def some(i, carry):
                both = dot_nt(hot_ref[...], orb[z, pl.ds(i * 2, 2)].reshape(2 * LANES, norb))
                for k in range(2):
                    y = i * 2 + k
                    mine = both[:, k * LANES:(k + 1) * LANES]
                    value = mine[:pairs] * mine[pairs:] + carry
                    sent = value.astype(BF).astype(F32)
                    scr[h, pl.ds(pl.multiple_of(y * pitch, 8), pairs), :] = sent
                    psi[h, t, y] = mine[pairs:].astype(BF)
                    carry = value - sent
                return carry

            lax.fori_loop(0, rows // 2, some, jnp.zeros((pairs, LANES), F32), unroll=12)

        def pair(p, _):
            acc = jnp.zeros((rows, LANES), F32)
            a = anchor(2, pair_of(p))
            for h in range(2):
                base = h * B
                x = scr[h, pl.ds(p, rows, stride=pitch), :]
                near = pltpu.roll(x, lax.rem(base - a + 2 * LANES, LANES), 1)
                far = pltpu.roll(x, lax.rem(base + across - a + 2 * LANES, LANES), 1)
                rel = lane_rows - base
                acc = jnp.where((rel >= 0) & (rel < B), jnp.where(rel < across - a, near, far), acc)
            send[t, p] = acc.astype(BF)
            return 0

        lax.fori_loop(0, pairs, pair, 0, unroll=16)
        @pl.when(t == gate)
        def _():
            pl.semaphore_wait(barrier, n_gy + n_gz - 2)
            for early in range(gate):
                start_y(outward, 0, early)

        @pl.when(t >= gate)
        def _():
            start_y(outward, 0, t)

        if parts > 1:

            @pl.when((t >= gate) & (t - gate < soon))
            def _():
                start_y(outward, 1, t - gate)

    def advance(q, c):
        m = table_ref[0, pl.ds(start_y_of(q), extent), :].astype(BF)
        planes = []
        for s in range(wide):
            got = [recv[c * wide + s, place(j, q)].astype(F32) for j in range(n_gy)]
            planes.append(jnp.concatenate(got, axis=0).astype(BF))
        y = dot_tn(m, jnp.concatenate(planes, axis=1))
        y = y[:B] + y[B:]
        hi, lo = split(jnp.concatenate([y[:, s * LANES:(s + 1) * LANES] for s in range(wide)], axis=0))
        x = dot_nn(jnp.concatenate([hi, lo], axis=1), wide_ref[...])
        x = x[:, :LANES] + x[:, LANES:]
        for s in range(wide):
            d_ref[q, c * wide + s] = x[s * B:(s + 1) * B] * g_ref[...]

    def forward(part_at, first, count):
        for s in range(count * wide):
            wait_y(outward, part_at, first * wide + s)

        def one(i, _):
            advance(part_at * few + lax.rem(i, few), first + lax.div(i, few))
            return 0

        lax.fori_loop(0, few * count, one, 0, unroll=min(8, few * count))

    def stage(c, _):
        @pl.when(c < chunks)
        def _():
            def one(s, _):
                density(c * wide + s)
                return 0

            lax.fori_loop(0, wide, one, 0)

        @pl.when(c == chunks)
        def _():
            for h in range(1, parts):

                def rest(t, _, h=h):
                    start_y(outward, h, t)
                    return 0

                lax.fori_loop(soon if h == 1 else 0, half, rest, 0)

        @pl.when(c >= behind)
        def _():
            forward(0, c - behind, 1)

        return 0

    lax.fori_loop(0, chunks + behind, stage, 0)

    def weights(q):
        az = anchor(0, gy * group + q)
        out = []
        for t in range(half):
            lu, lw = cell_index(az, extent, gz * depth + t)
            hu, hw = cell_index(az, extent, gz * depth + half + t)
            if half + t >= depth:
                hu, hw = 0, 0
            out.append((jnp.where(lower, e_ref[lu], e_ref[hu]), jnp.where(lower, e_ref[lw], e_ref[hw])))
        return out

    def rate(r, t):
        return r if half + t < depth else jnp.where(lower, r, 1.0)

    def give(h, q):
        j = lax.rem(q, n_gz)
        return remote(pq.at[q], pq_in.at[h, gz], z_out, z_in.at[h], "gz", j)

    def keep_own(h, q):
        return pltpu.make_async_copy(pq.at[q], pq_in.at[h, gz], z_in.at[h])

    def own_at(h):
        return h * few + gz - h * few % n_gz

    def give_back(h, k):
        j = at_z(k)
        return remote(edge.at[h, j], edge_in.at[own_at(h)], e_out, e_in.at[h], "gz", j)

    def keep_edge(h):
        return pltpu.make_async_copy(edge.at[h, gz], edge_in.at[own_at(h)], e_in.at[h])

    def ends(h):
        def one(k, _):
            q = h * few + lax.rem(gz + 1 + k, few)
            r = r_ref[...]
            at = weights(q)
            d = [d_ref[q, t] for t in range(half)]
            f = at[0][0] * d[0]
            for t in range(1, half):
                f = rate(r, t) * f + at[t][0] * d[t]
            b = r * (at[half - 1][1] * d[half - 1])
            for t in reversed(range(half - 1)):
                b = r * (b + at[t][1] * d[t])
            f_ref[q] = f
            h_ref[q] = b
            p_sum = power_of(r, depth - half) * f + pltpu.roll(f, B, 1)
            q_sum = pltpu.roll(b, B, 1) + power_of(r, half) * b
            pq[q] = jnp.where(lower, p_sum, q_sum).astype(BF)
            away = lax.rem(q, n_gz) != gz

            @pl.when(away)
            def _():
                give(h, q).start()

            @pl.when(jnp.logical_not(away))
            def _():
                keep_own(h, q).start()

            return 0

        lax.fori_loop(0, few, one, 0)

    def chain(h):
        first = h * few % n_gz

        @pl.when((gz >= first) & (gz < first + few))
        def _():
            pltpu.make_async_copy(pq_in.at[h], pq_in.at[h], z_in.at[h]).wait()
            slab_rate = power_of(r_ref[...], depth)
            az = anchor(0, gy * group + own_at(h))

            def up(k, f):
                i = lax.rem(k, n_gz)
                start = lax.rem(depth * i - az + extent, extent)
                f = jnp.where(start < B, f, 0.0)
                keep[i] = f
                return pq_in[h, i].astype(F32) + slab_rate * f

            lax.fori_loop(0, 2 * n_gz, up, jnp.zeros((B, LANES), F32))

            def down(k, b):
                i = lax.rem(2 * n_gz - k, n_gz)
                end = lax.rem(depth * i + depth - 1 - az + extent, extent)
                b = jnp.where(end < B, b, 0.0)
                edge[h, i] = jnp.where(lower, keep[i], b).astype(BF)
                return pq_in[h, i].astype(F32) + slab_rate * b

            lax.fori_loop(0, 2 * n_gz, down, jnp.zeros((B, LANES), F32))

            def back(k, _):
                give_back(h, k).start()
                return 0

            lax.fori_loop(0, n_gz - 1, back, 0)
            keep_edge(h).start()

    def solve(h):
        every = edge_in.at[pl.ds(h * few, few)]
        pltpu.make_async_copy(every, every, e_in.at[h]).wait()

        def one(k, _):
            q = h * few + k
            r = r_ref[...]
            at = weights(q)
            came = edge_in[q].astype(F32)
            swap = pltpu.roll(came, B, 1)
            f = jnp.where(lower, came, power_of(r, half) * swap + pltpu.roll(f_ref[q], B, 1))
            b = jnp.where(lower, power_of(r, depth - half) * swap + pltpu.roll(h_ref[q], B, 1), came)
            d = [d_ref[q, t] for t in range(half)]
            v = []
            for t in range(half):
                f = rate(r, t) * f + at[t][0] * d[t]
                v.append(at[t][1] * f)
            for t in reversed(range(half)):
                d_ref[q, t] = v[t] + at[t][0] * b
                b = rate(r, t) * (b + at[t][1] * d[t])
            return 0

        lax.fori_loop(0, few, one, 0)

    def inverse(part_at, c):
        def pair(n, _):
            q = part_at * few + n
            at = pl.ds(start_y_of(q), extent)
            m = jnp.concatenate([table_ref[0, at, :], table_ref[1, at, :]], axis=1).astype(BF)[:, :3 * B]
            hi, lo = split(jnp.concatenate([d_ref[q, c * wide + s] for s in range(wide)], axis=0))
            x = dot_nn(jnp.concatenate([hi, lo], axis=1), wide_ref[...])
            x = x[:, :LANES] + x[:, LANES:]
            hi, lo = split(jnp.concatenate([x[s * B:(s + 1) * B] for s in range(wide)], axis=1))
            y = dot_nn(m, jnp.concatenate([hi, hi, lo], axis=0))
            for s in range(wide):
                for j in range(n_gy):
                    out = y[j * rows:(j + 1) * rows, s * LANES:(s + 1) * LANES]
                    field[c * wide + s, place(j, q)] = out.astype(BF)
            return 0

        lax.fori_loop(0, few, pair, 0, unroll=min(8, few))
        for s in range(wide):
            start_y(inward, part_at, c * wide + s)

    def finish(h):
        solve(h)

        def one(c, _):
            inverse(h, c)
            return 0

        lax.fori_loop(0, chunks, one, 0)

    part[...] = jnp.zeros_like(part)

    def put(i):
        slot = lax.rem(i, 2)
        return pltpu.make_async_copy(
            term_buf.at[slot], term_hbm.at[lax.div(i, half), :, lax.rem(i, half)], t_sem.at[slot]
        )

    def term(e, t):
        for h in range(e * parts // sets, (e + 1) * parts // sets):
            wait_y(inward, h, t)
        turn = e * half + t

        def pair(p, _):
            v = field_in[t, p].astype(F32)
            a = anchor(2, pair_of(p))
            lit = live_ref[pair_of(p)] > 0
            rel = lane_rows - a
            for h in range(2):
                base = h * B
                near = pltpu.roll(v, lax.rem(a - base + 2 * LANES, LANES), 1)
                far = pltpu.roll(v, lax.rem(a - across - base + 3 * LANES, LANES), 1)
                v_p = jnp.where((rel >= 0) & (rel < B) & lit, near, 0.0)
                v_p = jnp.where((rel + across < B) & lit, far, v_p)
                scr[h, pl.ds(p, rows, stride=pitch), :] = v_p
            return 0

        lax.fori_loop(e * share_of, (e + 1) * share_of, pair, 0, unroll=16)

        @pl.when(turn >= 2)
        def _():
            put(turn - 2).wait()

        slot = lax.rem(turn, 2)
        mine = pl.ds(e * share_of, share_of)
        for h in range(2):
            z = jnp.minimum(h * half + t, depth - 1)

            def some(i, _):
                got = []
                for k in range(block):
                    y = i * block + k
                    v = scr[h, pl.ds(pl.multiple_of(y * pitch + e * share_of, 8), share_of), :]
                    got.append((v * psi[h, t, y, mine].astype(F32)).astype(BF))
                for k in range(0, block, side):
                    turned = jnp.concatenate(got[k:k + side], axis=0).T
                    term_buf[slot, h, i * (block // side) + k // side] = turned[:across]
                o = orb[z, pl.ds(i * block, block)].reshape(block * LANES, norb)
                part[mine] += dot_nn(jnp.concatenate(got, axis=1), o)
                return 0

            lax.fori_loop(0, rows // block, some, 0, unroll=True)
        put(turn).start()

    def terms(e, first, last):
        def one(t, _):
            term(e, t)
            return 0

        lax.fori_loop(first, last, one, 0)

    early_terms = half // 3 if sets > 1 and parts > 2 else 0
    ends(0)
    for h in range(1, parts):
        forward(h, 0, chunks)
        ends(h)
        chain(h - 1)
        if h >= 2:
            finish(h - 2)
    chain(parts - 1)
    if parts > 1:
        finish(parts - 2)
    terms(0, 0, early_terms)
    finish(parts - 1)
    terms(0, early_terms, half)
    for e in range(1, sets):
        terms(e, 0, half)

    def share(k):
        return remote(part.at[of(at_y(k), group)], part_in.at[k], a_out, a_in, "gy", at_y(k))

    def spread(k):
        return remote(slab_sum, slab_in.at[gz], b_out, b_in, "gz", at_z(k))

    def gather(k):
        return remote(total.at[of(gy, group)], total.at[of(gy, group)], c_out, c_in, "gy", at_y(k))

    for k in range(1, n_gy):
        share(k).start()
    own = part[of(gy, group), :]
    others = part_in.at[pl.ds(1, n_gy - 1)]
    pltpu.make_async_copy(others, others, a_in).wait()
    for k in range(1, n_gy):
        own = own + part_in[k]
    slab_sum[...] = own

    def begin(k, _):
        spread(k).start()
        return 0

    lax.fori_loop(0, n_gz - 1, begin, 0)
    slab_in[gz] = own

    others = slab_in.at[pl.ds(0, n_gz - 1)]
    pltpu.make_async_copy(others, others, b_in).wait()

    def add(i, acc):
        return acc + slab_in[i]

    total[of(gy, group), :] = lax.fori_loop(1, n_gz, add, slab_in[0])
    for k in range(1, n_gy):
        gather(k).start()
    others = total.at[pl.ds(0, (n_gy - 1) * group)]
    pltpu.make_async_copy(others, others, c_in).wait()
    high, low = split(total[...])
    rest = (total[...] - high.astype(F32) - low.astype(F32)).astype(BF)
    sel = hot_ref[:pairs]
    inner = dot_tn(jnp.concatenate([high, low, rest], axis=0), jnp.concatenate([sel, sel, sel], axis=0))
    mix_ref[:norb] = -(inner / (float(B) ** 3 / 4.0)).astype(BF)
    for e in range(sets):
        for k in range(side):
            at = norb + (e * side + k) * share_of
            mix_ref[at:at + share_of] = sel[e * share_of:(e + 1) * share_of]

    sent_y(outward)
    sent_y(inward)
    given = pl.ds(0, per_dev * (n_gz - 1))
    remote(pq.at[given], edge_in.at[given], z_out, z_in.at[0], "gz", at_z(0)).wait_send()
    remote(pq.at[given], edge_in.at[given], e_out, e_in.at[0], "gz", at_z(0)).wait_send()
    spare = part_in.at[pl.ds(1, n_gy - 1)]
    remote(spare, spare, a_out, a_in, "gy", at_y(1)).wait_send()
    remote(spare, spare, c_out, c_in, "gy", at_y(1)).wait_send()
    spare = slab_in.at[pl.ds(0, n_gz - 1)]
    remote(spare, spare, b_out, b_in, "gz", at_z(0)).wait_send()
    for turn in range(max(sets * half - 2, 0), sets * half):
        put(turn).wait()


def gradient_kernel(side, mix_ref, orb_ref, term_ref, out_ref):
    lump, rows, across, norb = orb_ref.shape
    sets = term_ref.shape[0]
    share_of = term_ref.shape[-1] // side
    lane = lax.broadcasted_iota(jnp.int32, (across, side * share_of), 1)

    def plane(z, _):
        held = [[] for _ in range(sets)]
        for y in range(rows):
            for e in range(sets):
                c = term_ref[e, 0, z, y // side]
                if side > 1:
                    k = y % side
                    c = jnp.where((lane >= k * share_of) & (lane < (k + 1) * share_of), c, jnp.zeros_like(c))
                held[e].append(c)
        o = orb_ref[z].reshape(rows * across, norb)
        columns = [o] + [jnp.concatenate(h, axis=0) for h in held]
        out = dot_nn(jnp.concatenate(columns, axis=1), mix_ref[...])
        out_ref[z] = out.reshape(rows, across, norb)
        return 0

    lax.fori_loop(0, lump, plane, 0)


def tables():
    index = np.arange(1, B + 1, dtype=np.float64)
    s = np.sqrt(2.0 / (B + 1.0)) * np.sin(np.pi * index[:, None] * index[None, :] / (B + 1.0))
    eigen = 2.0 - 2.0 * np.cos(np.pi * index / (B + 1.0))
    hi = s.astype(jnp.bfloat16).astype(np.float64)
    lo = (s - hi).astype(jnp.bfloat16).astype(np.float64)
    eye = np.eye(LANES // B)
    bd = lambda m: np.kron(eye, m)
    wide = np.block([[bd(hi), bd(lo)], [bd(hi), np.zeros((LANES, LANES))]]).astype(jnp.bfloat16)
    left = np.stack([np.concatenate([hi, lo], axis=1), np.concatenate([hi, np.zeros((B, B))], axis=1)])
    cosh = 1.0 + 0.5 * (eigen[:, None] + eigen[None, :])
    r = cosh - np.sqrt(cosh * cosh - 1.0)
    g = 1.0 / ((1.0 / r - r) * (1.0 - r ** (2 * B + 2)))
    twice = lambda m: np.tile(m, (1, LANES // B)).astype(np.float32)
    return left.astype(np.float32), wide, twice(r), twice(g)


def body(orbitals, pair_list, box_anchor, pair_live):
    depth, rows, across, norb = orbitals.shape
    n_gz = lax.axis_size("gz")
    n_gy = lax.axis_size("gy")
    pairs = pair_list.shape[0]
    group = pairs // n_gy
    per_dev = group // n_gz
    extent = depth * n_gz
    half = (depth + 1) // 2
    block = 8 if rows % 8 == 0 else 1
    sets = 2 if per_dev * (2 if n_gz % 2 == 0 else 1) % 2 == 0 else 1
    side = max(LANES * sets // pairs, 1) if block > 1 else 1
    columns = side * pairs // sets

    smem = pl.BlockSpec(memory_space=pltpu.SMEM)
    vmem = pl.BlockSpec(memory_space=pltpu.VMEM)
    hbm = pl.BlockSpec(memory_space=pl.ANY)
    left, wide, rate, gain = (jnp.asarray(m) for m in tables())
    cycle = jnp.concatenate([left, jnp.zeros((2, extent - B, LANES), F32)], axis=1)
    table = jnp.concatenate([cycle, cycle], axis=1)
    mail = pltpu.VMEM((half, pairs, rows, LANES), BF)
    mode = pltpu.VMEM((group, B, LANES), F32)
    edges = pltpu.VMEM((group, B, LANES), BF)
    parts = per_dev * (2 if n_gz % 2 == 0 else 1)
    owners = pltpu.VMEM((parts, n_gz, B, LANES), BF)
    flags = lambda *shape: pltpu.SemaphoreType.DMA(shape)
    one = pltpu.SemaphoreType.DMA
    scratch = [
        pltpu.VMEM((2 * pairs, norb), F32),
        pltpu.VMEM((2 * pairs, norb), BF),
        pltpu.VMEM((depth, rows, LANES, norb), BF),
        pltpu.VMEM((2, half, rows, pairs, LANES), BF),
        pltpu.VMEM((2, rows * (pairs + GAP), LANES), F32),
        mail,
        mail,
        pltpu.VMEM((group, half, B, LANES), F32),
        pltpu.VMEM((B + 1, B, LANES), F32),
        mode,
        mode,
        edges,
        owners,
        owners,
        edges,
        pltpu.VMEM((n_gz, B, LANES), F32),
        mail,
        mail,
        pltpu.VMEM((2, 2, rows // side, across, columns), BF),
        pltpu.VMEM((pairs, norb), F32),
        pltpu.VMEM((n_gy, group, norb), F32),
        pltpu.VMEM((group, norb), F32),
        pltpu.VMEM((n_gz, group, norb), F32),
        pltpu.VMEM((pairs, norb), F32),
    ]
    semaphores = [
        flags(depth),
        one,
        flags(parts, half),
        one,
        flags(parts),
        one,
        flags(parts),
        one,
        flags(parts, half),
        flags(2),
        one,
        one,
        one,
        one,
        one,
        one,
    ]
    held = sum(math.prod(buffer.shape) * buffer.dtype.itemsize for buffer in scratch)
    stay = lambda x: pltpu.with_memory_space_constraint(x, pltpu.HBM)
    term, mix = pl.pallas_call(
        functools.partial(exchange_kernel, n_gz, n_gy),
        out_shape=(
            jax.ShapeDtypeStruct((sets, 2, half, rows // side, across, columns), BF),
            jax.ShapeDtypeStruct((norb + side * pairs, norb), BF),
        ),
        in_specs=[smem] * 3 + [vmem] * 4 + [hbm],
        out_specs=(hbm, vmem),
        scratch_shapes=scratch + semaphores,
        compiler_params=pltpu.CompilerParams(
            vmem_limit_bytes=held + SPARE_VMEM, collective_id=0, has_side_effects=True
        ),
        name="exchange",
    )(*(stay(x) for x in (pair_list.T, box_anchor.T, pair_live, table, wide, rate, gain, orbitals)))

    lump = 2 if depth == 2 * half and half % 2 == 0 else 1
    plane = pl.BlockSpec((lump, rows, across, norb), lambda z: (z, 0, 0, 0))
    per_half = half // lump
    return pl.pallas_call(
        functools.partial(gradient_kernel, side),
        grid=(depth // lump,),
        out_shape=jax.ShapeDtypeStruct(orbitals.shape, F32),
        in_specs=[
            pl.BlockSpec((norb + side * pairs, norb), lambda z: (0, 0)),
            plane,
            pl.BlockSpec(
                (sets, 1, lump, rows // side, across, columns),
                lambda z: (0, z // per_half, z % per_half, 0, 0, 0),
            ),
        ],
        out_specs=plane,
        compiler_params=pltpu.CompilerParams(dimension_semantics=("arbitrary",), vmem_limit_bytes=GRADIENT_VMEM),
        name="gradient",
    )(mix, orbitals, term)


def solution(mesh):
    return jax.shard_map(
        body,
        mesh=mesh,
        in_specs=(P("gz", "gy", None, None), P(), P(), P()),
        out_specs=P("gz", "gy", None, None),
        check_vma=False,
    )
```

```python
import functools
import math

import jax
import jax.numpy as jnp
import numpy as np
from jax import lax
from jax.experimental import pallas as pl
from jax.experimental.pallas import tpu as pltpu
from jax.sharding import PartitionSpec as P

B = 64
LANES = 128
GAP = 8
MESH = pl.DeviceIdType.MESH
BF = jnp.bfloat16
F32 = jnp.float32
SPARE_VMEM = 5 * 512 * 1024
GRADIENT_VMEM = 24 * 1024 * 1024


def dot_nt(a, b):
    return lax.dot_general(a, b, (((1,), (1,)), ((), ())), preferred_element_type=F32)


def dot_nn(a, b):
    return lax.dot_general(a, b, (((1,), (0,)), ((), ())), preferred_element_type=F32)


def dot_tn(a, b):
    return lax.dot_general(a, b, (((0,), (0,)), ((), ())), preferred_element_type=F32)


def split(a):
    hi = a.astype(BF)
    return hi, (a - hi.astype(F32)).astype(BF)


def cell_index(az, extent, z):
    a = lax.rem(z - az + 2 * extent, extent)
    live = a < B
    return jnp.where(live, a + 1, 0), jnp.where(live, B - a, 0)


def power_of(r, n):
    out = None
    while n:
        if n & 1:
            out = r if out is None else out * r
        r = r * r
        n >>= 1
    return out


def exchange_kernel(
    n_gz, n_gy, list_ref, anchor_ref, live_ref, table_ref, wide_ref, r_ref, g_ref, orb_hbm,
    term_hbm, mix_ref,
    column, hot, hot_ref, orb, psi, scr, send, recv, d_ref, e_ref, f_ref, h_ref, pq, pq_in, edge, edge_in, keep, field, field_in,
    term_buf, part, part_in, slab_sum, slab_in, total,
    orb_sem, y_out, y_in, z_out, z_in, e_out, e_in, v_out, v_in, t_sem, a_out, a_in, b_out, b_in, c_out, c_in,
):
    depth, rows, across, norb = orb_hbm.shape
    half = psi.shape[1]
    pairs = psi.shape[3]
    group = pairs // n_gy
    per_dev = group // n_gz
    extent = depth * n_gz
    pitch = pairs + GAP
    wide = 2 if half % 2 == 0 else 1
    chunks = half // wide
    block = 12 if rows % 12 == 0 else 1
    side = max(LANES // pairs, 1) if block > 1 else 1
    gate = 0
    gz = lax.axis_index("gz")
    gy = lax.axis_index("gy")
    at_y = lambda k: lax.rem(gy + k, n_gy)
    at_z = lambda k: lax.rem(gz + 1 + k, n_gz)
    lot = lambda j, h: pl.ds(pl.multiple_of(j * group + h * n_gz, n_gz), n_gz)
    of = lambda j, size: pl.ds(pl.multiple_of(j * size, size), size)

    def anchor(axis, p):
        return anchor_ref[axis, list_ref[0, p]]

    def start_y_of(q):
        return extent - anchor(1, gy * group + q)

    def remote(src, dst, out_sem, in_sem, axis, index):
        return pltpu.make_async_remote_copy(
            src_ref=src, dst_ref=dst, send_sem=out_sem, recv_sem=in_sem, device_id={axis: index}, device_id_type=MESH
        )

    def fetch(z):
        return pltpu.make_async_copy(orb_hbm.at[z], orb.at[z, :, pl.ds(0, across), :], orb_sem.at[z])

    def pad_and_fetch(z, _):
        orb[z, :, across:, :] = jnp.zeros((rows, LANES - across, norb), BF)
        fetch(z).start()
        return 0

    def pad_and_fetch_both(t, _):
        pad_and_fetch(t, 0)

        @pl.when(half + t < depth)
        def _():
            pad_and_fetch(half + t, 0)

        return 0

    lax.fori_loop(0, half, pad_and_fetch_both, 0)

    barrier = pltpu.get_barrier_semaphore()
    for k in range(1, n_gy):
        pl.semaphore_signal(barrier, inc=1, device_id={"gy": at_y(k)}, device_id_type=MESH)

    def greet(k, _):
        pl.semaphore_signal(barrier, inc=1, device_id={"gz": at_z(k)}, device_id_type=MESH)
        return 0

    lax.fori_loop(0, n_gz - 1, greet, 0)

    orbital = lax.broadcasted_iota(jnp.int32, (1, norb), 1)

    def mark(p, _):
        column[p] = anchor(2, p)
        for k in range(2):
            hot[pl.ds(k * pairs + p, 1), :] = (orbital == list_ref[k, p]).astype(F32)
        return 0

    lax.fori_loop(0, pairs, mark, 0, unroll=8)
    hot_ref[...] = hot[...].astype(BF)
    r2 = r_ref[...] * r_ref[...]
    e_ref[0] = jnp.zeros_like(r2)

    def fill(n, power):
        power = power * r2
        e_ref[n] = 1.0 - power
        return power

    lax.fori_loop(1, B + 1, fill, jnp.ones_like(r2))

    def across_y(mail, h, t, k):
        source, target, out_sem, in_sem = mail
        j = at_y(k)
        return remote(
            source.at[t, lot(j, h)], target.at[t, lot(gy, h)], out_sem, in_sem.at[h, t], "gy", j
        )

    def stay_y(mail, h, t):
        source, target, _, in_sem = mail
        return pltpu.make_async_copy(source.at[t, lot(gy, h)], target.at[t, lot(gy, h)], in_sem.at[h, t])

    def start_y(mail, h, t):
        for k in range(1, n_gy):
            across_y(mail, h, t, k).start()
        stay_y(mail, h, t).start()

    def wait_y(mail, h, t):
        _, target, _, in_sem = mail
        every = target.at[t, pl.ds(0, n_gy * n_gz)]
        pltpu.make_async_copy(every, every, in_sem.at[h, t]).wait()

    def sent_y(mail):
        source, target, out_sem, in_sem = mail
        every = pl.ds(0, (n_gy - 1) * group)
        remote(source.at[:, every], target.at[:, every], out_sem, in_sem.at[0, 0], "gy", at_y(1)).wait_send()

    outward = (send, recv, y_out, y_in)
    inward = (field, field_in, v_out, v_in)

    lane_rows = lax.broadcasted_iota(jnp.int32, (rows, LANES), 1)
    lane = lax.broadcasted_iota(jnp.int32, (B, LANES), 1)
    lower = lane < B

    def density(t):
        for h in range(2):
            z = jnp.minimum(h * half + t, depth - 1)

            @pl.when(h * half + t < depth)
            def _():
                fetch(z).wait()

            def some(i, carry):
                both = dot_nt(hot_ref[...], orb[z, pl.ds(i * 2, 2)].reshape(2 * LANES, norb))
                for k in range(2):
                    y = i * 2 + k
                    mine = both[:, k * LANES:(k + 1) * LANES]
                    value = mine[:pairs] * mine[pairs:] + carry
                    sent = value.astype(BF).astype(F32)
                    scr[h, pl.ds(pl.multiple_of(y * pitch, 8), pairs), :] = sent
                    psi[h, t, y] = mine[pairs:].astype(BF)
                    carry = value - sent
                return carry

            lax.fori_loop(0, rows // 2, some, jnp.zeros((pairs, LANES), F32), unroll=12)

        def pair(p, _):
            acc = jnp.zeros((rows, LANES), F32)
            a = column[p]
            for h in range(2):
                base = h * B
                x = scr[h, pl.ds(p, rows, stride=pitch), :]
                near = pltpu.roll(x, lax.rem(base - a + 2 * LANES, LANES), 1)
                far = pltpu.roll(x, lax.rem(base + across - a + 2 * LANES, LANES), 1)
                rel = lane_rows - base
                acc = jnp.where((rel >= 0) & (rel < B), jnp.where(rel < across - a, near, far), acc)
            send[t, p] = acc.astype(BF)
            return 0

        lax.fori_loop(0, pairs, pair, 0, unroll=32)
        @pl.when(t == gate)
        def _():
            pl.semaphore_wait(barrier, n_gy + n_gz - 2)
            for early in range(gate):
                start_y(outward, 0, early)

        @pl.when(t >= gate)
        def _():
            start_y(outward, 0, t)

    def forward(part_at, c):
        for s in range(wide):
            wait_y(outward, part_at, c * wide + s)

        def pair(n, _):
            q = part_at * n_gz + n
            m = table_ref[0, pl.ds(start_y_of(q), extent), :].astype(BF)
            planes = []
            for s in range(wide):
                got = [recv[c * wide + s, j * group + q].astype(F32) for j in range(n_gy)]
                planes.append(jnp.concatenate(got, axis=0).astype(BF))
            y = dot_tn(m, jnp.concatenate(planes, axis=1))
            y = y[:B] + y[B:]
            hi, lo = split(jnp.concatenate([y[:, s * LANES:(s + 1) * LANES] for s in range(wide)], axis=0))
            x = dot_nn(jnp.concatenate([hi, lo], axis=1), wide_ref[...])
            x = x[:, :LANES] + x[:, LANES:]
            for s in range(wide):
                d_ref[q, c * wide + s] = x[s * B:(s + 1) * B] * g_ref[...]
            return 0

        lax.fori_loop(0, n_gz, pair, 0, unroll=8)

    def stage(c, _):
        @pl.when(c < chunks)
        def _():
            def one(s, _):
                density(c * wide + s)
                return 0

            lax.fori_loop(0, wide, one, 0)

        @pl.when(c == chunks)
        def _():
            def rest(t, _):
                for h in range(1, per_dev):
                    start_y(outward, h, t)
                return 0

            lax.fori_loop(0, half, rest, 0)

        @pl.when(c >= 1)
        def _():
            forward(0, c - 1)

        return 0

    lax.fori_loop(0, chunks + 1, stage, 0)

    def weights(q):
        az = anchor(0, gy * group + q)
        out = []
        for t in range(half):
            lu, lw = cell_index(az, extent, gz * depth + t)
            hu, hw = cell_index(az, extent, gz * depth + half + t)
            if half + t >= depth:
                hu, hw = 0, 0
            out.append((jnp.where(lower, e_ref[lu], e_ref[hu]), jnp.where(lower, e_ref[lw], e_ref[hw])))
        return out

    def rate(r, t):
        return r if half + t < depth else jnp.where(lower, r, 1.0)

    def give(h, k):
        j = at_z(k)
        return remote(pq.at[h * n_gz + j], pq_in.at[h, gz], z_out, z_in.at[h], "gz", j)

    def give_back(h, k):
        j = at_z(k)
        return remote(edge.at[h, j], edge_in.at[h * n_gz + gz], e_out, e_in.at[h], "gz", j)

    def keep_own(h):
        return pltpu.make_async_copy(pq.at[h * n_gz + gz], pq_in.at[h, gz], z_in.at[h])

    def keep_edge(h):
        return pltpu.make_async_copy(edge.at[h, gz], edge_in.at[h * n_gz + gz], e_in.at[h])

    def ends(h):
        def one(k, _):
            q = h * n_gz + at_z(k)
            r = r_ref[...]
            at = weights(q)
            d = [d_ref[q, t] for t in range(half)]
            f = at[0][0] * d[0]
            for t in range(1, half):
                f = rate(r, t) * f + at[t][0] * d[t]
            b = r * (at[half - 1][1] * d[half - 1])
            for t in reversed(range(half - 1)):
                b = r * (b + at[t][1] * d[t])
            f_ref[q] = f
            h_ref[q] = b
            p_sum = power_of(r, depth - half) * f + pltpu.roll(f, B, 1)
            q_sum = pltpu.roll(b, B, 1) + power_of(r, half) * b
            pq[q] = jnp.where(lower, p_sum, q_sum).astype(BF)

            @pl.when(k < n_gz - 1)
            def _():
                give(h, k).start()

            return 0

        lax.fori_loop(0, n_gz, one, 0)
        keep_own(h).start()

    def chain(h):
        pltpu.make_async_copy(pq_in.at[h], pq_in.at[h], z_in.at[h]).wait()
        slab_rate = power_of(r_ref[...], depth)
        az = anchor(0, gy * group + h * n_gz + gz)

        def up(k, f):
            i = lax.rem(k, n_gz)
            start = lax.rem(depth * i - az + extent, extent)
            f = jnp.where(start < B, f, 0.0)
            keep[i] = f
            return pq_in[h, i].astype(F32) + slab_rate * f

        lax.fori_loop(0, 2 * n_gz, up, jnp.zeros((B, LANES), F32))

        def down(k, b):
            i = lax.rem(2 * n_gz - k, n_gz)
            end = lax.rem(depth * i + depth - 1 - az + extent, extent)
            b = jnp.where(end < B, b, 0.0)
            edge[h, i] = jnp.where(lower, keep[i], b).astype(BF)
            return pq_in[h, i].astype(F32) + slab_rate * b

        lax.fori_loop(0, 2 * n_gz, down, jnp.zeros((B, LANES), F32))

        def back(k, _):
            give_back(h, k).start()
            return 0

        lax.fori_loop(0, n_gz - 1, back, 0)
        keep_edge(h).start()

    def solve(h):
        every = edge_in.at[pl.ds(h * n_gz, n_gz)]
        pltpu.make_async_copy(every, every, e_in.at[h]).wait()

        def one(k, _):
            q = h * n_gz + k
            r = r_ref[...]
            at = weights(q)
            came = edge_in[q].astype(F32)
            swap = pltpu.roll(came, B, 1)
            f = jnp.where(lower, came, power_of(r, half) * swap + pltpu.roll(f_ref[q], B, 1))
            b = jnp.where(lower, power_of(r, depth - half) * swap + pltpu.roll(h_ref[q], B, 1), came)
            d = [d_ref[q, t] for t in range(half)]
            v = []
            for t in range(half):
                f = rate(r, t) * f + at[t][0] * d[t]
                v.append(at[t][1] * f)
            for t in reversed(range(half)):
                d_ref[q, t] = v[t] + at[t][0] * b
                b = rate(r, t) * (b + at[t][1] * d[t])
            return 0

        lax.fori_loop(0, n_gz, one, 0)

    def inverse(part_at, c):
        def pair(n, _):
            q = part_at * n_gz + n
            at = pl.ds(start_y_of(q), extent)
            m = jnp.concatenate([table_ref[0, at, :], table_ref[1, at, :]], axis=1).astype(BF)[:, :3 * B]
            hi, lo = split(jnp.concatenate([d_ref[q, c * wide + s] for s in range(wide)], axis=0))
            x = dot_nn(jnp.concatenate([hi, lo], axis=1), wide_ref[...])
            x = x[:, :LANES] + x[:, LANES:]
            hi, lo = split(jnp.concatenate([x[s * B:(s + 1) * B] for s in range(wide)], axis=1))
            y = dot_nn(m, jnp.concatenate([hi, hi, lo], axis=0))
            for s in range(wide):
                for j in range(n_gy):
                    out = y[j * rows:(j + 1) * rows, s * LANES:(s + 1) * LANES]
                    field[c * wide + s, j * group + q] = out.astype(BF)
            return 0

        lax.fori_loop(0, n_gz, pair, 0, unroll=8)
        for s in range(wide):
            start_y(inward, part_at, c * wide + s)

    def each(first, last, work):
        def one(c, _):
            work(c)
            return 0

        lax.fori_loop(first, last, one, 0)

    ends(0)
    for h in range(1, per_dev):
        ahead = functools.partial(inverse, h - 1)

        def pull(c, h=h, ahead=ahead):
            @pl.when(c == chunks - 1)
            def _():
                solve(h - 1)
                ahead(0)

            forward(h, c)

            @pl.when(c == 0)
            def _():
                chain(h - 1)

        if chunks > 1:
            each(0, chunks, pull)
            ends(h)
            each(1, chunks, ahead)
        else:
            forward(h, 0)
            chain(h - 1)
            ends(h)
            solve(h - 1)
            ahead(0)
    chain(per_dev - 1)
    solve(per_dev - 1)
    each(0, chunks, functools.partial(inverse, per_dev - 1))
    part[...] = jnp.zeros_like(part)

    def put(t):
        slot = lax.rem(t, 2)
        return pltpu.make_async_copy(term_buf.at[slot], term_hbm.at[:, t], t_sem.at[slot])

    def term(t, _):
        for h in range(per_dev):
            wait_y(inward, h, t)

        def pair(p, _):
            v = field_in[t, p].astype(F32)
            a = column[p]
            lit = live_ref[p] > 0
            rel = lane_rows - a
            for h in range(2):
                base = h * B
                near = pltpu.roll(v, lax.rem(a - base + 2 * LANES, LANES), 1)
                far = pltpu.roll(v, lax.rem(a - across - base + 3 * LANES, LANES), 1)
                v_p = jnp.where((rel >= 0) & (rel < B) & lit, near, 0.0)
                v_p = jnp.where((rel + across < B) & lit, far, v_p)
                scr[h, pl.ds(p, rows, stride=pitch), :] = v_p
            return 0

        lax.fori_loop(0, pairs, pair, 0, unroll=32)

        @pl.when(t >= 2)
        def _():
            put(t - 2).wait()

        slot = lax.rem(t, 2)
        for h in range(2):
            z = jnp.minimum(h * half + t, depth - 1)

            def some(i, _):
                got = []
                for k in range(block):
                    y = i * block + k
                    v = scr[h, pl.ds(pl.multiple_of(y * pitch, 8), pairs), :]
                    got.append((v * psi[h, t, y].astype(F32)).astype(BF))
                for k in range(0, block, side):
                    turned = jnp.concatenate(got[k:k + side], axis=0).T
                    term_buf[slot, h, i * (block // side) + k // side] = turned[:across]
                o = orb[z, pl.ds(i * block, block)].reshape(block * LANES, norb)
                part[...] += dot_nn(jnp.concatenate(got, axis=1), o)
                return 0

            lax.fori_loop(0, rows // block, some, 0, unroll=True)
        put(t).start()
        return 0

    lax.fori_loop(0, half, term, 0)

    def share(k):
        return remote(part.at[of(at_y(k), group)], part_in.at[k], a_out, a_in, "gy", at_y(k))

    def spread(k):
        return remote(slab_sum, slab_in.at[gz], b_out, b_in, "gz", at_z(k))

    def gather(k):
        return remote(total.at[of(gy, group)], total.at[of(gy, group)], c_out, c_in, "gy", at_y(k))

    for k in range(1, n_gy):
        share(k).start()
    own = part[of(gy, group), :]
    others = part_in.at[pl.ds(1, n_gy - 1)]
    pltpu.make_async_copy(others, others, a_in).wait()
    for k in range(1, n_gy):
        own = own + part_in[k]
    slab_sum[...] = own

    def begin(k, _):
        spread(k).start()
        return 0

    lax.fori_loop(0, n_gz - 1, begin, 0)
    slab_in[gz] = own

    others = slab_in.at[pl.ds(0, n_gz - 1)]
    pltpu.make_async_copy(others, others, b_in).wait()

    def add(i, acc):
        return acc + slab_in[i]

    total[of(gy, group), :] = lax.fori_loop(1, n_gz, add, slab_in[0])
    for k in range(1, n_gy):
        gather(k).start()
    others = total.at[pl.ds(0, (n_gy - 1) * group)]
    pltpu.make_async_copy(others, others, c_in).wait()
    high, low = split(total[...])
    rest = (total[...] - high.astype(F32) - low.astype(F32)).astype(BF)
    sel = hot_ref[:pairs]
    inner = dot_tn(jnp.concatenate([high, low, rest], axis=0), jnp.concatenate([sel, sel, sel], axis=0))
    mix_ref[:norb] = -(inner / (float(B) ** 3 / 4.0)).astype(BF)
    for k in range(side):
        mix_ref[norb + k * pairs:norb + (k + 1) * pairs] = sel

    sent_y(outward)
    sent_y(inward)
    given = pl.ds(0, per_dev * (n_gz - 1))
    remote(pq.at[given], edge_in.at[given], z_out, z_in.at[0], "gz", at_z(0)).wait_send()
    remote(pq.at[given], edge_in.at[given], e_out, e_in.at[0], "gz", at_z(0)).wait_send()
    spare = part_in.at[pl.ds(1, n_gy - 1)]
    remote(spare, spare, a_out, a_in, "gy", at_y(1)).wait_send()
    remote(spare, spare, c_out, c_in, "gy", at_y(1)).wait_send()
    spare = slab_in.at[pl.ds(0, n_gz - 1)]
    remote(spare, spare, b_out, b_in, "gz", at_z(0)).wait_send()
    for t in range(max(half - 2, 0), half):
        put(t).wait()


def gradient_kernel(side, mix_ref, orb_ref, term_ref, out_ref):
    lump, rows, across, norb = orb_ref.shape
    pairs = term_ref.shape[-1] // side
    lane = lax.broadcasted_iota(jnp.int32, (across, side * pairs), 1)

    def plane(z, _):
        held = []
        for y in range(rows):
            c = term_ref[0, z, y // side]
            if side > 1:
                k = y % side
                c = jnp.where((lane >= k * pairs) & (lane < (k + 1) * pairs), c, jnp.zeros_like(c))
            held.append(c)
        o = orb_ref[z].reshape(rows * across, norb)
        out = dot_nn(jnp.concatenate([o, jnp.concatenate(held, axis=0)], axis=1), mix_ref[...])
        out_ref[z] = out.reshape(rows, across, norb)
        return 0

    lax.fori_loop(0, lump, plane, 0, unroll=True)


def tables():
    index = np.arange(1, B + 1, dtype=np.float64)
    s = np.sqrt(2.0 / (B + 1.0)) * np.sin(np.pi * index[:, None] * index[None, :] / (B + 1.0))
    eigen = 2.0 - 2.0 * np.cos(np.pi * index / (B + 1.0))
    hi = s.astype(jnp.bfloat16).astype(np.float64)
    lo = (s - hi).astype(jnp.bfloat16).astype(np.float64)
    eye = np.eye(LANES // B)
    bd = lambda m: np.kron(eye, m)
    wide = np.block([[bd(hi), bd(lo)], [bd(hi), np.zeros((LANES, LANES))]]).astype(jnp.bfloat16)
    left = np.stack([np.concatenate([hi, lo], axis=1), np.concatenate([hi, np.zeros((B, B))], axis=1)])
    cosh = 1.0 + 0.5 * (eigen[:, None] + eigen[None, :])
    r = cosh - np.sqrt(cosh * cosh - 1.0)
    g = 1.0 / ((1.0 / r - r) * (1.0 - r ** (2 * B + 2)))
    twice = lambda m: np.tile(m, (1, LANES // B)).astype(np.float32)
    return left.astype(np.float32), wide, twice(r), twice(g)


def body(orbitals, pair_list, box_anchor, pair_live):
    depth, rows, across, norb = orbitals.shape
    n_gz = lax.axis_size("gz")
    n_gy = lax.axis_size("gy")
    pairs = pair_list.shape[0]
    group = pairs // n_gy
    per_dev = group // n_gz
    extent = depth * n_gz
    half = (depth + 1) // 2
    block = 12 if rows % 12 == 0 else 1
    side = max(LANES // pairs, 1) if block > 1 else 1

    smem = pl.BlockSpec(memory_space=pltpu.SMEM)
    vmem = pl.BlockSpec(memory_space=pltpu.VMEM)
    hbm = pl.BlockSpec(memory_space=pl.ANY)
    left, wide, rate, gain = (jnp.asarray(m) for m in tables())
    cycle = jnp.concatenate([left, jnp.zeros((2, extent - B, LANES), F32)], axis=1)
    table = jnp.concatenate([cycle, cycle], axis=1)
    mail = pltpu.VMEM((half, pairs, rows, LANES), BF)
    mode = pltpu.VMEM((group, B, LANES), F32)
    edges = pltpu.VMEM((group, B, LANES), BF)
    owners = pltpu.VMEM((per_dev, n_gz, B, LANES), BF)
    flags = lambda *shape: pltpu.SemaphoreType.DMA(shape)
    one = pltpu.SemaphoreType.DMA
    scratch = [
        pltpu.VMEM((2 * pairs, norb), F32),
        pltpu.VMEM((2 * pairs, norb), BF),
        pltpu.VMEM((depth, rows, LANES, norb), BF),
        pltpu.VMEM((2, half, rows, pairs, LANES), BF),
        pltpu.VMEM((2, rows * (pairs + GAP), LANES), F32),
        mail,
        mail,
        pltpu.VMEM((group, half, B, LANES), F32),
        pltpu.VMEM((B + 1, B, LANES), F32),
        mode,
        mode,
        edges,
        owners,
        owners,
        edges,
        pltpu.VMEM((n_gz, B, LANES), F32),
        mail,
        mail,
        pltpu.VMEM((2, 2, rows // side, across, side * pairs), BF),
        pltpu.VMEM((pairs, norb), F32),
        pltpu.VMEM((n_gy, group, norb), F32),
        pltpu.VMEM((group, norb), F32),
        pltpu.VMEM((n_gz, group, norb), F32),
        pltpu.VMEM((pairs, norb), F32),
    ]
    columns = [pltpu.SMEM((pairs,), jnp.int32)]
    semaphores = [
        flags(depth),
        one,
        flags(per_dev, half),
        one,
        flags(per_dev),
        one,
        flags(per_dev),
        one,
        flags(per_dev, half),
        flags(2),
        one,
        one,
        one,
        one,
        one,
        one,
    ]
    held = sum(math.prod(buffer.shape) * buffer.dtype.itemsize for buffer in scratch)
    stay = lambda x: pltpu.with_memory_space_constraint(x, pltpu.HBM)
    term, mix = pl.pallas_call(
        functools.partial(exchange_kernel, n_gz, n_gy),
        out_shape=(
            jax.ShapeDtypeStruct((2, half, rows // side, across, side * pairs), BF),
            jax.ShapeDtypeStruct((norb + side * pairs, norb), BF),
        ),
        in_specs=[smem] * 3 + [vmem] * 4 + [hbm],
        out_specs=(hbm, vmem),
        scratch_shapes=columns + scratch + semaphores,
        compiler_params=pltpu.CompilerParams(
            vmem_limit_bytes=held + SPARE_VMEM, collective_id=0, has_side_effects=True
        ),
        name="exchange",
    )(*(stay(x) for x in (pair_list.T, box_anchor.T, pair_live, table, wide, rate, gain, orbitals)))

    lump = 2 if depth == 2 * half and half % 2 == 0 else 1
    plane = pl.BlockSpec((lump, rows, across, norb), lambda z: (z, 0, 0, 0))
    per_half = half // lump
    return pl.pallas_call(
        functools.partial(gradient_kernel, side),
        grid=(depth // lump,),
        out_shape=jax.ShapeDtypeStruct(orbitals.shape, F32),
        in_specs=[
            pl.BlockSpec((norb + side * pairs, norb), lambda z: (0, 0)),
            plane,
            pl.BlockSpec(
                (1, lump, rows // side, across, side * pairs), lambda z: (z // per_half, z % per_half, 0, 0, 0)
            ),
        ],
        out_specs=plane,
        compiler_params=pltpu.CompilerParams(dimension_semantics=("arbitrary",), vmem_limit_bytes=GRADIENT_VMEM),
        name="gradient",
    )(mix, orbitals, term)


def solution(mesh):
    return jax.shard_map(
        body,
        mesh=mesh,
        in_specs=(P("gz", "gy", None, None), P(), P(), P()),
        out_specs=P("gz", "gy", None, None),
        check_vma=False,
    )
```

```python
import functools
import math

import jax
import jax.numpy as jnp
import numpy as np
from jax import lax
from jax.experimental import pallas as pl
from jax.experimental.pallas import tpu as pltpu
from jax.sharding import PartitionSpec as P

B = 64
LANES = 128
GAP = 8
MESH = pl.DeviceIdType.MESH
BF = jnp.bfloat16
F32 = jnp.float32
SPARE_VMEM = 5 * 512 * 1024
GRADIENT_VMEM = 24 * 1024 * 1024


def dot_nt(a, b):
    return lax.dot_general(a, b, (((1,), (1,)), ((), ())), preferred_element_type=F32)


def dot_nn(a, b):
    return lax.dot_general(a, b, (((1,), (0,)), ((), ())), preferred_element_type=F32)


def dot_tn(a, b):
    return lax.dot_general(a, b, (((0,), (0,)), ((), ())), preferred_element_type=F32)


def split(a):
    hi = a.astype(BF)
    return hi, (a - hi.astype(F32)).astype(BF)


def cell_index(az, extent, z):
    a = lax.rem(z - az + 2 * extent, extent)
    live = a < B
    return jnp.where(live, a + 1, 0), jnp.where(live, B - a, 0)


def power_of(r, n):
    out = None
    while n:
        if n & 1:
            out = r if out is None else out * r
        r = r * r
        n >>= 1
    return out


def exchange_kernel(
    n_gz, n_gy, list_ref, anchor_ref, live_ref, table_ref, wide_ref, r_ref, g_ref, orb_hbm,
    term_hbm, mix_ref,
    column, hot, hot_ref, orb, psi, scr, send, recv, d_ref, e_ref, f_ref, h_ref, pq, pq_in, edge, edge_in, keep, field, field_in,
    term_buf, part, part_in, slab_sum, slab_in, total,
    orb_sem, y_out, y_in, z_out, z_in, e_out, e_in, v_out, v_in, t_sem, a_out, a_in, b_out, b_in, c_out, c_in,
):
    depth, rows, across, norb = orb_hbm.shape
    half = psi.shape[1]
    pairs = psi.shape[3]
    group = pairs // n_gy
    per_dev = group // n_gz
    extent = depth * n_gz
    pitch = pairs + GAP
    wide = 2 if half % 2 == 0 else 1
    chunks = half // wide
    block = 12 if rows % 12 == 0 else 1
    side = max(LANES // pairs, 1) if block > 1 else 1
    gate = 0
    gz = lax.axis_index("gz")
    gy = lax.axis_index("gy")
    at_y = lambda k: lax.rem(gy + k, n_gy)
    at_z = lambda k: lax.rem(gz + 1 + k, n_gz)
    lot = lambda j, h: pl.ds(pl.multiple_of(j * group + h * n_gz, n_gz), n_gz)
    of = lambda j, size: pl.ds(pl.multiple_of(j * size, size), size)

    def anchor(axis, p):
        return anchor_ref[axis, list_ref[0, p]]

    def start_y_of(q):
        return extent - anchor(1, gy * group + q)

    def remote(src, dst, out_sem, in_sem, axis, index):
        return pltpu.make_async_remote_copy(
            src_ref=src, dst_ref=dst, send_sem=out_sem, recv_sem=in_sem, device_id={axis: index}, device_id_type=MESH
        )

    def fetch(z):
        return pltpu.make_async_copy(orb_hbm.at[z], orb.at[z, :, pl.ds(0, across), :], orb_sem.at[z])

    def pad_and_fetch(z, _):
        orb[z, :, across:, :] = jnp.zeros((rows, LANES - across, norb), BF)
        fetch(z).start()
        return 0

    def pad_and_fetch_both(t, _):
        pad_and_fetch(t, 0)

        @pl.when(half + t < depth)
        def _():
            pad_and_fetch(half + t, 0)

        return 0

    lax.fori_loop(0, half, pad_and_fetch_both, 0)

    barrier = pltpu.get_barrier_semaphore()
    for k in range(1, n_gy):
        pl.semaphore_signal(barrier, inc=1, device_id={"gy": at_y(k)}, device_id_type=MESH)

    def greet(k, _):
        pl.semaphore_signal(barrier, inc=1, device_id={"gz": at_z(k)}, device_id_type=MESH)
        return 0

    lax.fori_loop(0, n_gz - 1, greet, 0)

    orbital = lax.broadcasted_iota(jnp.int32, (1, norb), 1)

    def mark(p, _):
        column[p] = anchor(2, p)
        for k in range(2):
            hot[pl.ds(k * pairs + p, 1), :] = (orbital == list_ref[k, p]).astype(F32)
        return 0

    lax.fori_loop(0, pairs, mark, 0, unroll=8)
    hot_ref[...] = hot[...].astype(BF)
    r2 = r_ref[...] * r_ref[...]
    e_ref[0] = jnp.zeros_like(r2)

    def fill(n, power):
        power = power * r2
        e_ref[n] = 1.0 - power
        return power

    lax.fori_loop(1, B + 1, fill, jnp.ones_like(r2))

    def across_y(mail, h, t, k):
        source, target, out_sem, in_sem = mail
        j = at_y(k)
        return remote(
            source.at[t, lot(j, h)], target.at[t, lot(gy, h)], out_sem, in_sem.at[h, t], "gy", j
        )

    def stay_y(mail, h, t):
        source, target, _, in_sem = mail
        return pltpu.make_async_copy(source.at[t, lot(gy, h)], target.at[t, lot(gy, h)], in_sem.at[h, t])

    def start_y(mail, h, t):
        for k in range(1, n_gy):
            across_y(mail, h, t, k).start()
        stay_y(mail, h, t).start()

    def wait_y(mail, h, t):
        _, target, _, in_sem = mail
        every = target.at[t, pl.ds(0, n_gy * n_gz)]
        pltpu.make_async_copy(every, every, in_sem.at[h, t]).wait()

    def sent_y(mail):
        source, target, out_sem, in_sem = mail
        every = pl.ds(0, (n_gy - 1) * group)
        remote(source.at[:, every], target.at[:, every], out_sem, in_sem.at[0, 0], "gy", at_y(1)).wait_send()

    outward = (send, recv, y_out, y_in)
    inward = (field, field_in, v_out, v_in)

    lane_rows = lax.broadcasted_iota(jnp.int32, (rows, LANES), 1)
    lane = lax.broadcasted_iota(jnp.int32, (B, LANES), 1)
    lower = lane < B

    def density(t):
        for h in range(2):
            z = jnp.minimum(h * half + t, depth - 1)

            @pl.when(h * half + t < depth)
            def _():
                fetch(z).wait()

            def some(i, carry):
                both = dot_nt(hot_ref[...], orb[z, pl.ds(i * 2, 2)].reshape(2 * LANES, norb))
                for k in range(2):
                    y = i * 2 + k
                    mine = both[:, k * LANES:(k + 1) * LANES]
                    value = mine[:pairs] * mine[pairs:] + carry
                    sent = value.astype(BF).astype(F32)
                    scr[h, pl.ds(pl.multiple_of(y * pitch, 8), pairs), :] = sent
                    psi[h, t, y] = mine[pairs:].astype(BF)
                    carry = value - sent
                return carry

            lax.fori_loop(0, rows // 2, some, jnp.zeros((pairs, LANES), F32), unroll=12)

        def pair(p, _):
            acc = jnp.zeros((rows, LANES), F32)
            a = column[p]
            for h in range(2):
                base = h * B
                x = scr[h, pl.ds(p, rows, stride=pitch), :]
                near = pltpu.roll(x, lax.rem(base - a + 2 * LANES, LANES), 1)
                far = pltpu.roll(x, lax.rem(base + across - a + 2 * LANES, LANES), 1)
                rel = lane_rows - base
                acc = jnp.where((rel >= 0) & (rel < B), jnp.where(rel < across - a, near, far), acc)
            send[t, p] = acc.astype(BF)
            return 0

        lax.fori_loop(0, pairs, pair, 0, unroll=32)
        @pl.when(t == gate)
        def _():
            pl.semaphore_wait(barrier, n_gy + n_gz - 2)
            for early in range(gate):
                start_y(outward, 0, early)

        @pl.when(t >= gate)
        def _():
            start_y(outward, 0, t)

    def forward(part_at, c):
        for s in range(wide):
            wait_y(outward, part_at, c * wide + s)

        def pair(n, _):
            q = part_at * n_gz + n
            m = table_ref[0, pl.ds(start_y_of(q), extent), :].astype(BF)
            planes = []
            for s in range(wide):
                got = [recv[c * wide + s, j * group + q].astype(F32) for j in range(n_gy)]
                planes.append(jnp.concatenate(got, axis=0).astype(BF))
            y = dot_tn(m, jnp.concatenate(planes, axis=1))
            y = y[:B] + y[B:]
            hi, lo = split(jnp.concatenate([y[:, s * LANES:(s + 1) * LANES] for s in range(wide)], axis=0))
            x = dot_nn(jnp.concatenate([hi, lo], axis=1), wide_ref[...])
            x = x[:, :LANES] + x[:, LANES:]
            for s in range(wide):
                d_ref[q, c * wide + s] = x[s * B:(s + 1) * B] * g_ref[...]
            return 0

        lax.fori_loop(0, n_gz, pair, 0, unroll=8)

    def stage(c, _):
        @pl.when(c < chunks)
        def _():
            def one(s, _):
                density(c * wide + s)
                return 0

            lax.fori_loop(0, wide, one, 0)

        @pl.when(c == chunks)
        def _():
            def rest(t, _):
                for h in range(1, per_dev):
                    start_y(outward, h, t)
                return 0

            lax.fori_loop(0, half, rest, 0)

        @pl.when(c >= 1)
        def _():
            forward(0, c - 1)

        return 0

    lax.fori_loop(0, chunks + 1, stage, 0)

    def weights(q):
        az = anchor(0, gy * group + q)
        out = []
        for t in range(half):
            lu, lw = cell_index(az, extent, gz * depth + t)
            hu, hw = cell_index(az, extent, gz * depth + half + t)
            if half + t >= depth:
                hu, hw = 0, 0
            out.append((jnp.where(lower, e_ref[lu], e_ref[hu]), jnp.where(lower, e_ref[lw], e_ref[hw])))
        return out

    def rate(r, t):
        return r if half + t < depth else jnp.where(lower, r, 1.0)

    def give(h, k):
        j = at_z(k)
        return remote(pq.at[h * n_gz + j], pq_in.at[h, gz], z_out, z_in.at[h], "gz", j)

    def give_back(h, k):
        j = at_z(k)
        return remote(edge.at[h, j], edge_in.at[h * n_gz + gz], e_out, e_in.at[h], "gz", j)

    def keep_own(h):
        return pltpu.make_async_copy(pq.at[h * n_gz + gz], pq_in.at[h, gz], z_in.at[h])

    def keep_edge(h):
        return pltpu.make_async_copy(edge.at[h, gz], edge_in.at[h * n_gz + gz], e_in.at[h])

    def ends(h):
        def one(k, _):
            q = h * n_gz + at_z(k)
            r = r_ref[...]
            at = weights(q)
            d = [d_ref[q, t] for t in range(half)]
            f = at[0][0] * d[0]
            for t in range(1, half):
                f = rate(r, t) * f + at[t][0] * d[t]
            b = r * (at[half - 1][1] * d[half - 1])
            for t in reversed(range(half - 1)):
                b = r * (b + at[t][1] * d[t])
            f_ref[q] = f
            h_ref[q] = b
            p_sum = power_of(r, depth - half) * f + pltpu.roll(f, B, 1)
            q_sum = pltpu.roll(b, B, 1) + power_of(r, half) * b
            pq[q] = jnp.where(lower, p_sum, q_sum).astype(BF)

            @pl.when(k < n_gz - 1)
            def _():
                give(h, k).start()

            return 0

        lax.fori_loop(0, n_gz, one, 0, unroll=2)
        keep_own(h).start()

    def chain(h):
        pltpu.make_async_copy(pq_in.at[h], pq_in.at[h], z_in.at[h]).wait()
        slab_rate = power_of(r_ref[...], depth)
        az = anchor(0, gy * group + h * n_gz + gz)

        def up(k, f):
            i = lax.rem(k, n_gz)
            start = lax.rem(depth * i - az + extent, extent)
            f = jnp.where(start < B, f, 0.0)
            keep[i] = f
            return pq_in[h, i].astype(F32) + slab_rate * f

        lax.fori_loop(0, 2 * n_gz, up, jnp.zeros((B, LANES), F32), unroll=8)

        def down(k, b):
            i = lax.rem(2 * n_gz - k, n_gz)
            end = lax.rem(depth * i + depth - 1 - az + extent, extent)
            b = jnp.where(end < B, b, 0.0)
            edge[h, i] = jnp.where(lower, keep[i], b).astype(BF)
            return pq_in[h, i].astype(F32) + slab_rate * b

        lax.fori_loop(0, 2 * n_gz, down, jnp.zeros((B, LANES), F32), unroll=8)

        def back(k, _):
            give_back(h, k).start()
            return 0

        lax.fori_loop(0, n_gz - 1, back, 0)
        keep_edge(h).start()

    def solve(h):
        every = edge_in.at[pl.ds(h * n_gz, n_gz)]
        pltpu.make_async_copy(every, every, e_in.at[h]).wait()

        def one(k, _):
            q = h * n_gz + k
            r = r_ref[...]
            at = weights(q)
            came = edge_in[q].astype(F32)
            swap = pltpu.roll(came, B, 1)
            f = jnp.where(lower, came, power_of(r, half) * swap + pltpu.roll(f_ref[q], B, 1))
            b = jnp.where(lower, power_of(r, depth - half) * swap + pltpu.roll(h_ref[q], B, 1), came)
            d = [d_ref[q, t] for t in range(half)]
            v = []
            for t in range(half):
                f = rate(r, t) * f + at[t][0] * d[t]
                v.append(at[t][1] * f)
            for t in reversed(range(half)):
                d_ref[q, t] = v[t] + at[t][0] * b
                b = rate(r, t) * (b + at[t][1] * d[t])
            return 0

        lax.fori_loop(0, n_gz, one, 0, unroll=2)

    def inverse(part_at, c):
        def pair(n, _):
            q = part_at * n_gz + n
            at = pl.ds(start_y_of(q), extent)
            m = jnp.concatenate([table_ref[0, at, :], table_ref[1, at, :]], axis=1).astype(BF)[:, :3 * B]
            hi, lo = split(jnp.concatenate([d_ref[q, c * wide + s] for s in range(wide)], axis=0))
            x = dot_nn(jnp.concatenate([hi, lo], axis=1), wide_ref[...])
            x = x[:, :LANES] + x[:, LANES:]
            hi, lo = split(jnp.concatenate([x[s * B:(s + 1) * B] for s in range(wide)], axis=1))
            y = dot_nn(m, jnp.concatenate([hi, hi, lo], axis=0))
            for s in range(wide):
                for j in range(n_gy):
                    out = y[j * rows:(j + 1) * rows, s * LANES:(s + 1) * LANES]
                    field[c * wide + s, j * group + q] = out.astype(BF)
            return 0

        lax.fori_loop(0, n_gz, pair, 0, unroll=8)
        for s in range(wide):
            start_y(inward, part_at, c * wide + s)

    def each(first, last, work):
        def one(c, _):
            work(c)
            return 0

        lax.fori_loop(first, last, one, 0)

    ends(0)
    for h in range(1, per_dev):
        ahead = functools.partial(inverse, h - 1)

        def pull(c, h=h, ahead=ahead):
            @pl.when(c == chunks - 1)
            def _():
                solve(h - 1)
                ahead(0)

            forward(h, c)

            @pl.when(c == 0)
            def _():
                chain(h - 1)

        if chunks > 1:
            each(0, chunks, pull)
            ends(h)
            each(1, chunks, ahead)
        else:
            forward(h, 0)
            chain(h - 1)
            ends(h)
            solve(h - 1)
            ahead(0)
    chain(per_dev - 1)
    solve(per_dev - 1)
    each(0, chunks, functools.partial(inverse, per_dev - 1))
    part[...] = jnp.zeros_like(part)

    def put(t):
        slot = lax.rem(t, 2)
        return pltpu.make_async_copy(term_buf.at[slot], term_hbm.at[:, t], t_sem.at[slot])

    def term(t, _):
        for h in range(per_dev):
            wait_y(inward, h, t)

        def pair(p, _):
            v = field_in[t, p].astype(F32)
            a = column[p]
            lit = live_ref[p] > 0
            rel = lane_rows - a
            for h in range(2):
                base = h * B
                near = pltpu.roll(v, lax.rem(a - base + 2 * LANES, LANES), 1)
                far = pltpu.roll(v, lax.rem(a - across - base + 3 * LANES, LANES), 1)
                v_p = jnp.where((rel >= 0) & (rel < B) & lit, near, 0.0)
                v_p = jnp.where((rel + across < B) & lit, far, v_p)
                scr[h, pl.ds(p, rows, stride=pitch), :] = v_p
            return 0

        lax.fori_loop(0, pairs, pair, 0, unroll=32)

        @pl.when(t >= 2)
        def _():
            put(t - 2).wait()

        slot = lax.rem(t, 2)
        for h in range(2):
            z = jnp.minimum(h * half + t, depth - 1)

            def some(i, _):
                got = []
                for k in range(block):
                    y = i * block + k
                    v = scr[h, pl.ds(pl.multiple_of(y * pitch, 8), pairs), :]
                    got.append((v * psi[h, t, y].astype(F32)).astype(BF))
                for k in range(0, block, side):
                    turned = jnp.concatenate(got[k:k + side], axis=0).T
                    term_buf[slot, h, i * (block // side) + k // side] = turned[:across]
                o = orb[z, pl.ds(i * block, block)].reshape(block * LANES, norb)
                part[...] += dot_nn(jnp.concatenate(got, axis=1), o)
                return 0

            lax.fori_loop(0, rows // block, some, 0, unroll=True)
        put(t).start()
        return 0

    lax.fori_loop(0, half, term, 0)

    def share(k):
        return remote(part.at[of(at_y(k), group)], part_in.at[k], a_out, a_in, "gy", at_y(k))

    def spread(k):
        return remote(slab_sum, slab_in.at[gz], b_out, b_in, "gz", at_z(k))

    def gather(k):
        return remote(total.at[of(gy, group)], total.at[of(gy, group)], c_out, c_in, "gy", at_y(k))

    for k in range(1, n_gy):
        share(k).start()
    own = part[of(gy, group), :]
    others = part_in.at[pl.ds(1, n_gy - 1)]
    pltpu.make_async_copy(others, others, a_in).wait()
    for k in range(1, n_gy):
        own = own + part_in[k]
    slab_sum[...] = own

    def begin(k, _):
        spread(k).start()
        return 0

    lax.fori_loop(0, n_gz - 1, begin, 0)
    slab_in[gz] = own

    others = slab_in.at[pl.ds(0, n_gz - 1)]
    pltpu.make_async_copy(others, others, b_in).wait()

    def add(i, acc):
        return acc + slab_in[i]

    total[of(gy, group), :] = lax.fori_loop(1, n_gz, add, slab_in[0])
    for k in range(1, n_gy):
        gather(k).start()
    others = total.at[pl.ds(0, (n_gy - 1) * group)]
    pltpu.make_async_copy(others, others, c_in).wait()
    high, low = split(total[...])
    rest = (total[...] - high.astype(F32) - low.astype(F32)).astype(BF)
    sel = hot_ref[:pairs]
    inner = dot_tn(jnp.concatenate([high, low, rest], axis=0), jnp.concatenate([sel, sel, sel], axis=0))
    mix_ref[:norb] = -(inner / (float(B) ** 3 / 4.0)).astype(BF)
    for k in range(side):
        mix_ref[norb + k * pairs:norb + (k + 1) * pairs] = sel

    sent_y(outward)
    sent_y(inward)
    given = pl.ds(0, per_dev * (n_gz - 1))
    remote(pq.at[given], edge_in.at[given], z_out, z_in.at[0], "gz", at_z(0)).wait_send()
    remote(pq.at[given], edge_in.at[given], e_out, e_in.at[0], "gz", at_z(0)).wait_send()
    spare = part_in.at[pl.ds(1, n_gy - 1)]
    remote(spare, spare, a_out, a_in, "gy", at_y(1)).wait_send()
    remote(spare, spare, c_out, c_in, "gy", at_y(1)).wait_send()
    spare = slab_in.at[pl.ds(0, n_gz - 1)]
    remote(spare, spare, b_out, b_in, "gz", at_z(0)).wait_send()
    for t in range(max(half - 2, 0), half):
        put(t).wait()


def gradient_kernel(side, mix_ref, orb_ref, term_ref, out_ref):
    lump, rows, across, norb = orb_ref.shape
    pairs = term_ref.shape[-1] // side
    lane = lax.broadcasted_iota(jnp.int32, (across, side * pairs), 1)

    def plane(z, _):
        held = []
        for y in range(rows):
            c = term_ref[0, z, y // side]
            if side > 1:
                k = y % side
                c = jnp.where((lane >= k * pairs) & (lane < (k + 1) * pairs), c, jnp.zeros_like(c))
            held.append(c)
        o = orb_ref[z].reshape(rows * across, norb)
        out = dot_nn(jnp.concatenate([o, jnp.concatenate(held, axis=0)], axis=1), mix_ref[...])
        out_ref[z] = out.reshape(rows, across, norb)
        return 0

    lax.fori_loop(0, lump, plane, 0, unroll=True)


def tables():
    index = np.arange(1, B + 1, dtype=np.float64)
    s = np.sqrt(2.0 / (B + 1.0)) * np.sin(np.pi * index[:, None] * index[None, :] / (B + 1.0))
    eigen = 2.0 - 2.0 * np.cos(np.pi * index / (B + 1.0))
    hi = s.astype(jnp.bfloat16).astype(np.float64)
    lo = (s - hi).astype(jnp.bfloat16).astype(np.float64)
    eye = np.eye(LANES // B)
    bd = lambda m: np.kron(eye, m)
    wide = np.block([[bd(hi), bd(lo)], [bd(hi), np.zeros((LANES, LANES))]]).astype(jnp.bfloat16)
    left = np.stack([np.concatenate([hi, lo], axis=1), np.concatenate([hi, np.zeros((B, B))], axis=1)])
    cosh = 1.0 + 0.5 * (eigen[:, None] + eigen[None, :])
    r = cosh - np.sqrt(cosh * cosh - 1.0)
    g = 1.0 / ((1.0 / r - r) * (1.0 - r ** (2 * B + 2)))
    twice = lambda m: np.tile(m, (1, LANES // B)).astype(np.float32)
    return left.astype(np.float32), wide, twice(r), twice(g)


def body(orbitals, pair_list, box_anchor, pair_live):
    depth, rows, across, norb = orbitals.shape
    n_gz = lax.axis_size("gz")
    n_gy = lax.axis_size("gy")
    pairs = pair_list.shape[0]
    group = pairs // n_gy
    per_dev = group // n_gz
    extent = depth * n_gz
    half = (depth + 1) // 2
    block = 12 if rows % 12 == 0 else 1
    side = max(LANES // pairs, 1) if block > 1 else 1

    smem = pl.BlockSpec(memory_space=pltpu.SMEM)
    vmem = pl.BlockSpec(memory_space=pltpu.VMEM)
    hbm = pl.BlockSpec(memory_space=pl.ANY)
    left, wide, rate, gain = (jnp.asarray(m) for m in tables())
    cycle = jnp.concatenate([left, jnp.zeros((2, extent - B, LANES), F32)], axis=1)
    table = jnp.concatenate([cycle, cycle], axis=1)
    mail = pltpu.VMEM((half, pairs, rows, LANES), BF)
    mode = pltpu.VMEM((group, B, LANES), F32)
    edges = pltpu.VMEM((group, B, LANES), BF)
    owners = pltpu.VMEM((per_dev, n_gz, B, LANES), BF)
    flags = lambda *shape: pltpu.SemaphoreType.DMA(shape)
    one = pltpu.SemaphoreType.DMA
    scratch = [
        pltpu.VMEM((2 * pairs, norb), F32),
        pltpu.VMEM((2 * pairs, norb), BF),
        pltpu.VMEM((depth, rows, LANES, norb), BF),
        pltpu.VMEM((2, half, rows, pairs, LANES), BF),
        pltpu.VMEM((2, rows * (pairs + GAP), LANES), F32),
        mail,
        mail,
        pltpu.VMEM((group, half, B, LANES), F32),
        pltpu.VMEM((B + 1, B, LANES), F32),
        mode,
        mode,
        edges,
        owners,
        owners,
        edges,
        pltpu.VMEM((n_gz, B, LANES), F32),
        mail,
        mail,
        pltpu.VMEM((2, 2, rows // side, across, side * pairs), BF),
        pltpu.VMEM((pairs, norb), F32),
        pltpu.VMEM((n_gy, group, norb), F32),
        pltpu.VMEM((group, norb), F32),
        pltpu.VMEM((n_gz, group, norb), F32),
        pltpu.VMEM((pairs, norb), F32),
    ]
    columns = [pltpu.SMEM((pairs,), jnp.int32)]
    semaphores = [
        flags(depth),
        one,
        flags(per_dev, half),
        one,
        flags(per_dev),
        one,
        flags(per_dev),
        one,
        flags(per_dev, half),
        flags(2),
        one,
        one,
        one,
        one,
        one,
        one,
    ]
    held = sum(math.prod(buffer.shape) * buffer.dtype.itemsize for buffer in scratch)
    stay = lambda x: pltpu.with_memory_space_constraint(x, pltpu.HBM)
    term, mix = pl.pallas_call(
        functools.partial(exchange_kernel, n_gz, n_gy),
        out_shape=(
            jax.ShapeDtypeStruct((2, half, rows // side, across, side * pairs), BF),
            jax.ShapeDtypeStruct((norb + side * pairs, norb), BF),
        ),
        in_specs=[smem] * 3 + [vmem] * 4 + [hbm],
        out_specs=(hbm, vmem),
        scratch_shapes=columns + scratch + semaphores,
        compiler_params=pltpu.CompilerParams(
            vmem_limit_bytes=held + SPARE_VMEM, collective_id=0, has_side_effects=True
        ),
        name="exchange",
    )(*(stay(x) for x in (pair_list.T, box_anchor.T, pair_live, table, wide, rate, gain, orbitals)))

    lump = 2 if depth == 2 * half and half % 2 == 0 else 1
    plane = pl.BlockSpec((lump, rows, across, norb), lambda z: (z, 0, 0, 0))
    per_half = half // lump
    return pl.pallas_call(
        functools.partial(gradient_kernel, side),
        grid=(depth // lump,),
        out_shape=jax.ShapeDtypeStruct(orbitals.shape, F32),
        in_specs=[
            pl.BlockSpec((norb + side * pairs, norb), lambda z: (0, 0)),
            plane,
            pl.BlockSpec(
                (1, lump, rows // side, across, side * pairs), lambda z: (z // per_half, z % per_half, 0, 0, 0)
            ),
        ],
        out_specs=plane,
        compiler_params=pltpu.CompilerParams(dimension_semantics=("arbitrary",), vmem_limit_bytes=GRADIENT_VMEM),
        name="gradient",
    )(mix, orbitals, term)


def solution(mesh):
    return jax.shard_map(
        body,
        mesh=mesh,
        in_specs=(P("gz", "gy", None, None), P(), P(), P()),
        out_specs=P("gz", "gy", None, None),
        check_vma=False,
    )
```

```python
import functools
import math

import jax
import jax.numpy as jnp
import numpy as np
from jax import lax
from jax.experimental import pallas as pl
from jax.experimental.pallas import tpu as pltpu
from jax.sharding import PartitionSpec as P

B = 64
LANES = 128
GAP = 8
MESH = pl.DeviceIdType.MESH
BF = jnp.bfloat16
F32 = jnp.float32
SPARE_VMEM = 5 * 512 * 1024
GRADIENT_VMEM = 24 * 1024 * 1024


def dot_nt(a, b):
    return lax.dot_general(a, b, (((1,), (1,)), ((), ())), preferred_element_type=F32)


def dot_nn(a, b):
    return lax.dot_general(a, b, (((1,), (0,)), ((), ())), preferred_element_type=F32)


def dot_tn(a, b):
    return lax.dot_general(a, b, (((0,), (0,)), ((), ())), preferred_element_type=F32)


def split(a):
    hi = a.astype(BF)
    return hi, (a - hi.astype(F32)).astype(BF)


def cell_index(az, extent, z):
    a = lax.rem(z - az + 2 * extent, extent)
    live = a < B
    return jnp.where(live, a + 1, 0), jnp.where(live, B - a, 0)


def power_of(r, n):
    out = None
    while n:
        if n & 1:
            out = r if out is None else out * r
        r = r * r
        n >>= 1
    return out


def exchange_kernel(
    n_gz, n_gy, list_ref, anchor_ref, live_ref, table_ref, wide_ref, r_ref, g_ref, orb_hbm,
    term_hbm, mix_ref,
    column, hot, hot_ref, orb, psi, scr, send, recv, d_ref, e_ref, f_ref, h_ref, pq, pq_in, edge, edge_in, keep, field, field_in,
    term_buf, part, part_in, slab_sum, slab_in, total,
    orb_sem, y_out, y_in, z_out, z_in, e_out, e_in, v_out, v_in, t_sem, a_out, a_in, b_out, b_in, c_out, c_in,
):
    depth, rows, across, norb = orb_hbm.shape
    half = psi.shape[1]
    pairs = psi.shape[3]
    group = pairs // n_gy
    per_dev = group // n_gz
    extent = depth * n_gz
    pitch = pairs + GAP
    wide = 2 if half % 2 == 0 else 1
    chunks = half // wide
    block = 12 if rows % 12 == 0 else 1
    side = max(LANES // pairs, 1) if block > 1 else 1
    gate = 0
    behind = min(2, chunks)
    gz = lax.axis_index("gz")
    gy = lax.axis_index("gy")
    at_y = lambda k: lax.rem(gy + k, n_gy)
    at_z = lambda k: lax.rem(gz + 1 + k, n_gz)
    lot = lambda j, h: pl.ds(pl.multiple_of(j * group + h * n_gz, n_gz), n_gz)
    of = lambda j, size: pl.ds(pl.multiple_of(j * size, size), size)

    def anchor(axis, p):
        return anchor_ref[axis, list_ref[0, p]]

    def start_y_of(q):
        return extent - anchor(1, gy * group + q)

    def remote(src, dst, out_sem, in_sem, axis, index):
        return pltpu.make_async_remote_copy(
            src_ref=src, dst_ref=dst, send_sem=out_sem, recv_sem=in_sem, device_id={axis: index}, device_id_type=MESH
        )

    def fetch(z):
        return pltpu.make_async_copy(orb_hbm.at[z], orb.at[z, :, pl.ds(0, across), :], orb_sem.at[z])

    def pad_and_fetch(z, _):
        orb[z, :, across:, :] = jnp.zeros((rows, LANES - across, norb), BF)
        fetch(z).start()
        return 0

    def pad_and_fetch_both(t, _):
        pad_and_fetch(t, 0)

        @pl.when(half + t < depth)
        def _():
            pad_and_fetch(half + t, 0)

        return 0

    lax.fori_loop(0, half, pad_and_fetch_both, 0)

    barrier = pltpu.get_barrier_semaphore()
    for k in range(1, n_gy):
        pl.semaphore_signal(barrier, inc=1, device_id={"gy": at_y(k)}, device_id_type=MESH)

    def greet(k, _):
        pl.semaphore_signal(barrier, inc=1, device_id={"gz": at_z(k)}, device_id_type=MESH)
        return 0

    lax.fori_loop(0, n_gz - 1, greet, 0)

    orbital = lax.broadcasted_iota(jnp.int32, (1, norb), 1)

    def mark(p, _):
        column[p] = anchor(2, p)
        for k in range(2):
            hot[pl.ds(k * pairs + p, 1), :] = (orbital == list_ref[k, p]).astype(F32)
        return 0

    lax.fori_loop(0, pairs, mark, 0, unroll=8)
    hot_ref[...] = hot[...].astype(BF)
    r2 = r_ref[...] * r_ref[...]
    e_ref[0] = jnp.zeros_like(r2)

    def fill(n, power):
        power = power * r2
        e_ref[n] = 1.0 - power
        return power

    lax.fori_loop(1, B + 1, fill, jnp.ones_like(r2))

    def across_y(mail, h, t, k):
        source, target, out_sem, in_sem = mail
        j = at_y(k)
        return remote(
            source.at[t, lot(j, h)], target.at[t, lot(gy, h)], out_sem, in_sem.at[h, t], "gy", j
        )

    def stay_y(mail, h, t):
        source, target, _, in_sem = mail
        return pltpu.make_async_copy(source.at[t, lot(gy, h)], target.at[t, lot(gy, h)], in_sem.at[h, t])

    def start_y(mail, h, t):
        for k in range(1, n_gy):
            across_y(mail, h, t, k).start()
        stay_y(mail, h, t).start()

    def wait_y(mail, h, t):
        _, target, _, in_sem = mail
        every = target.at[t, pl.ds(0, n_gy * n_gz)]
        pltpu.make_async_copy(every, every, in_sem.at[h, t]).wait()

    def sent_y(mail):
        source, target, out_sem, in_sem = mail
        every = pl.ds(0, (n_gy - 1) * group)
        remote(source.at[:, every], target.at[:, every], out_sem, in_sem.at[0, 0], "gy", at_y(1)).wait_send()

    outward = (send, recv, y_out, y_in)
    inward = (field, field_in, v_out, v_in)

    lane_rows = lax.broadcasted_iota(jnp.int32, (rows, LANES), 1)
    lane = lax.broadcasted_iota(jnp.int32, (B, LANES), 1)
    lower = lane < B

    def density(t):
        for h in range(2):
            z = jnp.minimum(h * half + t, depth - 1)

            @pl.when(h * half + t < depth)
            def _():
                fetch(z).wait()

            def some(i, carry):
                both = dot_nt(hot_ref[...], orb[z, pl.ds(i * 2, 2)].reshape(2 * LANES, norb))
                for k in range(2):
                    y = i * 2 + k
                    mine = both[:, k * LANES:(k + 1) * LANES]
                    value = mine[:pairs] * mine[pairs:] + carry
                    sent = value.astype(BF).astype(F32)
                    scr[h, pl.ds(pl.multiple_of(y * pitch, 8), pairs), :] = sent
                    psi[h, t, y] = mine[pairs:].astype(BF)
                    carry = value - sent
                return carry

            lax.fori_loop(0, rows // 2, some, jnp.zeros((pairs, LANES), F32), unroll=12)

        def pair(p, _):
            acc = jnp.zeros((rows, LANES), F32)
            a = column[p]
            for h in range(2):
                base = h * B
                x = scr[h, pl.ds(p, rows, stride=pitch), :]
                near = pltpu.roll(x, lax.rem(base - a + 2 * LANES, LANES), 1)
                far = pltpu.roll(x, lax.rem(base + across - a + 2 * LANES, LANES), 1)
                rel = lane_rows - base
                acc = jnp.where((rel >= 0) & (rel < B), jnp.where(rel < across - a, near, far), acc)
            send[t, p] = acc.astype(BF)
            return 0

        lax.fori_loop(0, pairs, pair, 0, unroll=32)
        @pl.when(t == gate)
        def _():
            pl.semaphore_wait(barrier, n_gy + n_gz - 2)
            for early in range(gate):
                start_y(outward, 0, early)

        @pl.when(t >= gate)
        def _():
            start_y(outward, 0, t)

    def forward(part_at, c):
        for s in range(wide):
            wait_y(outward, part_at, c * wide + s)

        def pair(n, _):
            q = part_at * n_gz + n
            m = table_ref[0, pl.ds(start_y_of(q), extent), :].astype(BF)
            planes = []
            for s in range(wide):
                got = [recv[c * wide + s, j * group + q].astype(F32) for j in range(n_gy)]
                planes.append(jnp.concatenate(got, axis=0).astype(BF))
            y = dot_tn(m, jnp.concatenate(planes, axis=1))
            y = y[:B] + y[B:]
            hi, lo = split(jnp.concatenate([y[:, s * LANES:(s + 1) * LANES] for s in range(wide)], axis=0))
            x = dot_nn(jnp.concatenate([hi, lo], axis=1), wide_ref[...])
            x = x[:, :LANES] + x[:, LANES:]
            for s in range(wide):
                d_ref[q, c * wide + s] = x[s * B:(s + 1) * B] * g_ref[...]
            return 0

        lax.fori_loop(0, n_gz, pair, 0, unroll=8)

    def stage(c, _):
        @pl.when(c < chunks)
        def _():
            def one(s, _):
                density(c * wide + s)
                return 0

            lax.fori_loop(0, wide, one, 0)

        @pl.when(c == chunks)
        def _():
            def rest(t, _):
                for h in range(1, per_dev):
                    start_y(outward, h, t)
                return 0

            lax.fori_loop(0, half, rest, 0)

        @pl.when(c >= behind)
        def _():
            forward(0, c - behind)

        return 0

    lax.fori_loop(0, chunks + behind, stage, 0)

    def weights(q):
        az = anchor(0, gy * group + q)
        out = []
        for t in range(half):
            lu, lw = cell_index(az, extent, gz * depth + t)
            hu, hw = cell_index(az, extent, gz * depth + half + t)
            if half + t >= depth:
                hu, hw = 0, 0
            out.append((jnp.where(lower, e_ref[lu], e_ref[hu]), jnp.where(lower, e_ref[lw], e_ref[hw])))
        return out

    def rate(r, t):
        return r if half + t < depth else jnp.where(lower, r, 1.0)

    def give(h, k):
        j = at_z(k)
        return remote(pq.at[h * n_gz + j], pq_in.at[h, gz], z_out, z_in.at[h], "gz", j)

    def give_back(h, k):
        j = at_z(k)
        return remote(edge.at[h, j], edge_in.at[h * n_gz + gz], e_out, e_in.at[h], "gz", j)

    def keep_own(h):
        return pltpu.make_async_copy(pq.at[h * n_gz + gz], pq_in.at[h, gz], z_in.at[h])

    def keep_edge(h):
        return pltpu.make_async_copy(edge.at[h, gz], edge_in.at[h * n_gz + gz], e_in.at[h])

    def ends(h):
        def one(k, _):
            q = h * n_gz + at_z(k)
            r = r_ref[...]
            at = weights(q)
            d = [d_ref[q, t] for t in range(half)]
            f = at[0][0] * d[0]
            for t in range(1, half):
                f = rate(r, t) * f + at[t][0] * d[t]
            b = r * (at[half - 1][1] * d[half - 1])
            for t in reversed(range(half - 1)):
                b = r * (b + at[t][1] * d[t])
            f_ref[q] = f
            h_ref[q] = b
            p_sum = power_of(r, depth - half) * f + pltpu.roll(f, B, 1)
            q_sum = pltpu.roll(b, B, 1) + power_of(r, half) * b
            pq[q] = jnp.where(lower, p_sum, q_sum).astype(BF)

            @pl.when(k < n_gz - 1)
            def _():
                give(h, k).start()

            return 0

        lax.fori_loop(0, n_gz, one, 0, unroll=2)
        keep_own(h).start()

    def chain(h):
        pltpu.make_async_copy(pq_in.at[h], pq_in.at[h], z_in.at[h]).wait()
        slab_rate = power_of(r_ref[...], depth)
        az = anchor(0, gy * group + h * n_gz + gz)

        def up(k, f):
            i = lax.rem(k, n_gz)
            start = lax.rem(depth * i - az + extent, extent)
            f = jnp.where(start < B, f, 0.0)
            keep[i] = f
            return pq_in[h, i].astype(F32) + slab_rate * f

        lax.fori_loop(0, 2 * n_gz, up, jnp.zeros((B, LANES), F32), unroll=8)

        def down(k, b):
            i = lax.rem(2 * n_gz - k, n_gz)
            end = lax.rem(depth * i + depth - 1 - az + extent, extent)
            b = jnp.where(end < B, b, 0.0)
            edge[h, i] = jnp.where(lower, keep[i], b).astype(BF)
            return pq_in[h, i].astype(F32) + slab_rate * b

        lax.fori_loop(0, 2 * n_gz, down, jnp.zeros((B, LANES), F32), unroll=8)

        def back(k, _):
            give_back(h, k).start()
            return 0

        lax.fori_loop(0, n_gz - 1, back, 0)
        keep_edge(h).start()

    def solve(h):
        every = edge_in.at[pl.ds(h * n_gz, n_gz)]
        pltpu.make_async_copy(every, every, e_in.at[h]).wait()

        def one(k, _):
            q = h * n_gz + k
            r = r_ref[...]
            at = weights(q)
            came = edge_in[q].astype(F32)
            swap = pltpu.roll(came, B, 1)
            f = jnp.where(lower, came, power_of(r, half) * swap + pltpu.roll(f_ref[q], B, 1))
            b = jnp.where(lower, power_of(r, depth - half) * swap + pltpu.roll(h_ref[q], B, 1), came)
            d = [d_ref[q, t] for t in range(half)]
            v = []
            for t in range(half):
                f = rate(r, t) * f + at[t][0] * d[t]
                v.append(at[t][1] * f)
            for t in reversed(range(half)):
                d_ref[q, t] = v[t] + at[t][0] * b
                b = rate(r, t) * (b + at[t][1] * d[t])
            return 0

        lax.fori_loop(0, n_gz, one, 0, unroll=2)

    def inverse(part_at, c):
        def pair(n, _):
            q = part_at * n_gz + n
            at = pl.ds(start_y_of(q), extent)
            m = jnp.concatenate([table_ref[0, at, :], table_ref[1, at, :]], axis=1).astype(BF)[:, :3 * B]
            hi, lo = split(jnp.concatenate([d_ref[q, c * wide + s] for s in range(wide)], axis=0))
            x = dot_nn(jnp.concatenate([hi, lo], axis=1), wide_ref[...])
            x = x[:, :LANES] + x[:, LANES:]
            hi, lo = split(jnp.concatenate([x[s * B:(s + 1) * B] for s in range(wide)], axis=1))
            y = dot_nn(m, jnp.concatenate([hi, hi, lo], axis=0))
            for s in range(wide):
                for j in range(n_gy):
                    out = y[j * rows:(j + 1) * rows, s * LANES:(s + 1) * LANES]
                    field[c * wide + s, j * group + q] = out.astype(BF)
            return 0

        lax.fori_loop(0, n_gz, pair, 0, unroll=8)
        for s in range(wide):
            start_y(inward, part_at, c * wide + s)

    def each(first, last, work):
        def one(c, _):
            work(c)
            return 0

        lax.fori_loop(first, last, one, 0)

    ends(0)
    for h in range(1, per_dev):
        ahead = functools.partial(inverse, h - 1)

        def pull(c, h=h, ahead=ahead):
            @pl.when(c == chunks - 1)
            def _():
                solve(h - 1)
                ahead(0)

            forward(h, c)

            @pl.when(c == 0)
            def _():
                chain(h - 1)

        if chunks > 1:
            each(0, chunks, pull)
            ends(h)
            each(1, chunks, ahead)
        else:
            forward(h, 0)
            chain(h - 1)
            ends(h)
            solve(h - 1)
            ahead(0)
    chain(per_dev - 1)
    solve(per_dev - 1)
    each(0, chunks, functools.partial(inverse, per_dev - 1))
    part[...] = jnp.zeros_like(part)

    def put(t):
        slot = lax.rem(t, 2)
        return pltpu.make_async_copy(term_buf.at[slot], term_hbm.at[:, t], t_sem.at[slot])

    def term(t, _):
        for h in range(per_dev):
            wait_y(inward, h, t)

        def pair(p, _):
            v = field_in[t, p].astype(F32)
            a = column[p]
            lit = live_ref[p] > 0
            rel = lane_rows - a
            for h in range(2):
                base = h * B
                near = pltpu.roll(v, lax.rem(a - base + 2 * LANES, LANES), 1)
                far = pltpu.roll(v, lax.rem(a - across - base + 3 * LANES, LANES), 1)
                v_p = jnp.where((rel >= 0) & (rel < B) & lit, near, 0.0)
                v_p = jnp.where((rel + across < B) & lit, far, v_p)
                scr[h, pl.ds(p, rows, stride=pitch), :] = v_p
            return 0

        lax.fori_loop(0, pairs, pair, 0, unroll=32)

        @pl.when(t >= 2)
        def _():
            put(t - 2).wait()

        slot = lax.rem(t, 2)
        for h in range(2):
            z = jnp.minimum(h * half + t, depth - 1)

            def some(i, _):
                got = []
                for k in range(block):
                    y = i * block + k
                    v = scr[h, pl.ds(pl.multiple_of(y * pitch, 8), pairs), :]
                    got.append((v * psi[h, t, y].astype(F32)).astype(BF))
                for k in range(0, block, side):
                    turned = jnp.concatenate(got[k:k + side], axis=0).T
                    term_buf[slot, h, i * (block // side) + k // side] = turned[:across]
                o = orb[z, pl.ds(i * block, block)].reshape(block * LANES, norb)
                part[...] += dot_nn(jnp.concatenate(got, axis=1), o)
                return 0

            lax.fori_loop(0, rows // block, some, 0, unroll=True)
        put(t).start()
        return 0

    lax.fori_loop(0, half, term, 0)

    def share(k):
        return remote(part.at[of(at_y(k), group)], part_in.at[k], a_out, a_in, "gy", at_y(k))

    def spread(k):
        return remote(slab_sum, slab_in.at[gz], b_out, b_in, "gz", at_z(k))

    def gather(k):
        return remote(total.at[of(gy, group)], total.at[of(gy, group)], c_out, c_in, "gy", at_y(k))

    for k in range(1, n_gy):
        share(k).start()
    own = part[of(gy, group), :]
    others = part_in.at[pl.ds(1, n_gy - 1)]
    pltpu.make_async_copy(others, others, a_in).wait()
    for k in range(1, n_gy):
        own = own + part_in[k]
    slab_sum[...] = own

    def begin(k, _):
        spread(k).start()
        return 0

    lax.fori_loop(0, n_gz - 1, begin, 0)
    slab_in[gz] = own

    others = slab_in.at[pl.ds(0, n_gz - 1)]
    pltpu.make_async_copy(others, others, b_in).wait()

    def add(i, acc):
        return acc + slab_in[i]

    total[of(gy, group), :] = lax.fori_loop(1, n_gz, add, slab_in[0])
    for k in range(1, n_gy):
        gather(k).start()
    others = total.at[pl.ds(0, (n_gy - 1) * group)]
    pltpu.make_async_copy(others, others, c_in).wait()
    high, low = split(total[...])
    rest = (total[...] - high.astype(F32) - low.astype(F32)).astype(BF)
    sel = hot_ref[:pairs]
    inner = dot_tn(jnp.concatenate([high, low, rest], axis=0), jnp.concatenate([sel, sel, sel], axis=0))
    mix_ref[:norb] = -(inner / (float(B) ** 3 / 4.0)).astype(BF)
    for k in range(side):
        mix_ref[norb + k * pairs:norb + (k + 1) * pairs] = sel

    sent_y(outward)
    sent_y(inward)
    given = pl.ds(0, per_dev * (n_gz - 1))
    remote(pq.at[given], edge_in.at[given], z_out, z_in.at[0], "gz", at_z(0)).wait_send()
    remote(pq.at[given], edge_in.at[given], e_out, e_in.at[0], "gz", at_z(0)).wait_send()
    spare = part_in.at[pl.ds(1, n_gy - 1)]
    remote(spare, spare, a_out, a_in, "gy", at_y(1)).wait_send()
    remote(spare, spare, c_out, c_in, "gy", at_y(1)).wait_send()
    spare = slab_in.at[pl.ds(0, n_gz - 1)]
    remote(spare, spare, b_out, b_in, "gz", at_z(0)).wait_send()
    for t in range(max(half - 2, 0), half):
        put(t).wait()


def gradient_kernel(side, mix_ref, orb_ref, term_ref, out_ref):
    lump, rows, across, norb = orb_ref.shape
    pairs = term_ref.shape[-1] // side
    lane = lax.broadcasted_iota(jnp.int32, (across, side * pairs), 1)

    def plane(z, _):
        held = []
        for y in range(rows):
            c = term_ref[0, z, y // side]
            if side > 1:
                k = y % side
                c = jnp.where((lane >= k * pairs) & (lane < (k + 1) * pairs), c, jnp.zeros_like(c))
            held.append(c)
        o = orb_ref[z].reshape(rows * across, norb)
        out = dot_nn(jnp.concatenate([o, jnp.concatenate(held, axis=0)], axis=1), mix_ref[...])
        out_ref[z] = out.reshape(rows, across, norb)
        return 0

    lax.fori_loop(0, lump, plane, 0, unroll=True)


def tables():
    index = np.arange(1, B + 1, dtype=np.float64)
    s = np.sqrt(2.0 / (B + 1.0)) * np.sin(np.pi * index[:, None] * index[None, :] / (B + 1.0))
    eigen = 2.0 - 2.0 * np.cos(np.pi * index / (B + 1.0))
    hi = s.astype(jnp.bfloat16).astype(np.float64)
    lo = (s - hi).astype(jnp.bfloat16).astype(np.float64)
    eye = np.eye(LANES // B)
    bd = lambda m: np.kron(eye, m)
    wide = np.block([[bd(hi), bd(lo)], [bd(hi), np.zeros((LANES, LANES))]]).astype(jnp.bfloat16)
    left = np.stack([np.concatenate([hi, lo], axis=1), np.concatenate([hi, np.zeros((B, B))], axis=1)])
    cosh = 1.0 + 0.5 * (eigen[:, None] + eigen[None, :])
    r = cosh - np.sqrt(cosh * cosh - 1.0)
    g = 1.0 / ((1.0 / r - r) * (1.0 - r ** (2 * B + 2)))
    twice = lambda m: np.tile(m, (1, LANES // B)).astype(np.float32)
    return left.astype(np.float32), wide, twice(r), twice(g)


def body(orbitals, pair_list, box_anchor, pair_live):
    depth, rows, across, norb = orbitals.shape
    n_gz = lax.axis_size("gz")
    n_gy = lax.axis_size("gy")
    pairs = pair_list.shape[0]
    group = pairs // n_gy
    per_dev = group // n_gz
    extent = depth * n_gz
    half = (depth + 1) // 2
    block = 12 if rows % 12 == 0 else 1
    side = max(LANES // pairs, 1) if block > 1 else 1

    smem = pl.BlockSpec(memory_space=pltpu.SMEM)
    vmem = pl.BlockSpec(memory_space=pltpu.VMEM)
    hbm = pl.BlockSpec(memory_space=pl.ANY)
    left, wide, rate, gain = (jnp.asarray(m) for m in tables())
    cycle = jnp.concatenate([left, jnp.zeros((2, extent - B, LANES), F32)], axis=1)
    table = jnp.concatenate([cycle, cycle], axis=1)
    mail = pltpu.VMEM((half, pairs, rows, LANES), BF)
    mode = pltpu.VMEM((group, B, LANES), F32)
    edges = pltpu.VMEM((group, B, LANES), BF)
    owners = pltpu.VMEM((per_dev, n_gz, B, LANES), BF)
    flags = lambda *shape: pltpu.SemaphoreType.DMA(shape)
    one = pltpu.SemaphoreType.DMA
    scratch = [
        pltpu.VMEM((2 * pairs, norb), F32),
        pltpu.VMEM((2 * pairs, norb), BF),
        pltpu.VMEM((depth, rows, LANES, norb), BF),
        pltpu.VMEM((2, half, rows, pairs, LANES), BF),
        pltpu.VMEM((2, rows * (pairs + GAP), LANES), F32),
        mail,
        mail,
        pltpu.VMEM((group, half, B, LANES), F32),
        pltpu.VMEM((B + 1, B, LANES), F32),
        mode,
        mode,
        edges,
        owners,
        owners,
        edges,
        pltpu.VMEM((n_gz, B, LANES), F32),
        mail,
        mail,
        pltpu.VMEM((2, 2, rows // side, across, side * pairs), BF),
        pltpu.VMEM((pairs, norb), F32),
        pltpu.VMEM((n_gy, group, norb), F32),
        pltpu.VMEM((group, norb), F32),
        pltpu.VMEM((n_gz, group, norb), F32),
        pltpu.VMEM((pairs, norb), F32),
    ]
    columns = [pltpu.SMEM((pairs,), jnp.int32)]
    semaphores = [
        flags(depth),
        one,
        flags(per_dev, half),
        one,
        flags(per_dev),
        one,
        flags(per_dev),
        one,
        flags(per_dev, half),
        flags(2),
        one,
        one,
        one,
        one,
        one,
        one,
    ]
    held = sum(math.prod(buffer.shape) * buffer.dtype.itemsize for buffer in scratch)
    stay = lambda x: pltpu.with_memory_space_constraint(x, pltpu.HBM)
    term, mix = pl.pallas_call(
        functools.partial(exchange_kernel, n_gz, n_gy),
        out_shape=(
            jax.ShapeDtypeStruct((2, half, rows // side, across, side * pairs), BF),
            jax.ShapeDtypeStruct((norb + side * pairs, norb), BF),
        ),
        in_specs=[smem] * 3 + [vmem] * 4 + [hbm],
        out_specs=(hbm, vmem),
        scratch_shapes=columns + scratch + semaphores,
        compiler_params=pltpu.CompilerParams(
            vmem_limit_bytes=held + SPARE_VMEM, collective_id=0, has_side_effects=True
        ),
        name="exchange",
    )(*(stay(x) for x in (pair_list.T, box_anchor.T, pair_live, table, wide, rate, gain, orbitals)))

    lump = 2 if depth == 2 * half and half % 2 == 0 else 1
    plane = pl.BlockSpec((lump, rows, across, norb), lambda z: (z, 0, 0, 0))
    per_half = half // lump
    return pl.pallas_call(
        functools.partial(gradient_kernel, side),
        grid=(depth // lump,),
        out_shape=jax.ShapeDtypeStruct(orbitals.shape, F32),
        in_specs=[
            pl.BlockSpec((norb + side * pairs, norb), lambda z: (0, 0)),
            plane,
            pl.BlockSpec(
                (1, lump, rows // side, across, side * pairs), lambda z: (z // per_half, z % per_half, 0, 0, 0)
            ),
        ],
        out_specs=plane,
        compiler_params=pltpu.CompilerParams(dimension_semantics=("arbitrary",), vmem_limit_bytes=GRADIENT_VMEM),
        name="gradient",
    )(mix, orbitals, term)


def solution(mesh):
    return jax.shard_map(
        body,
        mesh=mesh,
        in_specs=(P("gz", "gy", None, None), P(), P(), P()),
        out_specs=P("gz", "gy", None, None),
        check_vma=False,
    )
```

```python
import functools
import math

import jax
import jax.numpy as jnp
import numpy as np
from jax import lax
from jax.experimental import pallas as pl
from jax.experimental.pallas import tpu as pltpu
from jax.sharding import PartitionSpec as P

B = 64
LANES = 128
GAP = 8
MESH = pl.DeviceIdType.MESH
BF = jnp.bfloat16
F32 = jnp.float32
SPARE_VMEM = 5 * 512 * 1024
GRADIENT_VMEM = 24 * 1024 * 1024


def dot_nt(a, b):
    return lax.dot_general(a, b, (((1,), (1,)), ((), ())), preferred_element_type=F32)


def dot_nn(a, b):
    return lax.dot_general(a, b, (((1,), (0,)), ((), ())), preferred_element_type=F32)


def dot_tn(a, b):
    return lax.dot_general(a, b, (((0,), (0,)), ((), ())), preferred_element_type=F32)


def split(a):
    hi = a.astype(BF)
    return hi, (a - hi.astype(F32)).astype(BF)


def cell_index(az, extent, z):
    a = lax.rem(z - az + 2 * extent, extent)
    live = a < B
    return jnp.where(live, a + 1, 0), jnp.where(live, B - a, 0)


def power_of(r, n):
    out = None
    while n:
        if n & 1:
            out = r if out is None else out * r
        r = r * r
        n >>= 1
    return out


def exchange_kernel(
    n_gz, n_gy, list_ref, anchor_ref, live_ref, table_ref, wide_ref, r_ref, g_ref, orb_hbm,
    term_hbm, mix_ref,
    column, hot, hot_ref, orb, psi, scr, send, recv, d_ref, e_ref, f_ref, h_ref, pq, pq_in, edge, edge_in, keep, field, field_in,
    term_buf, part, part_in, slab_sum, slab_in, total,
    orb_sem, y_out, y_in, z_out, z_in, e_out, e_in, v_out, v_in, t_sem, a_out, a_in, b_out, b_in, c_out, c_in,
):
    depth, rows, across, norb = orb_hbm.shape
    half = psi.shape[1]
    pairs = psi.shape[3]
    group = pairs // n_gy
    per_dev = group // n_gz
    extent = depth * n_gz
    pitch = pairs + GAP
    wide = 2 if half % 2 == 0 else 1
    chunks = half // wide
    block = 12 if rows % 12 == 0 else 1
    side = max(LANES // pairs, 1) if block > 1 else 1
    gate = 0
    behind = min(2, chunks)
    gz = lax.axis_index("gz")
    gy = lax.axis_index("gy")
    at_y = lambda k: lax.rem(gy + k, n_gy)
    at_z = lambda k: lax.rem(gz + 1 + k, n_gz)
    lot = lambda j, h: pl.ds(pl.multiple_of(j * group + h * n_gz, n_gz), n_gz)
    of = lambda j, size: pl.ds(pl.multiple_of(j * size, size), size)

    def anchor(axis, p):
        return anchor_ref[axis, list_ref[0, p]]

    def start_y_of(q):
        return extent - anchor(1, gy * group + q)

    def remote(src, dst, out_sem, in_sem, axis, index):
        return pltpu.make_async_remote_copy(
            src_ref=src, dst_ref=dst, send_sem=out_sem, recv_sem=in_sem, device_id={axis: index}, device_id_type=MESH
        )

    def fetch(z):
        return pltpu.make_async_copy(orb_hbm.at[z], orb.at[z, :, pl.ds(0, across), :], orb_sem.at[z])

    barrier = pltpu.get_barrier_semaphore()
    for k in range(1, n_gy):
        pl.semaphore_signal(barrier, inc=1, device_id={"gy": at_y(k)}, device_id_type=MESH)

    def greet(k, _):
        pl.semaphore_signal(barrier, inc=1, device_id={"gz": at_z(k)}, device_id_type=MESH)
        return 0

    lax.fori_loop(0, n_gz - 1, greet, 0)

    def pad_and_fetch(z, _):
        orb[z, :, across:, :] = jnp.zeros((rows, LANES - across, norb), BF)
        fetch(z).start()
        return 0

    def pad_and_fetch_both(t, _):
        pad_and_fetch(t, 0)

        @pl.when(half + t < depth)
        def _():
            pad_and_fetch(half + t, 0)

        return 0

    lax.fori_loop(0, half, pad_and_fetch_both, 0)

    orbital = lax.broadcasted_iota(jnp.int32, (1, norb), 1)

    def mark(p, _):
        column[p] = anchor(2, p)
        for k in range(2):
            hot[pl.ds(k * pairs + p, 1), :] = (orbital == list_ref[k, p]).astype(F32)
        return 0

    lax.fori_loop(0, pairs, mark, 0, unroll=8)
    hot_ref[...] = hot[...].astype(BF)
    r2 = r_ref[...] * r_ref[...]
    e_ref[0] = jnp.zeros_like(r2)

    def fill(n, power):
        power = power * r2
        e_ref[n] = 1.0 - power
        return power

    lax.fori_loop(1, B + 1, fill, jnp.ones_like(r2))

    def across_y(mail, h, t, k):
        source, target, out_sem, in_sem = mail
        j = at_y(k)
        return remote(
            source.at[t, lot(j, h)], target.at[t, lot(gy, h)], out_sem, in_sem.at[h, t], "gy", j
        )

    def stay_y(mail, h, t):
        source, target, _, in_sem = mail
        return pltpu.make_async_copy(source.at[t, lot(gy, h)], target.at[t, lot(gy, h)], in_sem.at[h, t])

    def start_y(mail, h, t):
        for k in range(1, n_gy):
            across_y(mail, h, t, k).start()
        stay_y(mail, h, t).start()

    def wait_y(mail, h, t):
        _, target, _, in_sem = mail
        every = target.at[t, pl.ds(0, n_gy * n_gz)]
        pltpu.make_async_copy(every, every, in_sem.at[h, t]).wait()

    def sent_y(mail):
        source, target, out_sem, in_sem = mail
        every = pl.ds(0, (n_gy - 1) * group)
        remote(source.at[:, every], target.at[:, every], out_sem, in_sem.at[0, 0], "gy", at_y(1)).wait_send()

    outward = (send, recv, y_out, y_in)
    inward = (field, field_in, v_out, v_in)

    lane_rows = lax.broadcasted_iota(jnp.int32, (rows, LANES), 1)
    lane = lax.broadcasted_iota(jnp.int32, (B, LANES), 1)
    lower = lane < B

    def density(t):
        for h in range(2):
            z = jnp.minimum(h * half + t, depth - 1)

            @pl.when(h * half + t < depth)
            def _():
                fetch(z).wait()

            def some(i, carry):
                both = dot_nt(hot_ref[...], orb[z, pl.ds(i * 2, 2)].reshape(2 * LANES, norb))
                for k in range(2):
                    y = i * 2 + k
                    mine = both[:, k * LANES:(k + 1) * LANES]
                    value = mine[:pairs] * mine[pairs:] + carry
                    sent = value.astype(BF).astype(F32)
                    scr[h, pl.ds(pl.multiple_of(y * pitch, 8), pairs), :] = sent
                    psi[h, t, y] = mine[pairs:].astype(BF)
                    carry = value - sent
                return carry

            lax.fori_loop(0, rows // 2, some, jnp.zeros((pairs, LANES), F32), unroll=12)

        def pair(p, _):
            acc = jnp.zeros((rows, LANES), F32)
            a = column[p]
            for h in range(2):
                base = h * B
                x = scr[h, pl.ds(p, rows, stride=pitch), :]
                near = pltpu.roll(x, lax.rem(base - a + 2 * LANES, LANES), 1)
                far = pltpu.roll(x, lax.rem(base + across - a + 2 * LANES, LANES), 1)
                rel = lane_rows - base
                acc = jnp.where((rel >= 0) & (rel < B), jnp.where(rel < across - a, near, far), acc)
            send[t, p] = acc.astype(BF)
            return 0

        lax.fori_loop(0, pairs, pair, 0, unroll=32)
        @pl.when(t == gate)
        def _():
            pl.semaphore_wait(barrier, n_gy + n_gz - 2)
            for early in range(gate):
                start_y(outward, 0, early)

        @pl.when(t >= gate)
        def _():
            start_y(outward, 0, t)

    def forward(part_at, c):
        for s in range(wide):
            wait_y(outward, part_at, c * wide + s)

        def pair(n, _):
            q = part_at * n_gz + n
            m = table_ref[0, pl.ds(start_y_of(q), extent), :].astype(BF)
            planes = []
            for s in range(wide):
                got = [recv[c * wide + s, j * group + q].astype(F32) for j in range(n_gy)]
                planes.append(jnp.concatenate(got, axis=0).astype(BF))
            y = dot_tn(m, jnp.concatenate(planes, axis=1))
            y = y[:B] + y[B:]
            hi, lo = split(jnp.concatenate([y[:, s * LANES:(s + 1) * LANES] for s in range(wide)], axis=0))
            x = dot_nn(jnp.concatenate([hi, lo], axis=1), wide_ref[...])
            x = x[:, :LANES] + x[:, LANES:]
            for s in range(wide):
                d_ref[q, c * wide + s] = x[s * B:(s + 1) * B] * g_ref[...]
            return 0

        lax.fori_loop(0, n_gz, pair, 0, unroll=8)

    def stage(c, _):
        @pl.when(c < chunks)
        def _():
            def one(s, _):
                density(c * wide + s)
                return 0

            lax.fori_loop(0, wide, one, 0)

        @pl.when(c == chunks)
        def _():
            def rest(t, _):
                for h in range(1, per_dev):
                    start_y(outward, h, t)
                return 0

            lax.fori_loop(0, half, rest, 0)

        @pl.when(c >= behind)
        def _():
            forward(0, c - behind)

        return 0

    lax.fori_loop(0, chunks + behind, stage, 0)

    def weights(q):
        az = anchor(0, gy * group + q)
        out = []
        for t in range(half):
            lu, lw = cell_index(az, extent, gz * depth + t)
            hu, hw = cell_index(az, extent, gz * depth + half + t)
            if half + t >= depth:
                hu, hw = 0, 0
            out.append((jnp.where(lower, e_ref[lu], e_ref[hu]), jnp.where(lower, e_ref[lw], e_ref[hw])))
        return out

    def rate(r, t):
        return r if half + t < depth else jnp.where(lower, r, 1.0)

    def give(h, k):
        j = at_z(k)
        return remote(pq.at[h * n_gz + j], pq_in.at[h, gz], z_out, z_in.at[h], "gz", j)

    def give_back(h, k):
        j = at_z(k)
        return remote(edge.at[h, j], edge_in.at[h * n_gz + gz], e_out, e_in.at[h], "gz", j)

    def keep_own(h):
        return pltpu.make_async_copy(pq.at[h * n_gz + gz], pq_in.at[h, gz], z_in.at[h])

    def keep_edge(h):
        return pltpu.make_async_copy(edge.at[h, gz], edge_in.at[h * n_gz + gz], e_in.at[h])

    def ends(h):
        def one(k, _):
            q = h * n_gz + at_z(k)
            r = r_ref[...]
            at = weights(q)
            d = [d_ref[q, t] for t in range(half)]
            f = at[0][0] * d[0]
            for t in range(1, half):
                f = rate(r, t) * f + at[t][0] * d[t]
            b = r * (at[half - 1][1] * d[half - 1])
            for t in reversed(range(half - 1)):
                b = r * (b + at[t][1] * d[t])
            f_ref[q] = f
            h_ref[q] = b
            p_sum = power_of(r, depth - half) * f + pltpu.roll(f, B, 1)
            q_sum = pltpu.roll(b, B, 1) + power_of(r, half) * b
            pq[q] = jnp.where(lower, p_sum, q_sum).astype(BF)

            @pl.when(k < n_gz - 1)
            def _():
                give(h, k).start()

            return 0

        lax.fori_loop(0, n_gz, one, 0, unroll=2)
        keep_own(h).start()

    def chain(h):
        pltpu.make_async_copy(pq_in.at[h], pq_in.at[h], z_in.at[h]).wait()
        slab_rate = power_of(r_ref[...], depth)
        az = anchor(0, gy * group + h * n_gz + gz)

        def up(k, f):
            i = lax.rem(k, n_gz)
            start = lax.rem(depth * i - az + extent, extent)
            f = jnp.where(start < B, f, 0.0)
            keep[i] = f
            return pq_in[h, i].astype(F32) + slab_rate * f

        lax.fori_loop(0, 2 * n_gz, up, jnp.zeros((B, LANES), F32), unroll=8)

        def down(k, b):
            i = lax.rem(2 * n_gz - k, n_gz)
            end = lax.rem(depth * i + depth - 1 - az + extent, extent)
            b = jnp.where(end < B, b, 0.0)
            edge[h, i] = jnp.where(lower, keep[i], b).astype(BF)
            return pq_in[h, i].astype(F32) + slab_rate * b

        lax.fori_loop(0, 2 * n_gz, down, jnp.zeros((B, LANES), F32), unroll=8)

        def back(k, _):
            give_back(h, k).start()
            return 0

        lax.fori_loop(0, n_gz - 1, back, 0)
        keep_edge(h).start()

    def solve(h):
        every = edge_in.at[pl.ds(h * n_gz, n_gz)]
        pltpu.make_async_copy(every, every, e_in.at[h]).wait()

        def one(k, _):
            q = h * n_gz + k
            r = r_ref[...]
            at = weights(q)
            came = edge_in[q].astype(F32)
            swap = pltpu.roll(came, B, 1)
            f = jnp.where(lower, came, power_of(r, half) * swap + pltpu.roll(f_ref[q], B, 1))
            b = jnp.where(lower, power_of(r, depth - half) * swap + pltpu.roll(h_ref[q], B, 1), came)
            d = [d_ref[q, t] for t in range(half)]
            v = []
            for t in range(half):
                f = rate(r, t) * f + at[t][0] * d[t]
                v.append(at[t][1] * f)
            for t in reversed(range(half)):
                d_ref[q, t] = v[t] + at[t][0] * b
                b = rate(r, t) * (b + at[t][1] * d[t])
            return 0

        lax.fori_loop(0, n_gz, one, 0, unroll=2)

    def inverse(part_at, c):
        def pair(n, _):
            q = part_at * n_gz + n
            at = pl.ds(start_y_of(q), extent)
            m = jnp.concatenate([table_ref[0, at, :], table_ref[1, at, :]], axis=1).astype(BF)[:, :3 * B]
            hi, lo = split(jnp.concatenate([d_ref[q, c * wide + s] for s in range(wide)], axis=0))
            x = dot_nn(jnp.concatenate([hi, lo], axis=1), wide_ref[...])
            x = x[:, :LANES] + x[:, LANES:]
            hi, lo = split(jnp.concatenate([x[s * B:(s + 1) * B] for s in range(wide)], axis=1))
            y = dot_nn(m, jnp.concatenate([hi, hi, lo], axis=0))
            for s in range(wide):
                for j in range(n_gy):
                    out = y[j * rows:(j + 1) * rows, s * LANES:(s + 1) * LANES]
                    field[c * wide + s, j * group + q] = out.astype(BF)
            return 0

        lax.fori_loop(0, n_gz, pair, 0, unroll=8)
        for s in range(wide):
            start_y(inward, part_at, c * wide + s)

    def each(first, last, work):
        def one(c, _):
            work(c)
            return 0

        lax.fori_loop(first, last, one, 0)

    ends(0)
    for h in range(1, per_dev):
        ahead = functools.partial(inverse, h - 1)

        def pull(c, h=h, ahead=ahead):
            @pl.when(c == chunks - 1)
            def _():
                solve(h - 1)
                ahead(0)

            forward(h, c)

            @pl.when(c == 0)
            def _():
                chain(h - 1)

        if chunks > 1:
            each(0, chunks, pull)
            ends(h)
            each(1, chunks, ahead)
        else:
            forward(h, 0)
            chain(h - 1)
            ends(h)
            solve(h - 1)
            ahead(0)
    chain(per_dev - 1)
    solve(per_dev - 1)
    each(0, chunks, functools.partial(inverse, per_dev - 1))
    part[...] = jnp.zeros_like(part)

    def put(t):
        slot = lax.rem(t, 2)
        return pltpu.make_async_copy(term_buf.at[slot], term_hbm.at[:, t], t_sem.at[slot])

    def term(t, _):
        for h in range(per_dev):
            wait_y(inward, h, t)

        def pair(p, _):
            v = field_in[t, p].astype(F32)
            a = column[p]
            lit = live_ref[p] > 0
            rel = lane_rows - a
            for h in range(2):
                base = h * B
                near = pltpu.roll(v, lax.rem(a - base + 2 * LANES, LANES), 1)
                far = pltpu.roll(v, lax.rem(a - across - base + 3 * LANES, LANES), 1)
                v_p = jnp.where((rel >= 0) & (rel < B) & lit, near, 0.0)
                v_p = jnp.where((rel + across < B) & lit, far, v_p)
                scr[h, pl.ds(p, rows, stride=pitch), :] = v_p
            return 0

        lax.fori_loop(0, pairs, pair, 0, unroll=32)

        @pl.when(t >= 2)
        def _():
            put(t - 2).wait()

        slot = lax.rem(t, 2)
        for h in range(2):
            z = jnp.minimum(h * half + t, depth - 1)

            def some(i, _):
                got = []
                for k in range(block):
                    y = i * block + k
                    v = scr[h, pl.ds(pl.multiple_of(y * pitch, 8), pairs), :]
                    got.append((v * psi[h, t, y].astype(F32)).astype(BF))
                for k in range(0, block, side):
                    turned = jnp.concatenate(got[k:k + side], axis=0).T
                    term_buf[slot, h, i * (block // side) + k // side] = turned[:across]
                o = orb[z, pl.ds(i * block, block)].reshape(block * LANES, norb)
                part[...] += dot_nn(jnp.concatenate(got, axis=1), o)
                return 0

            lax.fori_loop(0, rows // block, some, 0, unroll=True)
        put(t).start()
        return 0

    lax.fori_loop(0, half, term, 0)

    def share(k):
        return remote(part.at[of(at_y(k), group)], part_in.at[k], a_out, a_in, "gy", at_y(k))

    def spread(k):
        return remote(slab_sum, slab_in.at[gz], b_out, b_in, "gz", at_z(k))

    def gather(k):
        return remote(total.at[of(gy, group)], total.at[of(gy, group)], c_out, c_in, "gy", at_y(k))

    for k in range(1, n_gy):
        share(k).start()
    own = part[of(gy, group), :]
    others = part_in.at[pl.ds(1, n_gy - 1)]
    pltpu.make_async_copy(others, others, a_in).wait()
    for k in range(1, n_gy):
        own = own + part_in[k]
    slab_sum[...] = own

    def begin(k, _):
        spread(k).start()
        return 0

    lax.fori_loop(0, n_gz - 1, begin, 0)
    slab_in[gz] = own

    others = slab_in.at[pl.ds(0, n_gz - 1)]
    pltpu.make_async_copy(others, others, b_in).wait()

    def add(i, acc):
        return acc + slab_in[i]

    total[of(gy, group), :] = lax.fori_loop(1, n_gz, add, slab_in[0])
    for k in range(1, n_gy):
        gather(k).start()
    others = total.at[pl.ds(0, (n_gy - 1) * group)]
    pltpu.make_async_copy(others, others, c_in).wait()
    high, low = split(total[...])
    rest = (total[...] - high.astype(F32) - low.astype(F32)).astype(BF)
    sel = hot_ref[:pairs]
    inner = dot_tn(jnp.concatenate([high, low, rest], axis=0), jnp.concatenate([sel, sel, sel], axis=0))
    mix_ref[:norb] = -(inner / (float(B) ** 3 / 4.0)).astype(BF)
    for k in range(side):
        mix_ref[norb + k * pairs:norb + (k + 1) * pairs] = sel

    sent_y(outward)
    sent_y(inward)
    given = pl.ds(0, per_dev * (n_gz - 1))
    remote(pq.at[given], edge_in.at[given], z_out, z_in.at[0], "gz", at_z(0)).wait_send()
    remote(pq.at[given], edge_in.at[given], e_out, e_in.at[0], "gz", at_z(0)).wait_send()
    spare = part_in.at[pl.ds(1, n_gy - 1)]
    remote(spare, spare, a_out, a_in, "gy", at_y(1)).wait_send()
    remote(spare, spare, c_out, c_in, "gy", at_y(1)).wait_send()
    spare = slab_in.at[pl.ds(0, n_gz - 1)]
    remote(spare, spare, b_out, b_in, "gz", at_z(0)).wait_send()
    for t in range(max(half - 2, 0), half):
        put(t).wait()


def gradient_kernel(side, mix_ref, orb_ref, term_ref, out_ref):
    lump, rows, across, norb = orb_ref.shape
    pairs = term_ref.shape[-1] // side
    lane = lax.broadcasted_iota(jnp.int32, (across, side * pairs), 1)

    def plane(z, _):
        held = []
        for y in range(rows):
            c = term_ref[0, z, y // side]
            if side > 1:
                k = y % side
                c = jnp.where((lane >= k * pairs) & (lane < (k + 1) * pairs), c, jnp.zeros_like(c))
            held.append(c)
        o = orb_ref[z].reshape(rows * across, norb)
        out = dot_nn(jnp.concatenate([o, jnp.concatenate(held, axis=0)], axis=1), mix_ref[...])
        out_ref[z] = out.reshape(rows, across, norb)
        return 0

    lax.fori_loop(0, lump, plane, 0, unroll=True)


def tables():
    index = np.arange(1, B + 1, dtype=np.float64)
    s = np.sqrt(2.0 / (B + 1.0)) * np.sin(np.pi * index[:, None] * index[None, :] / (B + 1.0))
    eigen = 2.0 - 2.0 * np.cos(np.pi * index / (B + 1.0))
    hi = s.astype(jnp.bfloat16).astype(np.float64)
    lo = (s - hi).astype(jnp.bfloat16).astype(np.float64)
    eye = np.eye(LANES // B)
    bd = lambda m: np.kron(eye, m)
    wide = np.block([[bd(hi), bd(lo)], [bd(hi), np.zeros((LANES, LANES))]]).astype(jnp.bfloat16)
    left = np.stack([np.concatenate([hi, lo], axis=1), np.concatenate([hi, np.zeros((B, B))], axis=1)])
    cosh = 1.0 + 0.5 * (eigen[:, None] + eigen[None, :])
    r = cosh - np.sqrt(cosh * cosh - 1.0)
    g = 1.0 / ((1.0 / r - r) * (1.0 - r ** (2 * B + 2)))
    twice = lambda m: np.tile(m, (1, LANES // B)).astype(np.float32)
    return left.astype(np.float32), wide, twice(r), twice(g)


def body(orbitals, pair_list, box_anchor, pair_live):
    depth, rows, across, norb = orbitals.shape
    n_gz = lax.axis_size("gz")
    n_gy = lax.axis_size("gy")
    pairs = pair_list.shape[0]
    group = pairs // n_gy
    per_dev = group // n_gz
    extent = depth * n_gz
    half = (depth + 1) // 2
    block = 12 if rows % 12 == 0 else 1
    side = max(LANES // pairs, 1) if block > 1 else 1

    smem = pl.BlockSpec(memory_space=pltpu.SMEM)
    vmem = pl.BlockSpec(memory_space=pltpu.VMEM)
    hbm = pl.BlockSpec(memory_space=pl.ANY)
    left, wide, rate, gain = (jnp.asarray(m) for m in tables())
    cycle = jnp.concatenate([left, jnp.zeros((2, extent - B, LANES), F32)], axis=1)
    table = jnp.concatenate([cycle, cycle], axis=1)
    mail = pltpu.VMEM((half, pairs, rows, LANES), BF)
    mode = pltpu.VMEM((group, B, LANES), F32)
    edges = pltpu.VMEM((group, B, LANES), BF)
    owners = pltpu.VMEM((per_dev, n_gz, B, LANES), BF)
    flags = lambda *shape: pltpu.SemaphoreType.DMA(shape)
    one = pltpu.SemaphoreType.DMA
    scratch = [
        pltpu.VMEM((2 * pairs, norb), F32),
        pltpu.VMEM((2 * pairs, norb), BF),
        pltpu.VMEM((depth, rows, LANES, norb), BF),
        pltpu.VMEM((2, half, rows, pairs, LANES), BF),
        pltpu.VMEM((2, rows * (pairs + GAP), LANES), F32),
        mail,
        mail,
        pltpu.VMEM((group, half, B, LANES), F32),
        pltpu.VMEM((B + 1, B, LANES), F32),
        mode,
        mode,
        edges,
        owners,
        owners,
        edges,
        pltpu.VMEM((n_gz, B, LANES), F32),
        mail,
        mail,
        pltpu.VMEM((2, 2, rows // side, across, side * pairs), BF),
        pltpu.VMEM((pairs, norb), F32),
        pltpu.VMEM((n_gy, group, norb), F32),
        pltpu.VMEM((group, norb), F32),
        pltpu.VMEM((n_gz, group, norb), F32),
        pltpu.VMEM((pairs, norb), F32),
    ]
    columns = [pltpu.SMEM((pairs,), jnp.int32)]
    semaphores = [
        flags(depth),
        one,
        flags(per_dev, half),
        one,
        flags(per_dev),
        one,
        flags(per_dev),
        one,
        flags(per_dev, half),
        flags(2),
        one,
        one,
        one,
        one,
        one,
        one,
    ]
    held = sum(math.prod(buffer.shape) * buffer.dtype.itemsize for buffer in scratch)
    stay = lambda x: pltpu.with_memory_space_constraint(x, pltpu.HBM)
    term, mix = pl.pallas_call(
        functools.partial(exchange_kernel, n_gz, n_gy),
        out_shape=(
            jax.ShapeDtypeStruct((2, half, rows // side, across, side * pairs), BF),
            jax.ShapeDtypeStruct((norb + side * pairs, norb), BF),
        ),
        in_specs=[smem] * 3 + [vmem] * 4 + [hbm],
        out_specs=(hbm, vmem),
        scratch_shapes=columns + scratch + semaphores,
        compiler_params=pltpu.CompilerParams(
            vmem_limit_bytes=held + SPARE_VMEM, collective_id=0, has_side_effects=True
        ),
        name="exchange",
    )(*(stay(x) for x in (pair_list.T, box_anchor.T, pair_live, table, wide, rate, gain, orbitals)))

    lump = 2 if depth == 2 * half and half % 2 == 0 else 1
    plane = pl.BlockSpec((lump, rows, across, norb), lambda z: (z, 0, 0, 0))
    per_half = half // lump
    return pl.pallas_call(
        functools.partial(gradient_kernel, side),
        grid=(depth // lump,),
        out_shape=jax.ShapeDtypeStruct(orbitals.shape, F32),
        in_specs=[
            pl.BlockSpec((norb + side * pairs, norb), lambda z: (0, 0)),
            plane,
            pl.BlockSpec(
                (1, lump, rows // side, across, side * pairs), lambda z: (z // per_half, z % per_half, 0, 0, 0)
            ),
        ],
        out_specs=plane,
        compiler_params=pltpu.CompilerParams(dimension_semantics=("arbitrary",), vmem_limit_bytes=GRADIENT_VMEM),
        name="gradient",
    )(mix, orbitals, term)


def solution(mesh):
    return jax.shard_map(
        body,
        mesh=mesh,
        in_specs=(P("gz", "gy", None, None), P(), P(), P()),
        out_specs=P("gz", "gy", None, None),
        check_vma=False,
    )
```
